128 devices in a mesh: rows: 8 (over z, y_lo), cols: 16 (over x, y_hi, core).
Axes of the slice: x: 4, y: 4 (y_hi: 2, y_lo: 2; y = y_hi * 2 + y_lo), z: 4, core: 2. Of those that a mesh axis runs over, the one named last changes fastest.
Arguments:
- imagery: bfloat16 [128, 256, 192], P('rows', 'cols'), may hold values from -6 to 6
- cotangent: bfloat16 [128, 256, 192], P('rows', 'cols'), may hold values from -6 to 6
- norm_gain: float32 [2, 192], replicated, may hold values from 0.5 to 1.5
- norm_bias: float32 [2, 192], replicated, may hold values from -3 to 3
- qkv_weight: bfloat16 [2, 192, 576], replicated, may hold values from -0.4375 to 0.4375
- qkv_bias: float32 [2, 576], replicated, may hold values from -3 to 3
- rel_table: float32 [2, 6, 225], replicated, may hold values from -4 to 330
- proj_weight: bfloat16 [2, 192, 192], replicated, may hold values from -0.4375 to 0.4375
- proj_bias: float32 [2, 192], replicated, may hold values from -3 to 3
- mlp_gain: float32 [2, 192], replicated, may hold values from 0.5 to 1.5
- mlp_bias: float32 [2, 192], replicated, may hold values from -3 to 3
- up_weight: bfloat16 [2, 192, 768], replicated, may hold values from -0.4375 to 0.4375
- up_bias: float32 [2, 768], replicated, may hold values from -3 to 3
- down_weight: bfloat16 [2, 768, 192], replicated, may hold values from -0.21875 to 0.21875
- down_bias: float32 [2, 192], replicated, may hold values from -3 to 3
Outputs:
- output: bfloat16 [128, 256, 192], P('rows', 'cols')
- imagery_grad: bfloat16 [128, 256, 192], P('rows', 'cols')
- norm_gain_grad: float32 [2, 192], replicated
- norm_bias_grad: float32 [2, 192], replicated
- qkv_weight_grad: float32 [2, 192, 576], replicated
- qkv_bias_grad: float32 [2, 576], replicated
- rel_table_grad: float32 [2, 6, 225], replicated
- proj_weight_grad: float32 [2, 192, 192], replicated
- proj_bias_grad: float32 [2, 192], replicated
- mlp_gain_grad: float32 [2, 192], replicated
- mlp_bias_grad: float32 [2, 192], replicated
- up_weight_grad: float32 [2, 192, 768], replicated
- up_bias_grad: float32 [2, 768], replicated
- down_weight_grad: float32 [2, 768, 192], replicated
- down_bias_grad: float32 [2, 192], replicated
The draws below stay inside these ranges and needn't reach their ends.
All inputs are finite; a program needn't handle non-finite values.
Results may differ from the reference program's by a relative error of at most 0.02.
Values may be sent and summed in bfloat16 or wider, within the bound.
No kernel may reach another device: no remote copies, remote signals or barrier semaphores. Data moves between devices by JAX's collectives and lax.ppermute only.
A program may use at most 128 MiB of HBM per device.

```python
import jax
import jax.numpy as jnp
import numpy as np
from jax import lax

C = 192
HEADS = 6
MLP = 768
WIN = 8
TILE = 16
HEIGHT = 128
WIDTH = 256
N_ROWS = 8
N_COLS = 16


def draw_rel_table(key, part):
    columns = (2 * WIN - 1) ** 2
    return jnp.clip(jax.random.normal(key, (2, HEADS, columns), jnp.float32), -4.0, 4.0)


def levels(key, shape, pieces, low, high):
    loudness = 1.0
    for dim, parts in pieces:
        draws = jax.random.uniform(jax.random.fold_in(jax.random.fold_in(key, 6), dim), (parts,), jnp.float32, low / len(pieces), high / len(pieces))
        loudness = loudness * jnp.repeat(jnp.exp(draws), shape[dim] // parts).reshape((-1,) + (1,) * (len(shape) - 1 - dim))
    return loudness


def normal_values(own_key, extent, deviation, most, shards=(), kind=jnp.bfloat16):
    entries = jax.random.normal(own_key, extent, jnp.float32) * deviation
    if len(shards) > 0:
        entries = levels(own_key, extent, shards, -0.22, 0.18) * entries
    return jnp.clip(entries, min=-most, max=most).astype(kind)


def setup_inputs(seed: int = 0) -> dict:
    streams_of = jax.random.split(jax.random.key(seed), 16)
    imagery = normal_values(streams_of[0], (HEIGHT, WIDTH, C), 1.0, 6.0, ((0, 8), (1, 16)))
    cotangent = normal_values(streams_of[1], (HEIGHT, WIDTH, C), 1.0, 6.0, ((0, 8), (1, 16)))
    norm_gain = jnp.clip(1.0 + 0.1 * jax.random.normal(streams_of[2], (2, C), jnp.float32), 0.5, 1.5)
    norm_bias = normal_values(streams_of[3], (2, C), 0.5, 3.0, (), jnp.float32)
    qkv_weight = normal_values(streams_of[4], (2, C, 3 * C), C ** -0.5, 0.4375)
    qkv_bias = normal_values(streams_of[5], (2, 3 * C), 0.5, 3.0, (), jnp.float32)
    rel_table = draw_rel_table(jax.random.fold_in(streams_of[15], 71), 0)
    proj_weight = normal_values(streams_of[7], (2, C, C), C ** -0.5, 0.4375)
    proj_bias = normal_values(streams_of[8], (2, C), 0.5, 3.0, (), jnp.float32)
    mlp_gain = jnp.clip(1.0 + 0.1 * jax.random.normal(streams_of[9], (2, C), jnp.float32), 0.5, 1.5)
    mlp_bias = normal_values(streams_of[10], (2, C), 0.5, 3.0, (), jnp.float32)
    up_weight = normal_values(streams_of[11], (2, C, MLP), C ** -0.5, 0.4375)
    up_bias = normal_values(streams_of[12], (2, MLP), 0.5, 3.0, (), jnp.float32)
    down_weight = normal_values(streams_of[13], (2, MLP, C), MLP ** -0.5, 0.21875)
    down_bias = normal_values(streams_of[14], (2, C), 0.5, 3.0, (), jnp.float32)
    return dict(imagery=imagery, cotangent=cotangent, norm_gain=norm_gain, norm_bias=norm_bias, qkv_weight=qkv_weight, qkv_bias=qkv_bias, rel_table=rel_table, proj_weight=proj_weight, proj_bias=proj_bias, mlp_gain=mlp_gain, mlp_bias=mlp_bias, up_weight=up_weight, up_bias=up_bias, down_weight=down_weight, down_bias=down_bias)


EPSILON = 1e-05

def norm_rows(values, norm_scale, norm_shift):
    widened = values.astype(jnp.float32)
    center = widened - lax.optimization_barrier(jnp.mean(widened, axis=-1, keepdims=True))
    spread = lax.optimization_barrier(jnp.mean(center * center, axis=-1, keepdims=True))
    return (center * lax.rsqrt(spread + EPSILON) * norm_scale + norm_shift).astype(jnp.bfloat16)

def offset_table(window):
    cells = np.arange(window * window)
    row_of = cells // window
    col_of = cells % window
    offsets = (row_of[:, None] - row_of[None, :] + window - 1) * (2 * window - 1) + (col_of[:, None] - col_of[None, :] + window - 1)
    return (offsets.reshape(-1)[:, None] == np.arange((2 * window - 1) ** 2)[None, :]).astype(np.float32)

def to_windows(values, window):
    height, breadth, features = values.shape
    blocked = values.reshape(height // window, window, breadth // window, window, features)
    return blocked.transpose(0, 2, 1, 3, 4).reshape(-1, window * window, features)

def from_windows(values, height, breadth, window):
    features = values.shape[-1]
    blocked = values.reshape(height // window, breadth // window, window, window, features)
    return blocked.transpose(0, 2, 1, 3, 4).reshape(height, breadth, features)

def swin_block(inputs, params, row_start, col_start, total_rows, total_cols, masked):
    norm_gain, norm_bias, qkv_weight, qkv_bias, rel_table, proj_weight, proj_bias, mlp_gain, mlp_bias, up_weight, up_bias, down_weight, down_bias = params
    height, breadth, channels = inputs.shape
    head_count = rel_table.shape[0]
    head_size = channels // head_count
    window = WIN
    normed = norm_rows(inputs, norm_gain, norm_bias).reshape(height * breadth, channels)
    packed = (jnp.dot(normed, qkv_weight, preferred_element_type=jnp.float32) + qkv_bias).astype(jnp.bfloat16)
    grouped = to_windows(packed.reshape(height, breadth, 3 * channels), window)
    grouped = grouped.reshape(grouped.shape[0], window * window, 3, head_count, head_size)
    queries = grouped[:, :, 0]
    keys_win = grouped[:, :, 1]
    values_win = grouped[:, :, 2]
    scores = jnp.einsum('nqhd,nkhd->nhqk', queries, keys_win, preferred_element_type=jnp.float32) * head_size ** (-0.5)
    position = jnp.dot(rel_table, jnp.asarray(offset_table(window)).T, precision=lax.Precision.HIGHEST)
    scores = scores + position.reshape(head_count, window * window, window * window)[None]
    if masked:
        row_ids = row_start + jnp.arange(height, dtype=jnp.int32)
        col_ids = col_start + jnp.arange(breadth, dtype=jnp.int32)
        row_zone = (row_ids >= total_rows - window).astype(jnp.int32) + (row_ids >= total_rows - window // 2).astype(jnp.int32)
        col_zone = (col_ids >= total_cols - window).astype(jnp.int32) + (col_ids >= total_cols - window // 2).astype(jnp.int32)
        zones = (row_zone[:, None] * 3 + col_zone[None, :])[:, :, None]
        zones = to_windows(zones, window)[:, :, 0]
        same_zone = zones[:, :, None] == zones[:, None, :]
        scores = jnp.where(same_zone[:, None], scores, -1e+30)
    row_max = lax.stop_gradient(lax.optimization_barrier(jnp.max(scores, axis=-1, keepdims=True)))
    powers = jnp.exp(scores - row_max)
    attention = (powers / lax.optimization_barrier(jnp.sum(powers, axis=-1, keepdims=True))).astype(jnp.bfloat16)
    mixed_out = jnp.einsum('nhqk,nkhd->nqhd', attention, values_win, preferred_element_type=jnp.float32).astype(jnp.bfloat16)
    mixed_out = from_windows(mixed_out.reshape(mixed_out.shape[0], window * window, channels), height, breadth, window)
    attended = jnp.dot(mixed_out.reshape(height * breadth, channels), proj_weight, preferred_element_type=jnp.float32) + proj_bias
    middle = (inputs.astype(jnp.float32) + attended.reshape(height, breadth, channels)).astype(jnp.bfloat16)
    normed_mid = norm_rows(middle, mlp_gain, mlp_bias).reshape(height * breadth, channels)
    hidden = jax.nn.gelu(jnp.dot(normed_mid, up_weight, preferred_element_type=jnp.float32) + up_bias, approximate=False).astype(jnp.bfloat16)
    output = middle.astype(jnp.float32) + (jnp.dot(hidden, down_weight, preferred_element_type=jnp.float32) + down_bias).reshape(height, breadth, channels)
    return output.astype(jnp.bfloat16)

def reference(imagery, cotangent, norm_gain, norm_bias, qkv_weight, qkv_bias, rel_table, proj_weight, proj_bias, mlp_gain, mlp_bias, up_weight, up_bias, down_weight, down_bias):
    params = (norm_gain, norm_bias, qkv_weight, qkv_bias, rel_table, proj_weight, proj_bias, mlp_gain, mlp_bias, up_weight, up_bias, down_weight, down_bias)
    first = tuple((member[0] for member in params))
    second = tuple((member[1] for member in params))
    height = TILE * N_ROWS
    breadth = TILE * N_COLS
    tile_count = N_ROWS * N_COLS
    half_window = WIN // 2

    def to_tiles(values):
        return values.reshape(N_ROWS, TILE, N_COLS, TILE, C).transpose(0, 2, 1, 3, 4).reshape(tile_count, TILE, TILE, C)

    def from_tiles(values):
        return values.reshape(N_ROWS, N_COLS, TILE, TILE, C).transpose(0, 2, 1, 3, 4).reshape(height, breadth, C)
    row_starts = jnp.arange(tile_count, dtype=jnp.int32) // N_COLS * TILE
    col_starts = jnp.arange(tile_count, dtype=jnp.int32) % N_COLS * TILE
    image_tiles = to_tiles(imagery)
    level_one = from_tiles(lax.map(lambda member: swin_block(member, first, 0, 0, height, breadth, False), image_tiles))
    moved = to_tiles(jnp.roll(level_one, (-half_window, -half_window), (0, 1)))
    moved_back = to_tiles(jnp.roll(cotangent, (-half_window, -half_window), (0, 1)))

    def second_step(totals, items):
        inputs, grad_in, row_at, col_at = items

        def local(values, weights):
            return swin_block(values, weights, row_at, col_at, height, breadth, True)
        result, pull = jax.vjp(local, inputs, second)
        grad_values, grad_weights = pull(grad_in)
        totals = tuple((total + member.astype(jnp.float32) for total, member in zip(totals, grad_weights)))
        return (totals, (result, grad_values))
    zero_two = tuple((jnp.zeros(member.shape, jnp.float32) for member in second))
    grads_two, (level_two, back_two) = lax.scan(second_step, zero_two, (moved, moved_back, row_starts, col_starts))
    output = jnp.roll(from_tiles(level_two), (half_window, half_window), (0, 1))
    back_in = to_tiles(jnp.roll(from_tiles(back_two), (half_window, half_window), (0, 1)))

    def first_step(totals, items):
        inputs, grad_in = items

        def local(values, weights):
            return swin_block(values, weights, 0, 0, height, breadth, False)
        result, pull = jax.vjp(local, inputs, first)
        grad_values, grad_weights = pull(grad_in)
        totals = tuple((total + member.astype(jnp.float32) for total, member in zip(totals, grad_weights)))
        return (totals, grad_values)
    zero_one = tuple((jnp.zeros(member.shape, jnp.float32) for member in first))
    grads_one, back_one = lax.scan(first_step, zero_one, (image_tiles, back_in))
    imagery_grad = from_tiles(back_one)
    factor = float(height * breadth) ** (-0.5)
    grads = [jnp.stack([lower, upper]) * factor for lower, upper in zip(grads_one, grads_two)]
    return (output, imagery_grad, grads[0], grads[1], grads[2], grads[3], grads[4], grads[5], grads[6], grads[7], grads[8], grads[9], grads[10], grads[11], grads[12])
```

```python
import jax
import jax.numpy as jnp
from jax import lax
from jax.experimental import pallas as pl
from jax.experimental.pallas import tpu as pltpu
from jax.sharding import PartitionSpec as P

F32 = jnp.float32
BF16 = jnp.bfloat16
C = 192
HEADS = 6
DIM = 32
MLP = 768
TILE = 16
TOK = TILE * TILE
SPAN = 15
SCALE = DIM**-0.5
EPSILON = 1e-05
FLAT = 4096
SMALL = 3456
MASKED = -1e30


def dot_tn(a, b):
    return lax.dot_general(a, b, (((0,), (0,)), ((), ())), preferred_element_type=F32)


def dot_nn(a, b):
    return lax.dot_general(a, b, (((1,), (0,)), ((), ())), preferred_element_type=F32)


def dot_nt(a, b):
    return lax.dot_general(a, b, (((1,), (1,)), ((), ())), preferred_element_type=F32)


def iota(shape, dim):
    return lax.broadcasted_iota(jnp.int32, shape, dim)


def split3(value):
    high = value.astype(BF16)
    rest = value - high.astype(F32)
    mid = rest.astype(BF16)
    return high, mid, (rest - mid.astype(F32)).astype(BF16)


def window_row(r, wc):
    return ((r // 8) * 2 + wc) * 64 + (r % 8) * 8


def halves():
    return iota((64, 128), 1) < 64


def stack_windows(value, left):
    zero = jnp.zeros_like(value)
    return jnp.concatenate([jnp.where(left, value, zero), jnp.where(left, zero, value)], axis=0).astype(BF16)


def own_window(full, left):
    return jnp.where(left, full[:64], full[64:])


def norm_fwd(x):
    center = x - jnp.mean(x, axis=0, keepdims=True)
    rstd = lax.rsqrt(jnp.mean(center * center, axis=0, keepdims=True) + EPSILON)
    return center * rstd, rstd


def norm_bwd(dn, xhat, rstd, gain):
    dxh = dn * gain
    along = jnp.mean(dxh * xhat, axis=0, keepdims=True)
    return rstd * (dxh - jnp.mean(dxh, axis=0, keepdims=True) - xhat * along)


def spread(lane_q):
    q = lane_q % 64
    return (q // 8) * SPAN + q % 8


VEC_NAMES = ("ng", "nb", "pb", "mg", "mb", "db", "qb", "ub")


def load_columns(vec, par):
    for i, name in enumerate(VEC_NAMES):
        n = par[name].shape[-1]
        vec[i : i + 1, 0:n] = par[name][0]
    return vec[...].T


def position_bias(par, table, bias):
    table[...] = jnp.zeros((8, 256), F32)
    table[0:HEADS, 0 : SPAN * SPAN] = par["rel"][0]
    select = (iota((128, 128), 0) == spread(iota((128, 128), 1))).astype(BF16)
    for h in range(HEADS):
        row = jnp.broadcast_to(table[h : h + 1, :], (8, 256))
        rows = []
        for ky in range(8):
            shift = (249 - SPAN * (7 - ky)) % 256
            rows.append(pltpu.roll(row, shift, 1, stride=1, stride_axis=0)[:, 0:128])
        high, mid, low = split3(jnp.concatenate(rows, axis=0))
        bias[h] = dot_nn(high, select) + (dot_nn(mid, select) + dot_nn(low, select))


def same_zone(p, last_row, last_col):
    k = iota((64, 128), 0)
    lane = iota((64, 128), 1)
    q = lane % 64
    rows = ((q // 8) < 4) == ((k // 8) < 4)
    cols = ((q % 8) < 4) == ((k % 8) < 4)
    keep = jnp.logical_or(cols, jnp.logical_or(lane < 64, jnp.logical_not(last_col)))
    if p == 1:
        keep = jnp.logical_and(keep, jnp.logical_or(rows, jnp.logical_not(last_row)))
    return keep


def forward(x, par, cols, bias, res, zones):
    left = halves()
    xhat, _ = norm_fwd(x)
    normed = (xhat * cols[0:C, 0:1] + cols[0:C, 1:2]).astype(BF16)
    res["packed"][...] = (dot_tn(par["qw"][0], normed) + cols[0:576, 6:7]).astype(BF16)
    for p in range(2):
        lanes = slice(128 * p, 128 * p + 128)
        for h in range(HEADS):
            q = res["packed"][DIM * h : DIM * h + DIM, lanes]
            k = res["packed"][C + DIM * h : C + DIM * h + DIM, lanes]
            v = res["packed"][2 * C + DIM * h : 2 * C + DIM * h + DIM, lanes]
            s = own_window(dot_tn(k, q), left) * SCALE + bias[h]
            if zones is not None:
                s = jnp.where(zones[p], s, MASKED)
            e = jnp.exp(s - jnp.max(s, axis=0, keepdims=True))
            a = e * (1.0 / jnp.sum(e, axis=0, keepdims=True))
            res["attn"][p * HEADS + h] = a.astype(BF16)
            res["mixed"][DIM * h : DIM * h + DIM, lanes] = dot_nn(v, stack_windows(a, left)).astype(BF16)
    middle = x + dot_tn(par["pw"][0], res["mixed"][...]) + cols[0:C, 2:3]
    res["middle"][...] = middle.astype(BF16)
    middle = res["middle"][...].astype(F32)
    xhat, _ = norm_fwd(middle)
    normed = (xhat * cols[0:C, 3:4] + cols[0:C, 4:5]).astype(BF16)
    for i in range(0, MLP, 128):
        u = dot_tn(par["uw"][0, :, i : i + 128], normed) + cols[i : i + 128, 7:8]
        half = 0.5 + 0.5 * lax.erf(u * (0.5**0.5))
        res["hidden"][i : i + 128, :] = (u * half).astype(BF16)
        res["slope"][i : i + 128, :] = (half + u * (jnp.exp(-0.5 * u * u) * 0.3989422804014327)).astype(BF16)
    out = middle + dot_tn(par["dw"][0], res["hidden"][...]) + cols[0:C, 5:6]
    return out.astype(BF16)


def put_row(small, at, row):
    n = row.shape[-1]
    for i in range(0, n, 128):
        w = min(128, n - i)
        small[at + i // 128 : at + i // 128 + 1, 0:w] = row[0:1, i : i + w]


def backward(dout, x, par, cols, res, flat, small, du_ref, dpacked, rel_sum):
    left = halves()
    ones = jnp.ones((8, TOK), BF16)
    none = jnp.zeros((64, TOK), BF16)
    small[...] = jnp.zeros(small.shape, F32)
    middle = res["middle"][...].astype(F32)
    xhat, rstd = norm_fwd(middle)
    normed = (xhat * cols[0:C, 3:4] + cols[0:C, 4:5]).astype(BF16)
    flat[2304:3072, :] = dot_nt(res["hidden"][...], dout[0:128]).astype(BF16)
    tail = dot_nt(res["hidden"][0:384, :], jnp.concatenate([dout[128:192], none], axis=0))
    tail = tail + dot_nt(res["hidden"][384:768, :], jnp.concatenate([none, dout[128:192]], axis=0))
    flat[3072:3456, :] = tail.astype(BF16)
    put_row(small, 21, dot_nt(ones, dout))
    for i in range(0, MLP, 128):
        dh = dot_nn(par["dw"][0, i : i + 128, :], dout).astype(BF16).astype(F32)
        du = (dh * res["slope"][i : i + 128, :].astype(F32)).astype(BF16)
        du_ref[i : i + 128, :] = du
        flat[1152 + C * (i // 128) : 1152 + C * (i // 128) + C, :] = dot_nt(normed, du).astype(BF16)
    put_row(small, 15, dot_nt(ones, du_ref[...]))
    dn = dot_nn(par["uw"][0], du_ref[...]).astype(BF16)
    put_row(small, 13, dot_nt(ones, dn))
    dn = dn.astype(F32)
    put_row(small, 11, dot_nt(ones, (dn * xhat).astype(BF16)))
    dmid = (dout.astype(F32) + norm_bwd(dn, xhat, rstd, cols[0:C, 3:4])).astype(BF16)
    put_row(small, 9, dot_nt(ones, dmid))
    flat[960:1152, :] = dot_nt(res["mixed"][...], dmid[0:128]).astype(BF16)
    dmixed = dot_nn(par["pw"][0], dmid).astype(BF16)
    for h in range(HEADS):
        drel = None
        for p in range(2):
            lanes = slice(128 * p, 128 * p + 128)
            q = res["packed"][DIM * h : DIM * h + DIM, lanes]
            k = res["packed"][C + DIM * h : C + DIM * h + DIM, lanes]
            v = res["packed"][2 * C + DIM * h : 2 * C + DIM * h + DIM, lanes]
            a = res["attn"][p * HEADS + h].astype(F32)
            dm = dmixed[DIM * h : DIM * h + DIM, lanes]
            da = own_window(dot_tn(v, dm), left).astype(BF16).astype(F32)
            ds = a * (da - jnp.sum(da * a, axis=0, keepdims=True))
            drel = ds if drel is None else drel + ds
            wide = stack_windows(ds * SCALE, left)
            dpacked[DIM * h : DIM * h + DIM, lanes] = dot_nn(k, wide).astype(BF16)
            dpacked[C + DIM * h : C + DIM * h + DIM, lanes] = dot_nt(q, wide).astype(BF16)
            dpacked[2 * C + DIM * h : 2 * C + DIM * h + DIM, lanes] = dot_nt(dm, stack_windows(a, left)).astype(BF16)
        rel_sum[h] = drel
    mirror = ((127 - iota((128, 128), 0)) == spread(iota((128, 128), 1))).astype(BF16)
    for h in range(HEADS):
        high, mid, _ = split3(rel_sum[h])
        back = dot_nt(high, mirror) + dot_nt(mid, mirror)
        total = jnp.zeros((8, 256), F32)
        for ky in range(8):
            wide = jnp.concatenate([back[8 * ky : 8 * ky + 8], jnp.zeros((8, 128), F32)], axis=1)
            total = total + pltpu.roll(wide, 121 - SPAN * (7 - ky), 1, stride=1, stride_axis=0)
        total = jnp.sum(total, axis=0, keepdims=True)
        small[24 + h : 25 + h, :] = total[:, 0:128]
        small[32 + h : 33 + h, :] = total[:, 128:256]
    xhat, rstd = norm_fwd(x)
    normed = (xhat * cols[0:C, 0:1] + cols[0:C, 1:2]).astype(BF16)
    for j in range(4):
        flat[C * j : C * j + C, :] = dot_nt(normed, dpacked[128 * j : 128 * j + 128, :]).astype(BF16)
    tail = dot_nt(normed, jnp.concatenate([dpacked[512:576, :], none], axis=0))
    tail = tail + dot_nt(res["mixed"][...], jnp.concatenate([none, dmid[128:192]], axis=0))
    flat[768:960, :] = tail.astype(BF16)
    put_row(small, 4, dot_nt(ones, dpacked[...]))
    dn = dot_nn(par["qw"][0], dpacked[...]).astype(BF16)
    put_row(small, 2, dot_nt(ones, dn))
    dn = dn.astype(F32)
    put_row(small, 0, dot_nt(ones, (dn * xhat).astype(BF16)))
    flat[SMALL : SMALL + 48, :] = small[...].astype(BF16)
    flat[SMALL + 48 : FLAT, :] = jnp.zeros((FLAT - SMALL - 48, 128), BF16)
    return dmid.astype(F32) + norm_bwd(dn, xhat, rstd, cols[0:C, 0:1])


def to_channels(pieces):
    return jnp.concatenate(pieces, axis=0).T[0:C]


def to_tokens(value):
    return jnp.concatenate([value, jnp.zeros((64, TOK), F32)], axis=0).T


def grid_put(grid, tokens):
    for r in range(TILE):
        for wc in range(2):
            at = window_row(r, wc)
            grid[r, 8 * wc : 8 * wc + 8, :] = tokens[at : at + 8]


def grid_get(grid, row_at, col_at):
    pieces = []
    for wr in range(2):
        for wc in range(2):
            for ir in range(8):
                at = col_at + 8 * wc
                pieces.append(grid[row_at + 8 * wr + ir, at : at + 8, :])
    return pieces


def emit_strips(grid, edge, strips, which, row_at, col_at):
    col_out, row_out, corner_out = strips
    for r in range(TILE):
        edge[4 * r : 4 * r + 4, :] = grid[r, col_at : col_at + 4, :]
    col_out[64 * which : 64 * which + 64, :] = edge[:, 0:C].astype(BF16)
    for r in range(4):
        row_out[64 * which + 16 * r : 64 * which + 16 * r + 16, :] = grid[row_at + r, 0:TILE, 0:C].astype(BF16)
    for r in range(4):
        edge[4 * r : 4 * r + 4, :] = grid[row_at + r, col_at : col_at + 4, :]
    corner_out[16 * which : 16 * which + 16, :] = edge[0:16, 0:C].astype(BF16)


def fill_grid(grid, edge, own, strips, which, own_row, own_col, strip_row, strip_col):
    col_in, row_in, corner_in = strips
    for r in range(TILE):
        grid[own_row + r, own_col : own_col + TILE, 0:C] = own[r].astype(F32)
    edge[:, 0:C] = col_in[64 * which : 64 * which + 64, :].astype(F32)
    for r in range(TILE):
        grid[own_row + r, strip_col : strip_col + 4, :] = edge[4 * r : 4 * r + 4, :]
    for r in range(4):
        at = 64 * which + 16 * r
        grid[strip_row + r, own_col : own_col + TILE, 0:C] = row_in[at : at + 16, :].astype(F32)
    edge[0:16, 0:C] = corner_in[16 * which : 16 * which + 16, :].astype(F32)
    for r in range(4):
        grid[strip_row + r, strip_col : strip_col + 4, :] = edge[4 * r : 4 * r + 4, :]


PAR_NAMES = ("ng", "nb", "qw", "qb", "rel", "pw", "pb", "mg", "mb", "uw", "ub", "dw", "db")
RES_NAMES = ("packed", "attn", "mixed", "middle", "hidden", "slope")
RES_SHAPES = ((576, TOK), (12, 64, 128), (C, TOK), (C, TOK), (MLP, TOK), (MLP, TOK))


def first_forward(*refs):
    imagery, cotangent = refs[0:2]
    par = dict(zip(PAR_NAMES, refs[2:15]))
    own, xt = refs[15:17]
    strips = refs[17:20]
    res = dict(zip(RES_NAMES, refs[20:26]))
    grid, edge, vec, table, bias = refs[26:]
    cols = load_columns(vec, par)
    position_bias(par, table, bias)
    for r in range(TILE):
        grid[r, 0:TILE, 0:C] = cotangent[r].astype(F32)
    emit_strips(grid, edge, strips, 1, 0, 0)
    for r in range(TILE):
        grid[r, 0:TILE, 0:C] = imagery[r].astype(F32)
    x = to_channels(grid_get(grid, 0, 0))
    xt[...] = x.astype(BF16)
    out = forward(x, par, cols, bias, res, None)
    grid_put(grid, to_tokens(out.astype(F32)))
    for r in range(TILE):
        own[r] = grid[r, 0:TILE, 0:C].astype(BF16)
    emit_strips(grid, edge, strips, 0, 0, 0)


def second_block(*refs):
    own_in, cotangent = refs[0:2]
    strips_in = refs[2:5]
    par = dict(zip(PAR_NAMES, refs[5:18]))
    out_own, back_own = refs[18:20]
    strips = refs[20:23]
    flat = refs[23]
    grid, edge, vec, table, bias = refs[24:29]
    small, du_ref, dpacked, rel_sum = refs[29:33]
    res = dict(zip(RES_NAMES, refs[33:39]))
    cols = load_columns(vec, par)
    position_bias(par, table, bias)
    last_row = lax.axis_index("rows") == lax.axis_size("rows") - 1
    last_col = lax.axis_index("cols") == lax.axis_size("cols") - 1
    zones = [same_zone(p, last_row, last_col) for p in range(2)]
    fill_grid(grid, edge, own_in, strips_in, 0, 0, 0, 16, 16)
    x = to_channels(grid_get(grid, 4, 4))
    fill_grid(grid, edge, cotangent, strips_in, 1, 0, 0, 16, 16)
    dout = to_channels(grid_get(grid, 4, 4)).astype(BF16)
    out = forward(x, par, cols, bias, res, zones)
    grid_put(grid, to_tokens(out.astype(F32)))
    for r in range(TILE):
        out_own[r] = grid[r, 0:TILE, 0:C].astype(BF16)
    emit_strips(grid, edge, strips, 0, 12, 12)
    dx = backward(dout, x, par, cols, res, flat, small, du_ref, dpacked, rel_sum)
    grid_put(grid, to_tokens(dx))
    for r in range(TILE):
        back_own[r] = grid[r, 0:TILE, 0:C].astype(BF16)
    emit_strips(grid, edge, strips, 1, 12, 12)


def first_backward(*refs):
    out_in, back_in = refs[0:2]
    strips_in = refs[2:5]
    par = dict(zip(PAR_NAMES, refs[5:18]))
    xt = refs[18]
    res = dict(zip(RES_NAMES, refs[19:25]))
    output, grad, flat = refs[25:28]
    grid, edge, vec = refs[28:31]
    small, du_ref, dpacked, rel_sum = refs[31:35]
    cols = load_columns(vec, par)
    fill_grid(grid, edge, out_in, strips_in, 0, 4, 8, 0, 4)
    for r in range(TILE):
        output[r] = grid[r, 4:20, 0:C].astype(BF16)
    fill_grid(grid, edge, back_in, strips_in, 1, 4, 8, 0, 4)
    dout = to_channels(grid_get(grid, 0, 4)).astype(BF16)
    x = xt[...].astype(F32)
    dx = backward(dout, x, par, cols, res, flat, small, du_ref, dpacked, rel_sum)
    grid_put(grid, to_tokens(dx))
    for r in range(TILE):
        grad[r] = grid[r, 0:TILE, 0:C].astype(BF16)


def sum_spread(parts, out):
    n, rows, _ = parts.shape
    total = jnp.zeros((rows, 128), F32)
    for i in range(n):
        total = total + parts[i].astype(F32)
    total = total.astype(BF16)
    for i in range(n):
        out[i] = total


def unpack(one, two, *outs):
    ng, nb, qw, qb, rel, pw, pb, mg, mb, uw, ub, dw, db, small = outs
    factor = outs_factor
    flip = (iota((256, 256), 0) + iota((256, 256), 1) == 255).astype(BF16)
    for b, flat in enumerate((one, two)):

        def rows(at, n):
            return flat[at : at + n, :].astype(F32) * factor

        for j in range(4):
            qw[b, :, 128 * j : 128 * j + 128] = rows(C * j, C)
        tail = rows(768, C)
        qw[b, :, 512:576] = tail[:, 0:64]
        pw[b, :, 128:192] = pltpu.roll(tail, 64, 1)[:, 0:64]
        pw[b, :, 0:128] = rows(960, C)
        for j in range(6):
            uw[b, :, 128 * j : 128 * j + 128] = rows(1152 + C * j, C)
        dw[b, :, 0:128] = rows(2304, MLP)
        tail = rows(3072, 384)
        dw[b, 0:384, 128:192] = tail[:, 0:64]
        dw[b, 384:768, 128:192] = pltpu.roll(tail, 64, 1)[:, 0:64]
        small[...] = rows(SMALL, 48)
        for at, ref in ((0, ng), (2, nb), (4, qb), (9, pb), (11, mg), (13, mb), (15, ub), (21, db)):
            n = ref.shape[-1]
            for i in range(0, n, 128):
                w = min(128, n - i)
                ref[b : b + 1, i : i + w] = small[at + i // 128 : at + i // 128 + 1, 0:w]
        table = jnp.concatenate([flat[SMALL + 24 : SMALL + 32, :], flat[SMALL + 32 : SMALL + 40, :]], axis=1)
        rel[b] = (dot_nn(table, flip) * factor)[0:HEADS, 0 : SPAN * SPAN]


outs_factor = float(128 * 256) ** (-0.5)


def whole(shape):
    zeros = (0,) * len(shape)
    return pl.BlockSpec(shape, lambda *_: zeros)


def block_of(array, b):
    if array.ndim == 2:
        array = array.reshape(2, 1, array.shape[-1])
    tail = (0,) * (array.ndim - 1)
    return array, pl.BlockSpec((1,) + array.shape[1:], lambda *_: (b,) + tail)


def call(kernel, name, args, params, b, more, outs, scratch, flops):
    specs = [whole(a.shape) for a in args]
    values = list(args)
    for p in params:
        value, spec = block_of(p, b)
        values.append(value)
        specs.append(spec)
    for a in more:
        values.append(a)
        specs.append(whole(a.shape))
    return pl.pallas_call(
        kernel,
        grid=(1,),
        in_specs=specs,
        out_specs=[whole(o.shape) for o in outs],
        out_shape=outs,
        scratch_shapes=scratch,
        name=name,
        cost_estimate=pl.CostEstimate(flops=flops, transcendentals=0, bytes_accessed=4000000),
    )(*values)


def shaped(shape, dtype=BF16):
    return jax.ShapeDtypeStruct(shape, dtype)


def exchange(strips, step):
    n_rows = lax.axis_size("rows")
    n_cols = lax.axis_size("cols")
    col_strip, row_strip, corner = strips
    along = [(c, (c + step) % n_cols) for c in range(n_cols)]
    down = [(r, (r + step) % n_rows) for r in range(n_rows)]
    both = [
        (r * n_cols + c, ((r + step) % n_rows) * n_cols + (c + step) % n_cols)
        for r in range(n_rows)
        for c in range(n_cols)
    ]
    return [
        lax.ppermute(col_strip, "cols", along),
        lax.ppermute(row_strip, "rows", down),
        lax.ppermute(corner, ("rows", "cols"), both),
    ]


def reduce_flat(flat):
    axes = ("rows", "cols")
    n = lax.axis_size("rows") * lax.axis_size("cols")
    parts = lax.all_to_all(flat.reshape(n, FLAT // n, 128), axes, 0, 0, tiled=True)
    spread_out = pl.pallas_call(sum_spread, out_shape=shaped(parts.shape), name="sum_spread")(parts)
    return lax.all_to_all(spread_out, axes, 0, 0, tiled=True).reshape(FLAT, 128)


def per_device(imagery, cotangent, *params):
    tile = (TILE, TILE, C)
    strips = [shaped((128, C)), shaped((128, C)), shaped((32, C))]
    residuals = [shaped(s) for s in RES_SHAPES]
    grid = pltpu.VMEM((24, 24, 256), F32)
    edge = pltpu.VMEM((64, 256), F32)
    vec = pltpu.VMEM((128, MLP), F32)
    tables = [pltpu.VMEM((8, 256), F32), pltpu.VMEM((HEADS, 64, 128), F32)]
    work = [
        pltpu.VMEM((48, 128), F32),
        pltpu.VMEM((MLP, TOK), BF16),
        pltpu.VMEM((576, TOK), BF16),
        pltpu.VMEM((HEADS, 64, 128), F32),
    ]
    one = call(
        first_forward,
        "first_forward",
        (imagery, cotangent),
        params,
        0,
        (),
        [shaped(tile), shaped((C, TOK))] + strips + residuals,
        [grid, edge, vec] + tables,
        5 * 10**9,
    )
    own, xt, res = one[0], one[1], one[5:]
    got = exchange(one[2:5], -1)
    two = call(
        second_block,
        "second_block",
        (own, cotangent, *got),
        params,
        1,
        (),
        [shaped(tile), shaped(tile)] + strips + [shaped((FLAT, 128))],
        [grid, edge, vec] + tables + work + [pltpu.VMEM(s, BF16) for s in RES_SHAPES],
        10**10,
    )
    got = exchange(two[2:5], 1)
    output, grad, flat_one = call(
        first_backward,
        "first_backward",
        (two[0], two[1], *got),
        params,
        0,
        (xt, *res),
        [shaped(tile), shaped(tile), shaped((FLAT, 128))],
        [grid, edge, vec] + work,
        5 * 10**9,
    )
    sum_two = reduce_flat(two[5])
    sum_one = reduce_flat(flat_one)
    grads = pl.pallas_call(
        unpack,
        out_shape=[shaped(p.shape, F32) for p in params],
        scratch_shapes=[pltpu.VMEM((48, 128), F32)],
        name="unpack",
    )(sum_one, sum_two)
    return (output, grad, *grads)


def solution(mesh):
    tile = P("rows", "cols", None)
    return jax.shard_map(
        per_device,
        mesh=mesh,
        in_specs=(tile, tile) + (P(),) * 13,
        out_specs=(tile, tile) + (P(),) * 13,
        check_vma=False,
    )
```

```python
import functools

import jax
import jax.numpy as jnp
from jax import lax
from jax.experimental import pallas as pl
from jax.experimental.pallas import tpu as pltpu
from jax.sharding import PartitionSpec as P


F32 = jnp.float32
BF16 = jnp.bfloat16
C = 192
HEADS = 6
DIM = 32
MLP = 768
TILE = 16
TOK = TILE * TILE
SPAN = 15
SCALE = DIM**-0.5
EPSILON = 1e-05
FLAT = 3584
SMALL = 3456
MASKED = -1e30


def dot_tn(a, b):
    return lax.dot_general(a, b, (((0,), (0,)), ((), ())), preferred_element_type=F32)


def dot_nn(a, b):
    return lax.dot_general(a, b, (((1,), (0,)), ((), ())), preferred_element_type=F32)


def dot_nt(a, b):
    return lax.dot_general(a, b, (((1,), (1,)), ((), ())), preferred_element_type=F32)


def iota(shape, dim):
    return lax.broadcasted_iota(jnp.int32, shape, dim)


def split3(value):
    high = value.astype(BF16)
    rest = value - high.astype(F32)
    mid = rest.astype(BF16)
    return high, mid, (rest - mid.astype(F32)).astype(BF16)


def window_row(r, wc):
    return ((r // 8) * 2 + wc) * 64 + (r % 8) * 8


def halves():
    return iota((64, 128), 1) < 64


def stack_windows(value, left):
    zero = jnp.zeros_like(value)
    return jnp.concatenate([jnp.where(left, value, zero), jnp.where(left, zero, value)], axis=0).astype(BF16)


def own_window(full, left):
    return jnp.where(left, full[:64], full[64:])


def norm_fwd(x):
    center = x - jnp.mean(x, axis=0, keepdims=True)
    rstd = lax.rsqrt(jnp.mean(center * center, axis=0, keepdims=True) + EPSILON)
    return center * rstd, rstd


def norm_bwd(dn, xhat, rstd, gain):
    dxh = dn * gain
    along = jnp.mean(dxh * xhat, axis=0, keepdims=True)
    return rstd * (dxh - jnp.mean(dxh, axis=0, keepdims=True) - xhat * along)


def spread(lane_q):
    q = lane_q % 64
    return (q // 8) * SPAN + q % 8


VEC_NAMES = ("ng", "nb", "pb", "mg", "mb", "db", "qb", "ub")


def load_columns(vec, par, b):
    for i, name in enumerate(VEC_NAMES):
        n = par[name].shape[-1]
        vec[i : i + 1, 0:n] = par[name][b : b + 1, :]
    return vec[...].T


def position_bias(par, b, table, bias):
    table[...] = jnp.zeros((8, 256), F32)
    for h in range(HEADS):
        table[h : h + 1, 0 : SPAN * SPAN] = par["rel"][h, b : b + 1, :]
    select = (iota((128, 128), 0) == spread(iota((128, 128), 1))).astype(BF16)
    for h in range(HEADS):
        row = jnp.broadcast_to(table[h : h + 1, :], (8, 256))
        rows = []
        for ky in range(8):
            shift = (249 - SPAN * (7 - ky)) % 256
            rows.append(pltpu.roll(row, shift, 1, stride=1, stride_axis=0)[:, 0:128])
        high, mid, low = split3(jnp.concatenate(rows, axis=0))
        bias[h] = dot_nn(high, select) + (dot_nn(mid, select) + dot_nn(low, select))


def same_zone(p, last_row, last_col):
    k = iota((64, 128), 0)
    lane = iota((64, 128), 1)
    q = lane % 64
    rows = ((q // 8) < 4) == ((k // 8) < 4)
    cols = ((q % 8) < 4) == ((k % 8) < 4)
    keep = jnp.logical_or(cols, jnp.logical_or(lane < 64, jnp.logical_not(last_col)))
    if p == 1:
        keep = jnp.logical_and(keep, jnp.logical_or(rows, jnp.logical_not(last_row)))
    return keep


def forward(x, par, need, cols, bias, res, zones, keep):
    left = halves()
    xhat, _ = norm_fwd(x)
    normed = (xhat * cols[0:C, 0:1] + cols[0:C, 1:2]).astype(BF16)
    need("qw")
    res["packed"][...] = (dot_tn(par["qw"][...], normed) + cols[0:576, 6:7]).astype(BF16)
    for p in range(2):
        lanes = slice(128 * p, 128 * p + 128)
        for h in range(HEADS):
            q = res["packed"][DIM * h : DIM * h + DIM, lanes]
            k = res["packed"][C + DIM * h : C + DIM * h + DIM, lanes]
            v = res["packed"][2 * C + DIM * h : 2 * C + DIM * h + DIM, lanes]
            s = own_window(dot_tn(k, q), left) * SCALE + bias[h]
            if zones is not None:
                s = jnp.where(zones[p], s, MASKED)
            e = jnp.exp(s - jnp.max(s, axis=0, keepdims=True))
            a = e * (1.0 / jnp.sum(e, axis=0, keepdims=True))
            res["attn"][p * HEADS + h] = a.astype(BF16)
            res["mixed"][DIM * h : DIM * h + DIM, lanes] = dot_nn(v, stack_windows(a, left)).astype(BF16)
    keep("packed")
    need("pw")
    middle = x + dot_tn(par["pw"][...], res["mixed"][...]) + cols[0:C, 2:3]
    res["middle"][...] = middle.astype(BF16)
    middle = res["middle"][...].astype(F32)
    xhat, _ = norm_fwd(middle)
    normed = (xhat * cols[0:C, 3:4] + cols[0:C, 4:5]).astype(BF16)
    keep("attn", "mixed")
    need("uw")
    for i in range(0, MLP, 128):
        u = dot_tn(par["uw"][:, i : i + 128], normed) + cols[i : i + 128, 7:8]
        half = 0.5 + 0.5 * lax.erf(u * (0.5**0.5))
        res["hidden"][i : i + 128, :] = (u * half).astype(BF16)
        res["slope"][i : i + 128, :] = (half + u * (jnp.exp(-0.5 * u * u) * 0.3989422804014327)).astype(BF16)
    keep("middle")
    need("dw")
    out = middle + dot_nn(par["dw"][...], res["hidden"][...]) + cols[0:C, 5:6]
    return out.astype(BF16)


def put_row(small, at, row):
    n = row.shape[-1]
    for i in range(0, n, 128):
        w = min(128, n - i)
        small[at + i // 128 : at + i // 128 + 1, 0:w] = row[0:1, i : i + w]


def put_pairs(flat, at, lhs, rhs, n):
    for i in range(0, n, 256):
        wide = dot_nt(lhs, rhs[i : i + 256, :]).astype(BF16)
        for j in range(0, 256, 128):
            first = at + C * ((i + j) // 128)
            flat[first : first + C, :] = wide[:, j : j + 128]


def backward(dout, x, par, need, cols, res, flat, small, du_ref, dpacked, rel_sum):
    left = halves()
    ones = jnp.ones((8, TOK), BF16)
    none = jnp.zeros((64, TOK), BF16)
    small[...] = jnp.zeros(small.shape, F32)
    put_row(small, 21, dot_nt(ones, dout))
    need("dw", "slope")
    for i in range(0, MLP, 128):
        dh = dot_tn(par["dw"][:, i : i + 128], dout).astype(BF16).astype(F32)
        du = (dh * res["slope"][i : i + 128, :].astype(F32)).astype(BF16)
        du_ref[i : i + 128, :] = du
    need("middle", "uw")
    middle = res["middle"][...].astype(F32)
    xhat, rstd = norm_fwd(middle)
    normed = (xhat * cols[0:C, 3:4] + cols[0:C, 4:5]).astype(BF16)
    put_pairs(flat, 1152, normed, du_ref, MLP)
    need("hidden")
    put_pairs(flat, 2304, dout, res["hidden"], MLP)
    put_row(small, 15, dot_nt(ones, du_ref[...]))
    dn = dot_nn(par["uw"][...], du_ref[...]).astype(BF16)
    put_row(small, 13, dot_nt(ones, dn))
    dn = dn.astype(F32)
    put_row(small, 11, dot_nt(ones, (dn * xhat).astype(BF16)))
    dmid = (dout.astype(F32) + norm_bwd(dn, xhat, rstd, cols[0:C, 3:4])).astype(BF16)
    need("pw", "mixed")
    put_row(small, 9, dot_nt(ones, dmid))
    flat[960:1152, :] = dot_nt(res["mixed"][...], dmid[0:128]).astype(BF16)
    dmixed = dot_nn(par["pw"][...], dmid).astype(BF16)
    need("packed", "attn")
    for h in range(HEADS):
        drel = None
        for p in range(2):
            lanes = slice(128 * p, 128 * p + 128)
            q = res["packed"][DIM * h : DIM * h + DIM, lanes]
            k = res["packed"][C + DIM * h : C + DIM * h + DIM, lanes]
            v = res["packed"][2 * C + DIM * h : 2 * C + DIM * h + DIM, lanes]
            a = res["attn"][p * HEADS + h].astype(F32)
            dm = dmixed[DIM * h : DIM * h + DIM, lanes]
            da = own_window(dot_tn(v, dm), left).astype(BF16).astype(F32)
            ds = a * (da - jnp.sum(da * a, axis=0, keepdims=True))
            drel = ds if drel is None else drel + ds
            wide = stack_windows(ds * SCALE, left)
            dpacked[DIM * h : DIM * h + DIM, lanes] = dot_nn(k, wide).astype(BF16)
            dpacked[C + DIM * h : C + DIM * h + DIM, lanes] = dot_nt(q, wide).astype(BF16)
            dpacked[2 * C + DIM * h : 2 * C + DIM * h + DIM, lanes] = dot_nt(dm, stack_windows(a, left)).astype(BF16)
        rel_sum[h] = drel
    mirror = ((127 - iota((128, 128), 0)) == spread(iota((128, 128), 1))).astype(BF16)
    for h in range(HEADS):
        high, mid, _ = split3(rel_sum[h])
        back = dot_nt(high, mirror) + dot_nt(mid, mirror)
        total = jnp.zeros((8, 256), F32)
        for ky in range(8):
            wide = jnp.concatenate([back[8 * ky : 8 * ky + 8], jnp.zeros((8, 128), F32)], axis=1)
            total = total + pltpu.roll(wide, 121 - SPAN * (7 - ky), 1, stride=1, stride_axis=0)
        total = jnp.sum(total, axis=0, keepdims=True)
        small[24 + h : 25 + h, :] = total[:, 0:128]
        small[32 + h : 33 + h, :] = total[:, 128:256]
    xhat, rstd = norm_fwd(x)
    normed = (xhat * cols[0:C, 0:1] + cols[0:C, 1:2]).astype(BF16)
    put_pairs(flat, 0, normed, dpacked, 512)
    tail = dot_nt(normed, jnp.concatenate([dpacked[512:576, :], none], axis=0))
    tail = tail + dot_nt(res["mixed"][...], jnp.concatenate([none, dmid[128:192]], axis=0))
    flat[768:960, :] = tail.astype(BF16)
    put_row(small, 4, dot_nt(ones, dpacked[...]))
    need("qw")
    dn = dot_nn(par["qw"][...], dpacked[...]).astype(BF16)
    put_row(small, 2, dot_nt(ones, dn))
    dn = dn.astype(F32)
    put_row(small, 0, dot_nt(ones, (dn * xhat).astype(BF16)))
    flat[SMALL : SMALL + 48, :] = small[...].astype(BF16)
    flat[SMALL + 48 : FLAT, :] = jnp.zeros((FLAT - SMALL - 48, 128), BF16)
    return dmid.astype(F32) + norm_bwd(dn, xhat, rstd, cols[0:C, 0:1])


def to_channels(pieces):
    return jnp.concatenate(pieces, axis=0).T[0:C]


def to_tokens(value):
    return jnp.concatenate([value, jnp.zeros((64, TOK), F32)], axis=0).T


def grid_put(grid, tokens):
    for r in range(TILE):
        for wc in range(2):
            at = window_row(r, wc)
            grid[r, 8 * wc : 8 * wc + 8, :] = tokens[at : at + 8]


def grid_get(grid, row_at, col_at):
    pieces = []
    for wr in range(2):
        for wc in range(2):
            for ir in range(8):
                at = col_at + 8 * wc
                pieces.append(grid[row_at + 8 * wr + ir, at : at + 8, :])
    return pieces


def emit_strips(grid, edge, strips, which, row_at, col_at):
    col_out, row_out, corner_out = strips
    for r in range(TILE):
        edge[4 * r : 4 * r + 4, :] = grid[r, col_at : col_at + 4, :]
    col_out[64 * which : 64 * which + 64, :] = edge[:, 0:C].astype(BF16)
    for r in range(4):
        row_out[64 * which + 16 * r : 64 * which + 16 * r + 16, :] = grid[row_at + r, 0:TILE, 0:C].astype(BF16)
    for r in range(4):
        edge[4 * r : 4 * r + 4, :] = grid[row_at + r, col_at : col_at + 4, :]
    corner_out[16 * which : 16 * which + 16, :] = edge[0:16, 0:C].astype(BF16)


def fill_grid(grid, edge, own, strips, which, own_row, own_col, strip_row, strip_col):
    col_in, row_in, corner_in = strips
    for r in range(TILE):
        grid[own_row + r, own_col : own_col + TILE, 0:C] = own[r].astype(F32)
    edge[:, 0:C] = col_in[64 * which : 64 * which + 64, :].astype(F32)
    for r in range(TILE):
        grid[own_row + r, strip_col : strip_col + 4, :] = edge[4 * r : 4 * r + 4, :]
    for r in range(4):
        at = 64 * which + 16 * r
        grid[strip_row + r, own_col : own_col + TILE, 0:C] = row_in[at : at + 16, :].astype(F32)
    edge[0:16, 0:C] = corner_in[16 * which : 16 * which + 16, :].astype(F32)
    for r in range(4):
        grid[strip_row + r, strip_col : strip_col + 4, :] = edge[4 * r : 4 * r + 4, :]


PAR_NAMES = ("ng", "nb", "qw", "qb", "rel", "pw", "pb", "mg", "mb", "uw", "ub", "dw", "db")
RES_NAMES = ("packed", "attn", "mixed", "middle", "hidden", "slope")
RES_SHAPES = ((576, TOK), (12, 64, 128), (C, TOK), (C, TOK), (MLP, TOK), (MLP, TOK))


class Copies:
    def __init__(self, sems):
        self.sems = sems
        self.used = 0
        self.open = {}

    def start(self, name, source, target):
        self.open[name] = pltpu.make_async_copy(source, target, self.sems.at[self.used])
        self.open[name].start()
        self.used += 1

    def __call__(self, *names):
        for name in names:
            if name in self.open:
                self.open.pop(name).wait()

    def rest(self):
        self(*list(self.open))


def start_params(copies, names, far, par, b):
    for name in names:
        source = far[name].at[b] if name in WEIGHTS else far[name]
        copies.start(name, source, par[name])


WEIGHTS = ("qw", "pw", "uw", "dw")
PAR_SHAPES = dict(
    ng=(2, C), nb=(2, C), qw=(C, 3 * C), qb=(2, 3 * C), rel=(HEADS, 2, SPAN * SPAN), pw=(C, C), pb=(2, C),
    mg=(2, C), mb=(2, C), uw=(C, MLP), ub=(2, MLP), dw=(C, MLP), db=(2, C),
)


def nothing(*_):
    pass


def first_forward(*refs):
    imagery_far, cotangent_far = refs[0:2]
    far = dict(zip(PAR_NAMES, refs[2:15]))
    own = refs[15]
    strips = refs[16:19]
    xt_far = refs[19]
    res_far = dict(zip(RES_NAMES, refs[20:26]))
    grid, edge, vec, table, bias, sems = refs[26:32]
    par = dict(zip(PAR_NAMES, refs[32:45]))
    res = dict(zip(RES_NAMES, refs[45:51]))
    imagery, cotangent, xt = refs[51:]
    need = Copies(sems)
    need.start("imagery", imagery_far, imagery)
    start_params(need, VEC_NAMES, far, par, 0)
    start_params(need, ("qw", "rel", "pw"), far, par, 0)
    need.start("cotangent", cotangent_far, cotangent)
    start_params(need, ("uw", "dw"), far, par, 0)

    def keep(*names):
        for name in names:
            need.start("out " + name, res[name], res_far[name])

    need("imagery")
    for r in range(TILE):
        grid[r, 0:TILE, 0:C] = imagery[r].astype(F32)
    x = to_channels(grid_get(grid, 0, 0))
    xt[...] = x.astype(BF16)
    need(*VEC_NAMES)
    cols = load_columns(vec, par, 0)
    need("rel")
    position_bias(par, 0, table, bias)
    need("cotangent")
    for r in range(TILE):
        grid[r, 0:TILE, 0:C] = cotangent[r].astype(F32)
    emit_strips(grid, edge, strips, 1, 0, 0)
    need.start("out xt", xt, xt_far)
    out = forward(x, par, need, cols, bias, res, None, keep)
    grid_put(grid, to_tokens(out.astype(F32)))
    keep("hidden", "slope")
    for r in range(TILE):
        own[r] = grid[r, 0:TILE, 0:C].astype(BF16)
    emit_strips(grid, edge, strips, 0, 0, 0)
    need.rest()


def second_block(*refs):
    own_in = refs[0]
    strips_in = refs[1:4]
    cotangent_far = refs[4]
    far = dict(zip(PAR_NAMES, refs[5:18]))
    out_own, back_own = refs[18:20]
    strips = refs[20:23]
    flat = refs[23]
    grid, edge, vec, table, bias, sems = refs[24:30]
    par = dict(zip(PAR_NAMES, refs[30:43]))
    small, du_ref, dpacked, rel_sum = refs[43:47]
    res = dict(zip(RES_NAMES, refs[47:53]))
    cotangent = refs[53]
    need = Copies(sems)
    start_params(need, VEC_NAMES, far, par, 1)
    start_params(need, ("rel", "qw", "pw"), far, par, 1)
    need.start("cotangent", cotangent_far, cotangent)
    start_params(need, ("uw", "dw"), far, par, 1)
    last_row = lax.axis_index("rows") == lax.axis_size("rows") - 1
    last_col = lax.axis_index("cols") == lax.axis_size("cols") - 1
    zones = [same_zone(p, last_row, last_col) for p in range(2)]
    fill_grid(grid, edge, own_in, strips_in, 0, 0, 0, 16, 16)
    x = to_channels(grid_get(grid, 4, 4))
    need(*VEC_NAMES)
    cols = load_columns(vec, par, 1)
    need("rel")
    position_bias(par, 1, table, bias)
    out = forward(x, par, need, cols, bias, res, zones, nothing)
    need("cotangent")
    fill_grid(grid, edge, cotangent, strips_in, 1, 0, 0, 16, 16)
    dout = to_channels(grid_get(grid, 4, 4)).astype(BF16)
    grid_put(grid, to_tokens(out.astype(F32)))
    for r in range(TILE):
        out_own[r] = grid[r, 0:TILE, 0:C].astype(BF16)
    emit_strips(grid, edge, strips, 0, 12, 12)
    dx = backward(dout, x, par, need, cols, res, flat, small, du_ref, dpacked, rel_sum)
    grid_put(grid, to_tokens(dx))
    for r in range(TILE):
        back_own[r] = grid[r, 0:TILE, 0:C].astype(BF16)
    emit_strips(grid, edge, strips, 1, 12, 12)
    need.rest()


BACK_NAMES = VEC_NAMES + WEIGHTS


def first_backward(*refs):
    out_in, back_in = refs[0:2]
    strips_in = refs[2:5]
    far = dict(zip(BACK_NAMES, refs[5:17]))
    xt_far = refs[17]
    res_far = dict(zip(RES_NAMES, refs[18:24]))
    output, grad, flat = refs[24:27]
    grid, edge, vec, sems = refs[27:31]
    par = dict(zip(BACK_NAMES, refs[31:43]))
    small, du_ref, dpacked, rel_sum = refs[43:47]
    res = dict(zip(RES_NAMES, refs[47:53]))
    xt = refs[53]
    need = Copies(sems)
    start_params(need, VEC_NAMES + ("dw",), far, par, 0)
    need.start("slope", res_far["slope"], res["slope"])
    need.start("middle", res_far["middle"], res["middle"])
    start_params(need, ("uw",), far, par, 0)
    need.start("hidden", res_far["hidden"], res["hidden"])
    need.start("mixed", res_far["mixed"], res["mixed"])
    start_params(need, ("pw",), far, par, 0)
    need.start("packed", res_far["packed"], res["packed"])
    need.start("attn", res_far["attn"], res["attn"])
    start_params(need, ("qw",), far, par, 0)
    need.start("xt", xt_far, xt)
    fill_grid(grid, edge, back_in, strips_in, 1, 4, 8, 0, 4)
    dout = to_channels(grid_get(grid, 0, 4)).astype(BF16)
    fill_grid(grid, edge, out_in, strips_in, 0, 4, 8, 0, 4)
    for r in range(TILE):
        output[r] = grid[r, 4:20, 0:C].astype(BF16)
    need(*VEC_NAMES)
    cols = load_columns(vec, par, 0)
    need("xt")
    x = xt[...].astype(F32)
    dx = backward(dout, x, par, need, cols, res, flat, small, du_ref, dpacked, rel_sum)
    grid_put(grid, to_tokens(dx))
    for r in range(TILE):
        grad[r] = grid[r, 0:TILE, 0:C].astype(BF16)
    need.rest()


def add_parts(parts, share, fold):
    step = share if share % 8 == 0 else 2 * share
    total = jnp.zeros((step, 128), F32)
    for at in range(0, FLAT, step):
        total = total + parts[at : at + step, :].astype(F32)
    if step == share:
        return total
    fold[0:step, :] = total
    return fold[0:share, :] + fold[share:step, :]


def sum_parts(parts, out, fold):
    out[...] = add_parts(parts, out.shape[0], fold)


def sum_spread(parts, other, out, fold):
    share = other.shape[0]
    total = add_parts(parts, share, fold)
    fold[0:share, :] = other[...]
    fold[share : 2 * share, :] = total
    total = fold[0 : 2 * share, :].astype(BF16)
    for at in range(0, 2 * FLAT, 2 * share):
        out[at : at + 2 * share, :] = total


def unpack(share, both, *outs):
    ng, nb, qw_far, qb, rel, pw_far, pb, mg, mb, uw_far, ub, dw_far, db, wide, flats, qw, pw, uw, dw, sems = outs
    copies = Copies(sems)
    factor = outs_factor
    flip = (iota((256, 256), 0) + iota((256, 256), 1) == 255).astype(BF16)
    wide[...] = both[...].astype(F32) * factor
    for b in range(2):
        flat = flats.at[b]
        for at in range(0, FLAT, share):
            flat[at : at + share, :] = wide[2 * at + (1 - b) * share : 2 * at + (2 - b) * share, :]
        for j in range(4):
            qw[b, :, 128 * j : 128 * j + 128] = flat[C * j : C * j + C, :]
        tail = flat[768:960, :]
        qw[b, :, 512:576] = tail[:, 0:64]
        pw[b, :, 128:192] = pltpu.roll(tail, 64, 1)[:, 0:64]
        pw[b, :, 0:128] = flat[960:1152, :]
        copies.start(("qw", b), qw.at[b], qw_far.at[b])
        copies.start(("pw", b), pw.at[b], pw_far.at[b])
        for j in range(6):
            uw[b, :, 128 * j : 128 * j + 128] = flat[1152 + C * j : 1152 + C * j + C, :]
            dw[b, :, 128 * j : 128 * j + 128] = flat[2304 + C * j : 2304 + C * j + C, :]
        copies.start(("uw", b), uw.at[b], uw_far.at[b])
        copies.start(("dw", b), dw.at[b], dw_far.at[b])
        for at, ref in ((0, ng), (2, nb), (4, qb), (9, pb), (11, mg), (13, mb), (15, ub), (21, db)):
            n = ref.shape[-1]
            at = at + SMALL
            for i in range(0, n, 128):
                w = min(128, n - i)
                ref[b : b + 1, i : i + w] = flat[at + i // 128 : at + i // 128 + 1, 0:w]
        table = jnp.concatenate([flat[SMALL + 24 : SMALL + 32, :], flat[SMALL + 32 : SMALL + 40, :]], axis=1)
        high, mid, low = split3(table)
        table = dot_nn(high, flip) + (dot_nn(mid, flip) + dot_nn(low, flip))
        for h in range(HEADS):
            rel[h, b : b + 1, :] = table[h : h + 1, 0 : SPAN * SPAN]
    copies.rest()


outs_factor = float(128 * 256) ** (-0.5)


VMEM = pl.BlockSpec(memory_space=pltpu.VMEM)


def near(value):
    return pltpu.with_memory_space_constraint(value, pltpu.VMEM)


FAR = pl.BlockSpec(memory_space=pltpu.HBM)


def call(kernel, args, far_args, outs, far_outs, scratch, flops):
    return pl.pallas_call(
        kernel,
        in_specs=[VMEM] * len(args) + [FAR] * len(far_args),
        out_specs=[VMEM] * len(outs) + [FAR] * len(far_outs),
        out_shape=list(outs) + [pltpu.HBM(o.shape, o.dtype) for o in far_outs],
        scratch_shapes=scratch,
        compiler_params=pltpu.CompilerParams(vmem_limit_bytes=30 * 2**20),
        cost_estimate=pl.CostEstimate(flops=flops, transcendentals=0, bytes_accessed=4000000),
    )(*[near(a) for a in args], *[pltpu.with_memory_space_constraint(a, pltpu.HBM) for a in far_args])


def shaped(shape, dtype=BF16):
    return jax.ShapeDtypeStruct(shape, dtype)


def exchange(strips, step):
    n_rows = lax.axis_size("rows")
    n_cols = lax.axis_size("cols")
    col_strip, row_strip, corner = strips
    along = [(c, (c + step) % n_cols) for c in range(n_cols)]
    down = [(r, (r + step) % n_rows) for r in range(n_rows)]
    both = [
        (r * n_cols + c, ((r + step) % n_rows) * n_cols + (c + step) % n_cols)
        for r in range(n_rows)
        for c in range(n_cols)
    ]
    col_strip = lax.ppermute(col_strip, "cols", along)
    row_strip = lax.ppermute(row_strip, "rows", down)
    corner = lax.ppermute(corner, ("rows", "cols"), both)
    return [col_strip, row_strip, corner]


def send_parts(value):
    n = lax.axis_size("rows") * lax.axis_size("cols")
    share = value.shape[0] // n
    shape = (n, share, 128) if share % 8 == 0 else (n, share // 4, 4, 128)
    got = lax.all_to_all(value.reshape(shape), ("rows", "cols"), 0, 0, tiled=True)
    return got.reshape(value.shape)


def both_blocks(imagery, cotangent, *params):
    params = list(params)
    params[4] = params[4].transpose(1, 0, 2)
    params[11] = params[11].swapaxes(1, 2)
    tile = (TILE, TILE, C)
    strips = [pltpu.VMEM(s, BF16) for s in ((128, C), (128, C), (32, C))]
    packed_grads = pltpu.VMEM((FLAT, 128), BF16)
    held = pltpu.VMEM(tile, BF16)
    grid = pltpu.VMEM((24, 24, 256), F32)
    edge = pltpu.VMEM((64, 256), F32)
    vec = pltpu.VMEM((128, MLP), F32)
    tables = [pltpu.VMEM((8, 256), F32), pltpu.VMEM((HEADS, 64, 128), F32)]
    work = [
        pltpu.VMEM((48, 128), F32),
        pltpu.VMEM((MLP, TOK), BF16),
        pltpu.VMEM((576, TOK), BF16),
        pltpu.VMEM((HEADS, 64, 128), F32),
    ]
    par = dict(zip(PAR_NAMES, params))
    par_kinds = {n: BF16 if n in WEIGHTS else F32 for n in PAR_NAMES}
    par_vmem = {n: pltpu.VMEM(PAR_SHAPES[n], par_kinds[n]) for n in PAR_NAMES}
    res_vmem = [pltpu.VMEM(s, BF16) for s in RES_SHAPES]
    sems = pltpu.SemaphoreType.DMA((32,))
    one = call(
        first_forward,
        (),
        (imagery, cotangent, *params),
        [held] + strips,
        [shaped((C, TOK))] + [shaped(s) for s in RES_SHAPES],
        [grid, edge, vec] + tables + [sems] + list(par_vmem.values()) + res_vmem + [held, held, pltpu.VMEM((C, TOK), BF16)],
        5 * 10**9,
    )
    own, got, xt, res = one[0], exchange(one[1:4], -1), one[4], one[5:]
    two = call(
        second_block,
        (own, *got),
        (cotangent, *params),
        [held, held] + strips + [packed_grads],
        [],
        [grid, edge, vec] + tables + [sems] + list(par_vmem.values()) + work + res_vmem + [held],
        10**10,
    )
    got = exchange(two[2:5], 1)
    output, grad, flat_one = call(
        first_backward,
        (two[0], two[1], *got),
        (*[par[n] for n in BACK_NAMES], xt, *res),
        [shaped(tile), shaped(tile), packed_grads],
        [],
        [grid, edge, vec, sems] + [par_vmem[n] for n in BACK_NAMES] + work + res_vmem + [pltpu.VMEM((C, TOK), BF16)],
        5 * 10**9,
    )
    parts_two = send_parts(two[5])
    parts_one = send_parts(flat_one)
    share = FLAT // (lax.axis_size("rows") * lax.axis_size("cols"))
    fold = pltpu.VMEM((max(2 * share, 8), 128), F32)
    sum_two = call(sum_parts, (parts_two,), (), [pltpu.VMEM((share, 128), F32)], [], [fold], 10**6)[0]
    both = call(sum_spread, (parts_one, sum_two), (), [pltpu.VMEM((2 * FLAT, 128), BF16)], [], [fold], 10**6)[0]
    weights = [pltpu.VMEM((2,) + PAR_SHAPES[n], F32) for n in ("qw", "pw", "uw", "dw")]
    grads = pl.pallas_call(
        functools.partial(unpack, share),
        in_specs=[VMEM],
        out_specs=[FAR if n in WEIGHTS else VMEM for n in PAR_NAMES],
        out_shape=[shaped(p.shape, F32) for p in params],
        scratch_shapes=[pltpu.VMEM((2 * FLAT, 128), F32), pltpu.VMEM((2, FLAT, 128), F32)]
        + weights
        + [pltpu.SemaphoreType.DMA((8,))],
        name="unpack",
        compiler_params=pltpu.CompilerParams(vmem_limit_bytes=30 * 2**20),
    )(near(send_parts(both)))
    grads = list(grads)
    grads[4] = grads[4].transpose(1, 0, 2)
    grads[11] = grads[11].swapaxes(1, 2)
    return (output, grad, *grads)


def solution(mesh):
    tile = P("rows", "cols", None)
    return jax.shard_map(
        both_blocks,
        mesh=mesh,
        in_specs=(tile, tile) + (P(),) * 13,
        out_specs=(tile, tile) + (P(),) * 13,
        check_vma=False,
    )
```

```python
import functools

import jax
import jax.numpy as jnp
from jax import lax
from jax.experimental import pallas as pl
from jax.experimental.pallas import tpu as pltpu
from jax.sharding import PartitionSpec as P

F32 = jnp.float32
BF16 = jnp.bfloat16
C = 192
HEADS = 6
DIM = 32
MLP = 768
TILE = 16
TOK = TILE * TILE
SPAN = 15
SCALE = DIM**-0.5
EPSILON = 1e-05
FLAT = 3584
SMALL = 3456
MASKED = -1e30


def dot_tn(a, b):
    return lax.dot_general(a, b, (((0,), (0,)), ((), ())), preferred_element_type=F32)


def dot_nn(a, b):
    return lax.dot_general(a, b, (((1,), (0,)), ((), ())), preferred_element_type=F32)


def dot_nt(a, b):
    return lax.dot_general(a, b, (((1,), (1,)), ((), ())), preferred_element_type=F32)


def iota(shape, dim):
    return lax.broadcasted_iota(jnp.int32, shape, dim)


def split3(value):
    high = value.astype(BF16)
    rest = value - high.astype(F32)
    mid = rest.astype(BF16)
    return high, mid, (rest - mid.astype(F32)).astype(BF16)


def window_row(r, wc):
    return ((r // 8) * 2 + wc) * 64 + (r % 8) * 8


def halves():
    return iota((64, 128), 1) < 64


def stack_windows(value, left):
    zero = jnp.zeros_like(value)
    return jnp.concatenate([jnp.where(left, value, zero), jnp.where(left, zero, value)], axis=0).astype(BF16)


def own_window(full, left):
    return jnp.where(left, full[:64], full[64:])


def norm_fwd(x):
    center = x - jnp.mean(x, axis=0, keepdims=True)
    rstd = lax.rsqrt(jnp.mean(center * center, axis=0, keepdims=True) + EPSILON)
    return center * rstd, rstd


def norm_bwd(dn, xhat, rstd, gain):
    dxh = dn * gain
    along = jnp.mean(dxh * xhat, axis=0, keepdims=True)
    return rstd * (dxh - jnp.mean(dxh, axis=0, keepdims=True) - xhat * along)


def spread(lane_q):
    q = lane_q % 64
    return (q // 8) * SPAN + q % 8


VEC_NAMES = ("ng", "nb", "pb", "mg", "mb", "db", "qb", "ub")


def load_columns(vec, par, b):
    for i, name in enumerate(VEC_NAMES):
        n = par[name].shape[-1]
        vec[i : i + 1, 0:n] = par[name][b : b + 1, :]
    return vec[...].T


def position_bias(par, b, table, bias):
    table[...] = jnp.zeros((8, 256), F32)
    for h in range(HEADS):
        table[h : h + 1, 0 : SPAN * SPAN] = par["rel"][h, b : b + 1, :]
    select = (iota((128, 128), 0) == spread(iota((128, 128), 1))).astype(BF16)
    for h in range(HEADS):
        row = jnp.broadcast_to(table[h : h + 1, :], (8, 256))
        rows = []
        for ky in range(8):
            shift = (249 - SPAN * (7 - ky)) % 256
            rows.append(pltpu.roll(row, shift, 1, stride=1, stride_axis=0)[:, 0:128])
        high, mid, low = split3(jnp.concatenate(rows, axis=0))
        bias[h] = dot_nn(high, select) + (dot_nn(mid, select) + dot_nn(low, select))


def same_zone(p, last_row, last_col):
    k = iota((64, 128), 0)
    lane = iota((64, 128), 1)
    q = lane % 64
    rows = ((q // 8) < 4) == ((k // 8) < 4)
    cols = ((q % 8) < 4) == ((k % 8) < 4)
    keep = jnp.logical_or(cols, jnp.logical_or(lane < 64, jnp.logical_not(last_col)))
    if p == 1:
        keep = jnp.logical_and(keep, jnp.logical_or(rows, jnp.logical_not(last_row)))
    return keep


def forward(x, par, need, cols, bias, res, zones, keep):
    left = halves()
    xhat, _ = norm_fwd(x)
    normed = (xhat * cols[0:C, 0:1] + cols[0:C, 1:2]).astype(BF16)
    need("qw")
    res["packed"][...] = (dot_tn(par["qw"][...], normed) + cols[0:576, 6:7]).astype(BF16)
    for p in range(2):
        lanes = slice(128 * p, 128 * p + 128)
        for h in range(HEADS):
            q = res["packed"][DIM * h : DIM * h + DIM, lanes]
            k = res["packed"][C + DIM * h : C + DIM * h + DIM, lanes]
            v = res["packed"][2 * C + DIM * h : 2 * C + DIM * h + DIM, lanes]
            s = own_window(dot_tn(k, q), left) * SCALE + bias[h]
            if zones is not None:
                s = jnp.where(zones[p], s, MASKED)
            e = jnp.exp(s - jnp.max(s, axis=0, keepdims=True))
            a = e * (1.0 / jnp.sum(e, axis=0, keepdims=True))
            res["attn"][p * HEADS + h] = a.astype(BF16)
            res["mixed"][DIM * h : DIM * h + DIM, lanes] = dot_nn(v, stack_windows(a, left)).astype(BF16)
    keep("packed")
    need("pw")
    middle = x + dot_tn(par["pw"][...], res["mixed"][...]) + cols[0:C, 2:3]
    res["middle"][...] = middle.astype(BF16)
    middle = res["middle"][...].astype(F32)
    xhat, _ = norm_fwd(middle)
    normed = (xhat * cols[0:C, 3:4] + cols[0:C, 4:5]).astype(BF16)
    keep("attn", "mixed")
    need("uw")
    for i in range(0, MLP, 128):
        u = dot_tn(par["uw"][:, i : i + 128], normed) + cols[i : i + 128, 7:8]
        half = 0.5 + 0.5 * lax.erf(u * (0.5**0.5))
        res["hidden"][i : i + 128, :] = (u * half).astype(BF16)
        res["slope"][i : i + 128, :] = (half + u * (jnp.exp(-0.5 * u * u) * 0.3989422804014327)).astype(BF16)
    keep("middle")
    need("dw")
    out = middle + dot_nn(par["dw"][...], res["hidden"][...]) + cols[0:C, 5:6]
    return out.astype(BF16)


def put_row(small, at, row):
    n = row.shape[-1]
    for i in range(0, n, 128):
        w = min(128, n - i)
        small[at + i // 128 : at + i // 128 + 1, 0:w] = row[0:1, i : i + w]


def put_pairs(flat, at, lhs, rhs, n):
    for i in range(0, n, 256):
        wide = dot_nt(lhs, rhs[i : i + 256, :]).astype(BF16)
        for j in range(0, 256, 128):
            first = at + C * ((i + j) // 128)
            flat[first : first + C, :] = wide[:, j : j + 128]


def backward(dout, x, par, need, cols, res, flat, small, du_ref, dpacked, rel_sum):
    left = halves()
    ones = jnp.ones((8, TOK), BF16)
    none = jnp.zeros((64, TOK), BF16)
    small[...] = jnp.zeros(small.shape, F32)
    put_row(small, 21, dot_nt(ones, dout))
    need("dw", "slope")
    for i in range(0, MLP, 128):
        dh = dot_tn(par["dw"][:, i : i + 128], dout).astype(BF16).astype(F32)
        du = (dh * res["slope"][i : i + 128, :].astype(F32)).astype(BF16)
        du_ref[i : i + 128, :] = du
    need("middle", "uw")
    middle = res["middle"][...].astype(F32)
    xhat, rstd = norm_fwd(middle)
    normed = (xhat * cols[0:C, 3:4] + cols[0:C, 4:5]).astype(BF16)
    put_pairs(flat, 1152, normed, du_ref, MLP)
    need("hidden")
    put_pairs(flat, 2304, dout, res["hidden"], MLP)
    put_row(small, 15, dot_nt(ones, du_ref[...]))
    dn = dot_nn(par["uw"][...], du_ref[...]).astype(BF16)
    put_row(small, 13, dot_nt(ones, dn))
    dn = dn.astype(F32)
    put_row(small, 11, dot_nt(ones, (dn * xhat).astype(BF16)))
    dmid = (dout.astype(F32) + norm_bwd(dn, xhat, rstd, cols[0:C, 3:4])).astype(BF16)
    need("pw", "mixed")
    put_row(small, 9, dot_nt(ones, dmid))
    flat[960:1152, :] = dot_nt(res["mixed"][...], dmid[0:128]).astype(BF16)
    dmixed = dot_nn(par["pw"][...], dmid).astype(BF16)
    need("packed", "attn")
    for h in range(HEADS):
        drel = None
        for p in range(2):
            lanes = slice(128 * p, 128 * p + 128)
            q = res["packed"][DIM * h : DIM * h + DIM, lanes]
            k = res["packed"][C + DIM * h : C + DIM * h + DIM, lanes]
            v = res["packed"][2 * C + DIM * h : 2 * C + DIM * h + DIM, lanes]
            a = res["attn"][p * HEADS + h].astype(F32)
            dm = dmixed[DIM * h : DIM * h + DIM, lanes]
            da = own_window(dot_tn(v, dm), left).astype(BF16).astype(F32)
            ds = a * (da - jnp.sum(da * a, axis=0, keepdims=True))
            drel = ds if drel is None else drel + ds
            wide = stack_windows(ds * SCALE, left)
            dpacked[DIM * h : DIM * h + DIM, lanes] = dot_nn(k, wide).astype(BF16)
            dpacked[C + DIM * h : C + DIM * h + DIM, lanes] = dot_nt(q, wide).astype(BF16)
            dpacked[2 * C + DIM * h : 2 * C + DIM * h + DIM, lanes] = dot_nt(dm, stack_windows(a, left)).astype(BF16)
        rel_sum[h] = drel
    mirror = ((127 - iota((128, 128), 0)) == spread(iota((128, 128), 1))).astype(BF16)
    for h in range(HEADS):
        high, mid, _ = split3(rel_sum[h])
        back = dot_nt(high, mirror) + dot_nt(mid, mirror)
        total = jnp.zeros((8, 256), F32)
        for ky in range(8):
            wide = jnp.concatenate([back[8 * ky : 8 * ky + 8], jnp.zeros((8, 128), F32)], axis=1)
            total = total + pltpu.roll(wide, 121 - SPAN * (7 - ky), 1, stride=1, stride_axis=0)
        total = jnp.sum(total, axis=0, keepdims=True)
        small[24 + h : 25 + h, :] = total[:, 0:128]
        small[32 + h : 33 + h, :] = total[:, 128:256]
    xhat, rstd = norm_fwd(x)
    normed = (xhat * cols[0:C, 0:1] + cols[0:C, 1:2]).astype(BF16)
    put_pairs(flat, 0, normed, dpacked, 512)
    tail = dot_nt(normed, jnp.concatenate([dpacked[512:576, :], none], axis=0))
    tail = tail + dot_nt(res["mixed"][...], jnp.concatenate([none, dmid[128:192]], axis=0))
    flat[768:960, :] = tail.astype(BF16)
    put_row(small, 4, dot_nt(ones, dpacked[...]))
    need("qw")
    dn = dot_nn(par["qw"][...], dpacked[...]).astype(BF16)
    put_row(small, 2, dot_nt(ones, dn))
    dn = dn.astype(F32)
    put_row(small, 0, dot_nt(ones, (dn * xhat).astype(BF16)))
    flat[SMALL : SMALL + 48, :] = small[...].astype(BF16)
    flat[SMALL + 48 : FLAT, :] = jnp.zeros((FLAT - SMALL - 48, 128), BF16)
    return dmid.astype(F32) + norm_bwd(dn, xhat, rstd, cols[0:C, 0:1])


def to_channels(pieces):
    return jnp.concatenate(pieces, axis=0).T[0:C]


def to_tokens(value):
    return jnp.concatenate([value, jnp.zeros((64, TOK), F32)], axis=0).T


def grid_put(grid, tokens):
    for r in range(TILE):
        for wc in range(2):
            at = window_row(r, wc)
            grid[r, 8 * wc : 8 * wc + 8, :] = tokens[at : at + 8]


def grid_get(grid, row_at, col_at):
    pieces = []
    for wr in range(2):
        for wc in range(2):
            for ir in range(8):
                at = col_at + 8 * wc
                pieces.append(grid[row_at + 8 * wr + ir, at : at + 8, :])
    return pieces


def emit_strips(grid, edge, strips, which, row_at, col_at):
    col_out, row_out, corner_out = strips
    for r in range(TILE):
        edge[4 * r : 4 * r + 4, :] = grid[r, col_at : col_at + 4, :]
    col_out[64 * which : 64 * which + 64, :] = edge[:, 0:C].astype(BF16)
    for r in range(4):
        row_out[64 * which + 16 * r : 64 * which + 16 * r + 16, :] = grid[row_at + r, 0:TILE, 0:C].astype(BF16)
    for r in range(4):
        edge[4 * r : 4 * r + 4, :] = grid[row_at + r, col_at : col_at + 4, :]
    corner_out[16 * which : 16 * which + 16, :] = edge[0:16, 0:C].astype(BF16)


def fill_grid(grid, edge, own, strips, which, own_row, own_col, strip_row, strip_col):
    col_in, row_in, corner_in = strips
    for r in range(TILE):
        grid[own_row + r, own_col : own_col + TILE, 0:C] = own[r].astype(F32)
    edge[:, 0:C] = col_in[64 * which : 64 * which + 64, :].astype(F32)
    for r in range(TILE):
        grid[own_row + r, strip_col : strip_col + 4, :] = edge[4 * r : 4 * r + 4, :]
    for r in range(4):
        at = 64 * which + 16 * r
        grid[strip_row + r, own_col : own_col + TILE, 0:C] = row_in[at : at + 16, :].astype(F32)
    edge[0:16, 0:C] = corner_in[16 * which : 16 * which + 16, :].astype(F32)
    for r in range(4):
        grid[strip_row + r, strip_col : strip_col + 4, :] = edge[4 * r : 4 * r + 4, :]


PAR_NAMES = ("ng", "nb", "qw", "qb", "rel", "pw", "pb", "mg", "mb", "uw", "ub", "dw", "db")
RES_NAMES = ("packed", "attn", "mixed", "middle", "hidden", "slope")
RES_SHAPES = ((576, TOK), (12, 64, 128), (C, TOK), (C, TOK), (MLP, TOK), (MLP, TOK))


class Copies:
    def __init__(self, sems):
        self.sems = sems
        self.used = 0
        self.open = {}

    def start(self, name, source, target):
        self.open[name] = pltpu.make_async_copy(source, target, self.sems.at[self.used])
        self.open[name].start()
        self.used += 1

    def __call__(self, *names):
        for name in names:
            if name in self.open:
                self.open.pop(name).wait()

    def rest(self):
        self(*list(self.open))


def start_params(copies, names, far, par, b):
    for name in names:
        source = far[name].at[b] if name in WEIGHTS else far[name]
        copies.start(name, source, par[name])


WEIGHTS = ("qw", "pw", "uw", "dw")
PAR_SHAPES = dict(
    ng=(2, C), nb=(2, C), qw=(C, 3 * C), qb=(2, 3 * C), rel=(HEADS, 2, SPAN * SPAN), pw=(C, C), pb=(2, C),
    mg=(2, C), mb=(2, C), uw=(C, MLP), ub=(2, MLP), dw=(C, MLP), db=(2, C),
)


def nothing(*_):
    pass


def first_forward(*refs):
    imagery_far, cotangent_far = refs[0:2]
    far = dict(zip(PAR_NAMES, refs[2:15]))
    own = refs[15]
    strips = refs[16:19]
    xt_far = refs[19]
    res_far = dict(zip(RES_NAMES, refs[20:26]))
    grid, edge, vec, table, bias, sems = refs[26:32]
    par = dict(zip(PAR_NAMES, refs[32:45]))
    res = dict(zip(RES_NAMES, refs[45:51]))
    imagery, cotangent, xt = refs[51:]
    need = Copies(sems)
    need.start("imagery", imagery_far, imagery)
    start_params(need, VEC_NAMES, far, par, 0)
    start_params(need, ("qw", "rel", "pw"), far, par, 0)
    need.start("cotangent", cotangent_far, cotangent)
    start_params(need, ("uw", "dw"), far, par, 0)

    def keep(*names):
        for name in names:
            need.start("out " + name, res[name], res_far[name])

    need("imagery")
    for r in range(TILE):
        grid[r, 0:TILE, 0:C] = imagery[r].astype(F32)
    x = to_channels(grid_get(grid, 0, 0))
    xt[...] = x.astype(BF16)
    need(*VEC_NAMES)
    cols = load_columns(vec, par, 0)
    need("rel")
    position_bias(par, 0, table, bias)
    need("cotangent")
    for r in range(TILE):
        grid[r, 0:TILE, 0:C] = cotangent[r].astype(F32)
    emit_strips(grid, edge, strips, 1, 0, 0)
    need.start("out xt", xt, xt_far)
    out = forward(x, par, need, cols, bias, res, None, keep)
    grid_put(grid, to_tokens(out.astype(F32)))
    keep("hidden", "slope")
    for r in range(TILE):
        own[r] = grid[r, 0:TILE, 0:C].astype(BF16)
    emit_strips(grid, edge, strips, 0, 0, 0)
    need.rest()


def second_block(*refs):
    own_in = refs[0]
    strips_in = refs[1:4]
    cotangent_far = refs[4]
    far = dict(zip(PAR_NAMES, refs[5:18]))
    out_own, back_own = refs[18:20]
    strips = refs[20:23]
    flat = refs[23]
    grid, edge, vec, table, bias, sems = refs[24:30]
    par = dict(zip(PAR_NAMES, refs[30:43]))
    small, du_ref, dpacked, rel_sum = refs[43:47]
    res = dict(zip(RES_NAMES, refs[47:53]))
    cotangent = refs[53]
    need = Copies(sems)
    start_params(need, VEC_NAMES, far, par, 1)
    start_params(need, ("rel", "qw", "pw"), far, par, 1)
    need.start("cotangent", cotangent_far, cotangent)
    start_params(need, ("uw", "dw"), far, par, 1)
    last_row = lax.axis_index("rows") == lax.axis_size("rows") - 1
    last_col = lax.axis_index("cols") == lax.axis_size("cols") - 1
    zones = [same_zone(p, last_row, last_col) for p in range(2)]
    fill_grid(grid, edge, own_in, strips_in, 0, 0, 0, 16, 16)
    x = to_channels(grid_get(grid, 4, 4))
    need(*VEC_NAMES)
    cols = load_columns(vec, par, 1)
    need("rel")
    position_bias(par, 1, table, bias)
    out = forward(x, par, need, cols, bias, res, zones, nothing)
    need("cotangent")
    fill_grid(grid, edge, cotangent, strips_in, 1, 0, 0, 16, 16)
    dout = to_channels(grid_get(grid, 4, 4)).astype(BF16)
    grid_put(grid, to_tokens(out.astype(F32)))
    for r in range(TILE):
        out_own[r] = grid[r, 0:TILE, 0:C].astype(BF16)
    emit_strips(grid, edge, strips, 0, 12, 12)
    dx = backward(dout, x, par, need, cols, res, flat, small, du_ref, dpacked, rel_sum)
    grid_put(grid, to_tokens(dx))
    for r in range(TILE):
        back_own[r] = grid[r, 0:TILE, 0:C].astype(BF16)
    emit_strips(grid, edge, strips, 1, 12, 12)
    need.rest()


BACK_NAMES = VEC_NAMES + WEIGHTS


def first_backward(*refs):
    out_in, back_in = refs[0:2]
    strips_in = refs[2:5]
    flat_two = refs[5]
    far = dict(zip(BACK_NAMES, refs[6:18]))
    xt_far = refs[18]
    res_far = dict(zip(RES_NAMES, refs[19:25]))
    output, grad, kept, sent = refs[25:29]
    grid, edge, vec, sems = refs[29:33]
    par = dict(zip(BACK_NAMES, refs[33:45]))
    small, du_ref, dpacked, rel_sum = refs[45:49]
    res = dict(zip(RES_NAMES, refs[49:55]))
    xt, flat = refs[55:]
    need = Copies(sems)
    start_params(need, VEC_NAMES + ("dw",), far, par, 0)
    need.start("slope", res_far["slope"], res["slope"])
    need.start("middle", res_far["middle"], res["middle"])
    start_params(need, ("uw",), far, par, 0)
    need.start("hidden", res_far["hidden"], res["hidden"])
    need.start("mixed", res_far["mixed"], res["mixed"])
    start_params(need, ("pw",), far, par, 0)
    need.start("packed", res_far["packed"], res["packed"])
    need.start("attn", res_far["attn"], res["attn"])
    start_params(need, ("qw",), far, par, 0)
    need.start("xt", xt_far, xt)
    fill_grid(grid, edge, back_in, strips_in, 1, 4, 8, 0, 4)
    dout = to_channels(grid_get(grid, 0, 4)).astype(BF16)
    fill_grid(grid, edge, out_in, strips_in, 0, 4, 8, 0, 4)
    for r in range(TILE):
        output[r] = grid[r, 4:20, 0:C].astype(BF16)
    need(*VEC_NAMES)
    cols = load_columns(vec, par, 0)
    need("xt")
    x = xt[...].astype(F32)
    dx = backward(dout, x, par, need, cols, res, flat, small, du_ref, dpacked, rel_sum)
    grid_put(grid, to_tokens(dx))
    for r in range(TILE):
        grad[r] = grid[r, 0:TILE, 0:C].astype(BF16)
    even = lax.axis_index("cols") % 2 == 0
    for at in range(0, FLAT, 256):
        rows = slice(at, at + 256)
        kept[rows, :] = jnp.where(even, flat[rows, :], flat_two[rows, :])
        sent[rows, :] = jnp.where(even, flat_two[rows, :], flat[rows, :])
    need.rest()


def add_pair(kept, got, out):
    for at in range(0, FLAT, 256):
        rows = slice(at, at + 256)
        out[rows, :] = (kept[rows, :].astype(F32) + got[rows, :].astype(F32)).astype(BF16)


def sum_spread(share, parts, out):
    total = jnp.zeros((share, 128), F32)
    for at in range(0, FLAT, share):
        total = total + parts[at : at + share, :].astype(F32)
    total = total.astype(BF16)
    for at in range(0, FLAT, share):
        out[at : at + share, :] = total


def unpack(mine, other, *outs):
    ng, nb, qw_far, qb, rel, pw_far, pb, mg, mb, uw_far, ub, dw_far, db, qw, pw, uw, dw, sems = outs
    copies = Copies(sems)
    factor = outs_factor
    flip = (iota((256, 256), 0) + iota((256, 256), 1) == 255).astype(BF16)
    parity = lax.axis_index("cols") % 2
    for b in range(2):

        def raw(at, n):
            return jnp.where(parity == b, mine[at : at + n, :], other[at : at + n, :])

        def rows(at, n):
            return raw(at, n).astype(F32) * factor

        for j in range(4):
            qw[b, :, 128 * j : 128 * j + 128] = rows(C * j, C)
        tail = rows(768, C)
        qw[b, :, 512:576] = tail[:, 0:64]
        copies.start(("qw", b), qw.at[b], qw_far.at[b])
        pw[b, :, 128:192] = pltpu.roll(tail, 64, 1)[:, 0:64]
        pw[b, :, 0:128] = rows(960, C)
        copies.start(("pw", b), pw.at[b], pw_far.at[b])
        for j in range(6):
            uw[b, :, 128 * j : 128 * j + 128] = rows(1152 + C * j, C)
        copies.start(("uw", b), uw.at[b], uw_far.at[b])
        for j in range(6):
            dw[b, :, 128 * j : 128 * j + 128] = rows(2304 + C * j, C)
        copies.start(("dw", b), dw.at[b], dw_far.at[b])
        small = rows(SMALL, 48)
        for at, ref in ((0, ng), (2, nb), (4, qb), (9, pb), (11, mg), (13, mb), (15, ub), (21, db)):
            n = ref.shape[-1]
            for i in range(0, n, 128):
                w = min(128, n - i)
                ref[b : b + 1, i : i + w] = small[at + i // 128 : at + i // 128 + 1, 0:w]
        table = jnp.concatenate([raw(SMALL + 24, 8), raw(SMALL + 32, 8)], axis=1)
        table = dot_nn(table, flip) * factor
        for h in range(HEADS):
            rel[h, b : b + 1, :] = table[h : h + 1, 0 : SPAN * SPAN]
    copies.rest()


outs_factor = float(128 * 256) ** (-0.5)


VMEM = pl.BlockSpec(memory_space=pltpu.VMEM)


def near(value):
    return pltpu.with_memory_space_constraint(value, pltpu.VMEM)


FAR = pl.BlockSpec(memory_space=pltpu.HBM)


def call(kernel, name, args, far_args, outs, far_outs, scratch, flops):
    return pl.pallas_call(
        kernel,
        in_specs=[VMEM] * len(args) + [FAR] * len(far_args),
        out_specs=[VMEM] * len(outs) + [FAR] * len(far_outs),
        out_shape=list(outs) + [pltpu.HBM(o.shape, o.dtype) for o in far_outs],
        scratch_shapes=scratch,
        name=name,
        compiler_params=pltpu.CompilerParams(vmem_limit_bytes=30 * 2**20),
        cost_estimate=pl.CostEstimate(flops=flops, transcendentals=0, bytes_accessed=4000000),
    )(*[near(a) for a in args], *[pltpu.with_memory_space_constraint(a, pltpu.HBM) for a in far_args])


def shaped(shape, dtype=BF16):
    return jax.ShapeDtypeStruct(shape, dtype)


def exchange(strips, step):
    n_rows = lax.axis_size("rows")
    n_cols = lax.axis_size("cols")
    col_strip, row_strip, corner = strips
    along = [(c, (c + step) % n_cols) for c in range(n_cols)]
    down = [(r, (r + step) % n_rows) for r in range(n_rows)]
    both = [
        (r * n_cols + c, ((r + step) % n_rows) * n_cols + (c + step) % n_cols)
        for r in range(n_rows)
        for c in range(n_cols)
    ]
    return [
        lax.ppermute(col_strip, "cols", along),
        lax.ppermute(row_strip, "rows", down),
        lax.ppermute(corner, ("rows", "cols"), both),
    ]


def swap(value):
    return lax.ppermute(value, "cols", [(c, c ^ 1) for c in range(lax.axis_size("cols"))])


def send_parts(value):
    n_cols = lax.axis_size("cols")
    n = lax.axis_size("rows") * n_cols
    groups = [[d for d in range(n) if d % n_cols % 2 == p] for p in range(2)]
    parts = value.reshape(n // 2, 2 * FLAT // n, 128)
    got = lax.all_to_all(parts, ("rows", "cols"), 0, 0, axis_index_groups=groups, tiled=True)
    return got.reshape(value.shape)


def per_device(imagery, cotangent, *params):
    params = list(params)
    params[4] = params[4].transpose(1, 0, 2)
    params[11] = params[11].swapaxes(1, 2)
    tile = (TILE, TILE, C)
    strips = [pltpu.VMEM(s, BF16) for s in ((128, C), (128, C), (32, C))]
    packed_grads = pltpu.VMEM((FLAT, 128), BF16)
    held = pltpu.VMEM(tile, BF16)
    grid = pltpu.VMEM((24, 24, 256), F32)
    edge = pltpu.VMEM((64, 256), F32)
    vec = pltpu.VMEM((128, MLP), F32)
    tables = [pltpu.VMEM((8, 256), F32), pltpu.VMEM((HEADS, 64, 128), F32)]
    work = [
        pltpu.VMEM((48, 128), F32),
        pltpu.VMEM((MLP, TOK), BF16),
        pltpu.VMEM((576, TOK), BF16),
        pltpu.VMEM((HEADS, 64, 128), F32),
    ]
    par = dict(zip(PAR_NAMES, params))
    par_kinds = {n: BF16 if n in WEIGHTS else F32 for n in PAR_NAMES}
    par_vmem = {n: pltpu.VMEM(PAR_SHAPES[n], par_kinds[n]) for n in PAR_NAMES}
    res_vmem = [pltpu.VMEM(s, BF16) for s in RES_SHAPES]
    sems = pltpu.SemaphoreType.DMA((32,))
    one = call(
        first_forward,
        "first_forward",
        (),
        (imagery, cotangent, *params),
        [held] + strips,
        [shaped((C, TOK))] + [shaped(s) for s in RES_SHAPES],
        [grid, edge, vec] + tables + [sems] + list(par_vmem.values()) + res_vmem + [held, held, pltpu.VMEM((C, TOK), BF16)],
        5 * 10**9,
    )
    own, got, xt, res = one[0], exchange(one[1:4], -1), one[4], one[5:]
    two = call(
        second_block,
        "second_block",
        (own, *got),
        (cotangent, *params),
        [held, held] + strips + [packed_grads],
        [],
        [grid, edge, vec] + tables + [sems] + list(par_vmem.values()) + work + res_vmem + [held],
        10**10,
    )
    got = exchange(two[2:5], 1)
    output, grad, kept, sent = call(
        first_backward,
        "first_backward",
        (two[0], two[1], *got, two[5]),
        (*[par[n] for n in BACK_NAMES], xt, *res),
        [shaped(tile), shaped(tile), packed_grads, packed_grads],
        [],
        [grid, edge, vec, sems]
        + [par_vmem[n] for n in BACK_NAMES]
        + work
        + res_vmem
        + [pltpu.VMEM((C, TOK), BF16), packed_grads],
        5 * 10**9,
    )
    pair = call(add_pair, "add_pair", (kept, swap(sent)), (), [packed_grads], [], [], 10**6)[0]
    share = 2 * FLAT // (lax.axis_size("rows") * lax.axis_size("cols"))
    spread = functools.partial(sum_spread, share)
    mine = send_parts(call(spread, "sum_spread", (send_parts(pair),), (), [packed_grads], [], [], 10**6)[0])
    weights = [pltpu.VMEM((2,) + PAR_SHAPES[n], F32) for n in ("qw", "pw", "uw", "dw")]
    grads = pl.pallas_call(
        unpack,
        in_specs=[VMEM, VMEM],
        out_specs=[FAR if n in WEIGHTS else VMEM for n in PAR_NAMES],
        out_shape=[shaped(p.shape, F32) for p in params],
        scratch_shapes=weights + [pltpu.SemaphoreType.DMA((8,))],
        name="unpack",
        compiler_params=pltpu.CompilerParams(vmem_limit_bytes=30 * 2**20),
    )(near(mine), near(swap(mine)))
    grads = list(grads)
    grads[4] = grads[4].transpose(1, 0, 2)
    grads[11] = grads[11].swapaxes(1, 2)
    return (output, grad, *grads)


def solution(mesh):
    tile = P("rows", "cols", None)
    return jax.shard_map(
        per_device,
        mesh=mesh,
        in_specs=(tile, tile) + (P(),) * 13,
        out_specs=(tile, tile) + (P(),) * 13,
        check_vma=False,
    )
```

```python
import functools

import jax
import jax.numpy as jnp
from jax import lax
from jax.experimental import pallas as pl
from jax.experimental.pallas import tpu as pltpu
from jax.sharding import PartitionSpec as P


F32 = jnp.float32
BF16 = jnp.bfloat16
C = 192
HEADS = 6
DIM = 32
MLP = 768
TILE = 16
TOK = TILE * TILE
SPAN = 15
SCALE = DIM**-0.5
EPSILON = 1e-05
FLAT = 3584
SMALL = 3456
MASKED = -1e30


def dot_tn(a, b):
    return lax.dot_general(a, b, (((0,), (0,)), ((), ())), preferred_element_type=F32)


def dot_nn(a, b):
    return lax.dot_general(a, b, (((1,), (0,)), ((), ())), preferred_element_type=F32)


def dot_nt(a, b):
    return lax.dot_general(a, b, (((1,), (1,)), ((), ())), preferred_element_type=F32)


def iota(shape, dim):
    return lax.broadcasted_iota(jnp.int32, shape, dim)


def split3(value):
    high = value.astype(BF16)
    rest = value - high.astype(F32)
    mid = rest.astype(BF16)
    return high, mid, (rest - mid.astype(F32)).astype(BF16)


def window_row(r, wc):
    return ((r // 8) * 2 + wc) * 64 + (r % 8) * 8


def halves():
    return iota((64, 128), 1) < 64


def stack_windows(value, left):
    zero = jnp.zeros_like(value)
    return jnp.concatenate([jnp.where(left, value, zero), jnp.where(left, zero, value)], axis=0).astype(BF16)


def own_window(full, left):
    return jnp.where(left, full[:64], full[64:])


def norm_fwd(x):
    center = x - jnp.mean(x, axis=0, keepdims=True)
    rstd = lax.rsqrt(jnp.mean(center * center, axis=0, keepdims=True) + EPSILON)
    return center * rstd, rstd


def norm_bwd(dn, xhat, rstd, gain):
    dxh = dn * gain
    along = jnp.mean(dxh * xhat, axis=0, keepdims=True)
    return rstd * (dxh - jnp.mean(dxh, axis=0, keepdims=True) - xhat * along)


def spread(lane_q):
    q = lane_q % 64
    return (q // 8) * SPAN + q % 8


VEC_NAMES = ("ng", "nb", "pb", "mg", "mb", "db", "qb", "ub")


def load_columns(vec, par, b):
    for i, name in enumerate(VEC_NAMES):
        n = par[name].shape[-1]
        vec[i : i + 1, 0:n] = par[name][b : b + 1, :]
    return vec[...].T


def position_bias(par, b, table, bias):
    table[...] = jnp.zeros((8, 256), F32)
    for h in range(HEADS):
        table[h : h + 1, 0 : SPAN * SPAN] = par["rel"][h, b : b + 1, :]
    select = (iota((128, 128), 0) == spread(iota((128, 128), 1))).astype(BF16)
    for h in range(HEADS):
        row = jnp.broadcast_to(table[h : h + 1, :], (8, 256))
        rows = []
        for ky in range(8):
            shift = (249 - SPAN * (7 - ky)) % 256
            rows.append(pltpu.roll(row, shift, 1, stride=1, stride_axis=0)[:, 0:128])
        high, mid, low = split3(jnp.concatenate(rows, axis=0))
        bias[h] = dot_nn(high, select) + (dot_nn(mid, select) + dot_nn(low, select))


def same_zone(p, last_row, last_col):
    k = iota((64, 128), 0)
    lane = iota((64, 128), 1)
    q = lane % 64
    rows = ((q // 8) < 4) == ((k // 8) < 4)
    cols = ((q % 8) < 4) == ((k % 8) < 4)
    keep = jnp.logical_or(cols, jnp.logical_or(lane < 64, jnp.logical_not(last_col)))
    if p == 1:
        keep = jnp.logical_and(keep, jnp.logical_or(rows, jnp.logical_not(last_row)))
    return keep


def forward(x, par, need, cols, bias, res, zones, keep):
    left = halves()
    xhat, _ = norm_fwd(x)
    normed = (xhat * cols[0:C, 0:1] + cols[0:C, 1:2]).astype(BF16)
    need("qw")
    res["packed"][...] = (dot_tn(par["qw"][...], normed) + cols[0:576, 6:7]).astype(BF16)
    for p in range(2):
        lanes = slice(128 * p, 128 * p + 128)
        for h in range(HEADS):
            q = res["packed"][DIM * h : DIM * h + DIM, lanes]
            k = res["packed"][C + DIM * h : C + DIM * h + DIM, lanes]
            v = res["packed"][2 * C + DIM * h : 2 * C + DIM * h + DIM, lanes]
            s = own_window(dot_tn(k, q), left) * SCALE + bias[h]
            if zones is not None:
                s = jnp.where(zones[p], s, MASKED)
            e = jnp.exp(s - jnp.max(s, axis=0, keepdims=True))
            a = e * (1.0 / jnp.sum(e, axis=0, keepdims=True))
            res["attn"][p * HEADS + h] = a.astype(BF16)
            res["mixed"][DIM * h : DIM * h + DIM, lanes] = dot_nn(v, stack_windows(a, left)).astype(BF16)
    keep("packed")
    need("pw")
    middle = x + dot_tn(par["pw"][...], res["mixed"][...]) + cols[0:C, 2:3]
    res["middle"][...] = middle.astype(BF16)
    middle = res["middle"][...].astype(F32)
    xhat, _ = norm_fwd(middle)
    normed = (xhat * cols[0:C, 3:4] + cols[0:C, 4:5]).astype(BF16)
    keep("attn", "mixed")
    need("uw")
    for i in range(0, MLP, 128):
        u = dot_tn(par["uw"][:, i : i + 128], normed) + cols[i : i + 128, 7:8]
        half = 0.5 + 0.5 * lax.erf(u * (0.5**0.5))
        res["hidden"][i : i + 128, :] = (u * half).astype(BF16)
        res["slope"][i : i + 128, :] = (half + u * (jnp.exp(-0.5 * u * u) * 0.3989422804014327)).astype(BF16)
    keep("middle")
    need("dw")
    out = middle + dot_nn(par["dw"][...], res["hidden"][...]) + cols[0:C, 5:6]
    return out.astype(BF16)


def put_row(small, at, row):
    n = row.shape[-1]
    for i in range(0, n, 128):
        w = min(128, n - i)
        small[at + i // 128 : at + i // 128 + 1, 0:w] = row[0:1, i : i + w]


def put_pairs(flat, at, lhs, rhs, n):
    for i in range(0, n, 256):
        wide = dot_nt(lhs, rhs[i : i + 256, :]).astype(BF16)
        for j in range(0, 256, 128):
            first = at + C * ((i + j) // 128)
            flat[first : first + C, :] = wide[:, j : j + 128]


def mlp_grads(g, flat, small):
    ones = jnp.ones((8, TOK), BF16)
    small[...] = jnp.zeros(small.shape, F32)
    put_row(small, 21, dot_nt(ones, g["dout"][...]))
    put_row(small, 15, dot_nt(ones, g["du"][...]))
    put_row(small, 13, dot_nt(ones, g["dn2"][...]))
    put_row(small, 11, dot_nt(ones, g["dg2"][...]))
    put_pairs(flat, 1152, g["n2"][...], g["du"], MLP)
    put_pairs(flat, 2304, g["dout"][...], g["hidden"], MLP)


def attention_grads(g, flat, small):
    ones = jnp.ones((8, TOK), BF16)
    none = jnp.zeros((64, TOK), BF16)
    put_row(small, 9, dot_nt(ones, g["dmid"][...]))
    flat[960:1152, :] = dot_nt(g["mixed"][...], g["dmid"][0:128, :]).astype(BF16)
    mirror = ((127 - iota((128, 128), 0)) == spread(iota((128, 128), 1))).astype(BF16)
    for h in range(HEADS):
        high, mid, _ = split3(g["rel"][h])
        back = dot_nt(high, mirror) + dot_nt(mid, mirror)
        total = jnp.zeros((8, 256), F32)
        for ky in range(8):
            wide = jnp.concatenate([back[8 * ky : 8 * ky + 8], jnp.zeros((8, 128), F32)], axis=1)
            total = total + pltpu.roll(wide, 121 - SPAN * (7 - ky), 1, stride=1, stride_axis=0)
        total = jnp.sum(total, axis=0, keepdims=True)
        small[24 + h : 25 + h, :] = total[:, 0:128]
        small[32 + h : 33 + h, :] = total[:, 128:256]
    put_pairs(flat, 0, g["n1"][...], g["dpacked"], 512)
    tail = dot_nt(g["n1"][...], jnp.concatenate([g["dpacked"][512:576, :], none], axis=0))
    tail = tail + dot_nt(g["mixed"][...], jnp.concatenate([none, g["dmid"][128:192, :]], axis=0))
    flat[768:960, :] = tail.astype(BF16)
    put_row(small, 4, dot_nt(ones, g["dpacked"][...]))
    put_row(small, 2, dot_nt(ones, g["dn1"][...]))
    put_row(small, 0, dot_nt(ones, g["dg1"][...]))
    flat[SMALL : SMALL + 48, :] = small[...].astype(BF16)
    flat[SMALL + 48 : FLAT, :] = jnp.zeros((FLAT - SMALL - 48, 128), BF16)


def backward(x, par, need, cols, res, g, after_mlp):
    left = halves()
    dout = g["dout"][...]
    need("dw", "slope")
    for i in range(0, MLP, 128):
        dh = dot_tn(par["dw"][:, i : i + 128], dout).astype(BF16).astype(F32)
        g["du"][i : i + 128, :] = (dh * res["slope"][i : i + 128, :].astype(F32)).astype(BF16)
    need("middle", "uw")
    xhat, rstd = norm_fwd(res["middle"][...].astype(F32))
    g["n2"][...] = (xhat * cols[0:C, 3:4] + cols[0:C, 4:5]).astype(BF16)
    dn = dot_nn(par["uw"][...], g["du"][...]).astype(BF16)
    g["dn2"][...] = dn
    dn = dn.astype(F32)
    g["dg2"][...] = (dn * xhat).astype(BF16)
    dmid = (dout.astype(F32) + norm_bwd(dn, xhat, rstd, cols[0:C, 3:4])).astype(BF16)
    g["dmid"][...] = dmid
    after_mlp()
    need("pw", "mixed")
    dmixed = dot_nn(par["pw"][...], dmid).astype(BF16)
    need("packed", "attn")
    for h in range(HEADS):
        drel = None
        for p in range(2):
            lanes = slice(128 * p, 128 * p + 128)
            q = res["packed"][DIM * h : DIM * h + DIM, lanes]
            k = res["packed"][C + DIM * h : C + DIM * h + DIM, lanes]
            v = res["packed"][2 * C + DIM * h : 2 * C + DIM * h + DIM, lanes]
            a = res["attn"][p * HEADS + h].astype(F32)
            dm = dmixed[DIM * h : DIM * h + DIM, lanes]
            da = own_window(dot_tn(v, dm), left).astype(BF16).astype(F32)
            ds = a * (da - jnp.sum(da * a, axis=0, keepdims=True))
            drel = ds if drel is None else drel + ds
            wide = stack_windows(ds * SCALE, left)
            g["dpacked"][DIM * h : DIM * h + DIM, lanes] = dot_nn(k, wide).astype(BF16)
            g["dpacked"][C + DIM * h : C + DIM * h + DIM, lanes] = dot_nt(q, wide).astype(BF16)
            dv = dot_nt(dm, stack_windows(a, left)).astype(BF16)
            g["dpacked"][2 * C + DIM * h : 2 * C + DIM * h + DIM, lanes] = dv
        g["rel"][h] = drel
    xhat, rstd = norm_fwd(x)
    g["n1"][...] = (xhat * cols[0:C, 0:1] + cols[0:C, 1:2]).astype(BF16)
    need("qw")
    dn = dot_nn(par["qw"][...], g["dpacked"][...]).astype(BF16)
    g["dn1"][...] = dn
    dn = dn.astype(F32)
    g["dg1"][...] = (dn * xhat).astype(BF16)
    return dmid.astype(F32) + norm_bwd(dn, xhat, rstd, cols[0:C, 0:1])


def to_channels(pieces):
    return jnp.concatenate(pieces, axis=0).T[0:C]


def to_tokens(value):
    return jnp.concatenate([value, jnp.zeros((64, TOK), F32)], axis=0).T


def grid_put(grid, tokens):
    for r in range(TILE):
        for wc in range(2):
            at = window_row(r, wc)
            grid[r, 8 * wc : 8 * wc + 8, :] = tokens[at : at + 8]


def grid_get(grid, row_at, col_at):
    pieces = []
    for wr in range(2):
        for wc in range(2):
            for ir in range(8):
                at = col_at + 8 * wc
                pieces.append(grid[row_at + 8 * wr + ir, at : at + 8, :])
    return pieces


def emit_strips(grid, edge, strips, which, row_at, col_at):
    col_out, row_out, corner_out = strips
    for r in range(TILE):
        edge[4 * r : 4 * r + 4, :] = grid[r, col_at : col_at + 4, :]
    col_out[64 * which : 64 * which + 64, :] = edge[:, 0:C].astype(BF16)
    for r in range(4):
        row_out[64 * which + 16 * r : 64 * which + 16 * r + 16, :] = grid[row_at + r, 0:TILE, 0:C].astype(BF16)
    for r in range(4):
        edge[4 * r : 4 * r + 4, :] = grid[row_at + r, col_at : col_at + 4, :]
    corner_out[16 * which : 16 * which + 16, :] = edge[0:16, 0:C].astype(BF16)


def fill_grid(grid, edge, own, strips, which, own_row, own_col, strip_row, strip_col):
    col_in, row_in, corner_in = strips
    for r in range(TILE):
        grid[own_row + r, own_col : own_col + TILE, 0:C] = own[r].astype(F32)
    edge[:, 0:C] = col_in[64 * which : 64 * which + 64, :].astype(F32)
    for r in range(TILE):
        grid[own_row + r, strip_col : strip_col + 4, :] = edge[4 * r : 4 * r + 4, :]
    for r in range(4):
        at = 64 * which + 16 * r
        grid[strip_row + r, own_col : own_col + TILE, 0:C] = row_in[at : at + 16, :].astype(F32)
    edge[0:16, 0:C] = corner_in[16 * which : 16 * which + 16, :].astype(F32)
    for r in range(4):
        grid[strip_row + r, strip_col : strip_col + 4, :] = edge[4 * r : 4 * r + 4, :]


PAR_NAMES = ("ng", "nb", "qw", "qb", "rel", "pw", "pb", "mg", "mb", "uw", "ub", "dw", "db")
RES_NAMES = ("packed", "attn", "mixed", "middle", "hidden", "slope")
GRAD_NAMES = ("dout", "n1", "n2", "dmid", "dn1", "dn2", "dg1", "dg2", "du", "dpacked", "rel")
GRAD_SHAPES = ((C, TOK),) * 8 + ((MLP, TOK), (576, TOK), (HEADS, 64, 128))
RES_SHAPES = ((576, TOK), (12, 64, 128), (C, TOK), (C, TOK), (MLP, TOK), (MLP, TOK))


class Copies:
    def __init__(self, sems):
        self.sems = sems
        self.used = 0
        self.open = {}

    def start(self, name, source, target):
        self.open[name] = pltpu.make_async_copy(source, target, self.sems.at[self.used])
        self.open[name].start()
        self.used += 1

    def __call__(self, *names):
        for name in names:
            if name in self.open:
                self.open.pop(name).wait()

    def rest(self):
        self(*list(self.open))


def start_params(copies, names, far, par, b):
    for name in names:
        source = far[name].at[b] if name in WEIGHTS else far[name]
        copies.start(name, source, par[name])


WEIGHTS = ("qw", "pw", "uw", "dw")
PAR_SHAPES = dict(
    ng=(2, C), nb=(2, C), qw=(C, 3 * C), qb=(2, 3 * C), rel=(HEADS, 2, SPAN * SPAN), pw=(C, C), pb=(2, C),
    mg=(2, C), mb=(2, C), uw=(C, MLP), ub=(2, MLP), dw=(C, MLP), db=(2, C),
)


def nothing(*_):
    pass


def first_forward(*refs):
    imagery_far, cotangent_far = refs[0:2]
    far = dict(zip(PAR_NAMES, refs[2:15]))
    own = refs[15]
    strips = refs[16:19]
    xt_far = refs[19]
    res_far = dict(zip(RES_NAMES, refs[20:26]))
    grid, edge, vec, table, bias, sems = refs[26:32]
    par = dict(zip(PAR_NAMES, refs[32:45]))
    res = dict(zip(RES_NAMES, refs[45:51]))
    imagery, cotangent, xt = refs[51:]
    need = Copies(sems)
    need.start("imagery", imagery_far, imagery)
    start_params(need, VEC_NAMES, far, par, 0)
    start_params(need, ("qw", "rel", "pw"), far, par, 0)
    need.start("cotangent", cotangent_far, cotangent)
    start_params(need, ("uw", "dw"), far, par, 0)

    def keep(*names):
        for name in names:
            need.start("out " + name, res[name], res_far[name])

    need("imagery")
    for r in range(TILE):
        grid[r, 0:TILE, 0:C] = imagery[r].astype(F32)
    x = to_channels(grid_get(grid, 0, 0))
    xt[...] = x.astype(BF16)
    need(*VEC_NAMES)
    cols = load_columns(vec, par, 0)
    need("rel")
    position_bias(par, 0, table, bias)
    need("cotangent")
    for r in range(TILE):
        grid[r, 0:TILE, 0:C] = cotangent[r].astype(F32)
    emit_strips(grid, edge, strips, 1, 0, 0)
    need.start("out xt", xt, xt_far)
    out = forward(x, par, need, cols, bias, res, None, keep)
    grid_put(grid, to_tokens(out.astype(F32)))
    keep("hidden", "slope")
    for r in range(TILE):
        own[r] = grid[r, 0:TILE, 0:C].astype(BF16)
    emit_strips(grid, edge, strips, 0, 0, 0)
    need.rest()


def second_block(*refs):
    own_in = refs[0]
    strips_in = refs[1:4]
    cotangent_far = refs[4]
    far = dict(zip(PAR_NAMES, refs[5:18]))
    out_own, back_own = refs[18:20]
    strips = refs[20:23]
    g = dict(zip(GRAD_NAMES + ("hidden", "mixed"), refs[23:36]))
    grid, edge, vec, table, bias, sems = refs[36:42]
    par = dict(zip(PAR_NAMES, refs[42:55]))
    res = dict(zip(("packed", "attn", "middle", "slope"), refs[55:59]), hidden=g["hidden"], mixed=g["mixed"])
    cotangent = refs[59]
    need = Copies(sems)
    start_params(need, VEC_NAMES, far, par, 1)
    start_params(need, ("rel", "qw", "pw"), far, par, 1)
    need.start("cotangent", cotangent_far, cotangent)
    start_params(need, ("uw", "dw"), far, par, 1)
    last_row = lax.axis_index("rows") == lax.axis_size("rows") - 1
    last_col = lax.axis_index("cols") == lax.axis_size("cols") - 1
    zones = [same_zone(p, last_row, last_col) for p in range(2)]
    fill_grid(grid, edge, own_in, strips_in, 0, 0, 0, 16, 16)
    x = to_channels(grid_get(grid, 4, 4))
    need(*VEC_NAMES)
    cols = load_columns(vec, par, 1)
    need("rel")
    position_bias(par, 1, table, bias)
    need("cotangent")
    fill_grid(grid, edge, cotangent, strips_in, 1, 0, 0, 16, 16)
    g["dout"][...] = to_channels(grid_get(grid, 4, 4)).astype(BF16)
    out = forward(x, par, need, cols, bias, res, zones, nothing)
    grid_put(grid, to_tokens(out.astype(F32)))
    for r in range(TILE):
        out_own[r] = grid[r, 0:TILE, 0:C].astype(BF16)
    emit_strips(grid, edge, strips, 0, 12, 12)
    dx = backward(x, par, need, cols, res, g, nothing)
    grid_put(grid, to_tokens(dx))
    for r in range(TILE):
        back_own[r] = grid[r, 0:TILE, 0:C].astype(BF16)
    emit_strips(grid, edge, strips, 1, 12, 12)
    need.rest()


def second_grads(*refs):
    g = dict(zip(GRAD_NAMES + ("hidden", "mixed"), refs[0:13]))
    flat, small = refs[13:]
    mlp_grads(g, flat, small)
    attention_grads(g, flat, small)


BACK_NAMES = VEC_NAMES + WEIGHTS


def first_backward(*refs):
    back_in = refs[0]
    strips_in = refs[1:4]
    flat_two = refs[4]
    far = dict(zip(BACK_NAMES, refs[5:17]))
    xt_far = refs[17]
    res_far = dict(zip(RES_NAMES, refs[18:24]))
    dx_channels, kept, sent = refs[24:27]
    grid, edge, vec, sems = refs[27:31]
    par = dict(zip(BACK_NAMES, refs[31:43]))
    g = dict(zip(GRAD_NAMES, refs[43:54]))
    res = dict(zip(RES_NAMES, refs[54:60]))
    xt, flat, small = refs[60:]
    g["hidden"] = res["hidden"]
    g["mixed"] = res["mixed"]
    need = Copies(sems)
    start_params(need, ("dw",), far, par, 0)
    need.start("slope", res_far["slope"], res["slope"])
    start_params(need, VEC_NAMES, far, par, 0)
    need.start("middle", res_far["middle"], res["middle"])
    start_params(need, ("uw",), far, par, 0)
    need.start("hidden", res_far["hidden"], res["hidden"])
    need.start("mixed", res_far["mixed"], res["mixed"])
    start_params(need, ("pw",), far, par, 0)
    need.start("packed", res_far["packed"], res["packed"])
    need.start("attn", res_far["attn"], res["attn"])
    start_params(need, ("qw",), far, par, 0)
    need.start("xt", xt_far, xt)
    fill_grid(grid, edge, back_in, strips_in, 1, 4, 8, 0, 4)
    g["dout"][...] = to_channels(grid_get(grid, 0, 4)).astype(BF16)
    need(*VEC_NAMES)
    cols = load_columns(vec, par, 0)
    need("xt")
    x = xt[...].astype(F32)

    def after_mlp():
        need("hidden")
        mlp_grads(g, flat, small)

    dx_channels[...] = backward(x, par, need, cols, res, g, after_mlp).astype(BF16)
    attention_grads(g, flat, small)
    even = lax.axis_index("cols") % 2 == 0
    for at in range(0, FLAT, 256):
        rows = slice(at, at + 256)
        kept[rows, :] = jnp.where(even, flat[rows, :], flat_two[rows, :])
        sent[rows, :] = jnp.where(even, flat_two[rows, :], flat[rows, :])
    need.rest()


def make_tiles(out_own, col_in, row_in, corner_in, dx_channels, output, grad, grid, edge):
    fill_grid(grid, edge, out_own, (col_in, row_in, corner_in), 0, 4, 8, 0, 4)
    for r in range(TILE):
        output[r] = grid[r, 4:20, 0:C].astype(BF16)
    grid_put(grid, to_tokens(dx_channels[...].astype(F32)))
    for r in range(TILE):
        grad[r] = grid[r, 0:TILE, 0:C].astype(BF16)


def add_pair(kept, got, out):
    for at in range(0, FLAT, 256):
        rows = slice(at, at + 256)
        out[rows, :] = (kept[rows, :].astype(F32) + got[rows, :].astype(F32)).astype(BF16)


def sum_spread(share, parts, out):
    total = jnp.zeros((share, 128), F32)
    for at in range(0, FLAT, share):
        total = total + parts[at : at + share, :].astype(F32)
    total = total.astype(BF16)
    for at in range(0, FLAT, share):
        out[at : at + share, :] = total


def unpack_weights(rows, b, near_refs, far_refs, copies):
    qw, pw, uw, dw = near_refs
    for j in range(4):
        qw[:, 128 * j : 128 * j + 128] = rows(C * j, C)
    tail = rows(768, C)
    qw[:, 512:576] = tail[:, 0:64]
    copies.start("qw", qw, far_refs[0].at[b])
    pw[:, 128:192] = pltpu.roll(tail, 64, 1)[:, 0:64]
    pw[:, 0:128] = rows(960, C)
    copies.start("pw", pw, far_refs[1].at[b])
    for j in range(6):
        uw[:, 128 * j : 128 * j + 128] = rows(1152 + C * j, C)
    copies.start("uw", uw, far_refs[2].at[b])
    for j in range(6):
        dw[:, 128 * j : 128 * j + 128] = rows(2304 + C * j, C)
    copies.start("dw", dw, far_refs[3].at[b])


def unpack_mine(mine, *refs):
    copies = Copies(refs[8])
    parity = lax.axis_index("cols") % 2
    unpack_weights(lambda at, n: mine[at : at + n, :].astype(F32) * outs_factor, parity, refs[4:8], refs[0:4], copies)
    copies.rest()


def unpack_rest(mine, other, *refs):
    ng, nb, qw_far, qb, rel, pw_far, pb, mg, mb, uw_far, ub, dw_far, db = refs[4:17]
    copies = Copies(refs[21])
    factor = outs_factor
    parity = lax.axis_index("cols") % 2
    far_refs = (qw_far, pw_far, uw_far, dw_far)
    unpack_weights(lambda at, n: other[at : at + n, :].astype(F32) * factor, 1 - parity, refs[17:21], far_refs, copies)
    flip = (iota((256, 256), 0) + iota((256, 256), 1) == 255).astype(BF16)
    for b in range(2):

        def raw(at, n):
            return jnp.where(parity == b, mine[at : at + n, :], other[at : at + n, :])

        small = raw(SMALL, 48).astype(F32) * factor
        for at, ref in ((0, ng), (2, nb), (4, qb), (9, pb), (11, mg), (13, mb), (15, ub), (21, db)):
            n = ref.shape[-1]
            for i in range(0, n, 128):
                w = min(128, n - i)
                ref[b : b + 1, i : i + w] = small[at + i // 128 : at + i // 128 + 1, 0:w]
        table = jnp.concatenate([raw(SMALL + 24, 8), raw(SMALL + 32, 8)], axis=1)
        table = dot_nn(table, flip) * factor
        for h in range(HEADS):
            rel[h, b : b + 1, :] = table[h : h + 1, 0 : SPAN * SPAN]
    copies.rest()


outs_factor = float(128 * 256) ** (-0.5)


VMEM = pl.BlockSpec(memory_space=pltpu.VMEM)


def near(value):
    return pltpu.with_memory_space_constraint(value, pltpu.VMEM)


FAR = pl.BlockSpec(memory_space=pltpu.HBM)


def call(kernel, args, far_args, outs, far_outs, scratch, flops, plain=()):
    return pl.pallas_call(
        kernel,
        in_specs=[VMEM] * len(args) + [FAR] * len(far_args),
        out_specs=[VMEM] * (len(outs) + len(plain)) + [FAR] * len(far_outs),
        out_shape=list(outs) + list(plain) + [pltpu.HBM(o.shape, o.dtype) for o in far_outs],
        scratch_shapes=scratch,
        compiler_params=pltpu.CompilerParams(vmem_limit_bytes=30 * 2**20),
        cost_estimate=pl.CostEstimate(flops=flops, transcendentals=0, bytes_accessed=4000000),
    )(*[near(a) for a in args], *[pltpu.with_memory_space_constraint(a, pltpu.HBM) for a in far_args])


def shaped(shape, dtype=BF16):
    return jax.ShapeDtypeStruct(shape, dtype)


def exchange(strips, step):
    n_rows = lax.axis_size("rows")
    n_cols = lax.axis_size("cols")
    col_strip, row_strip, corner = strips
    along = [(c, (c + step) % n_cols) for c in range(n_cols)]
    down = [(r, (r + step) % n_rows) for r in range(n_rows)]
    both = [
        (r * n_cols + c, ((r + step) % n_rows) * n_cols + (c + step) % n_cols)
        for r in range(n_rows)
        for c in range(n_cols)
    ]
    return [
        lax.ppermute(col_strip, "cols", along),
        lax.ppermute(row_strip, "rows", down),
        lax.ppermute(corner, ("rows", "cols"), both),
    ]


def swap(value):
    return lax.ppermute(value, "cols", [(c, c ^ 1) for c in range(lax.axis_size("cols"))])


def send_parts(value):
    n_cols = lax.axis_size("cols")
    n = lax.axis_size("rows") * n_cols
    groups = [[d for d in range(n) if d % n_cols % 2 == p] for p in range(2)]
    parts = value.reshape(n // 2, 2 * FLAT // n, 128)
    got = lax.all_to_all(parts, ("rows", "cols"), 0, 0, axis_index_groups=groups, tiled=True)
    return got.reshape(value.shape)


def both_blocks(imagery, cotangent, *params):
    params = list(params)
    params[4] = params[4].transpose(1, 0, 2)
    params[11] = params[11].swapaxes(1, 2)
    tile = (TILE, TILE, C)
    strips = [pltpu.VMEM(s, BF16) for s in ((128, C), (128, C), (32, C))]
    packed_grads = pltpu.VMEM((FLAT, 128), BF16)
    held = pltpu.VMEM(tile, BF16)
    grid = pltpu.VMEM((24, 24, 256), F32)
    edge = pltpu.VMEM((64, 256), F32)
    vec = pltpu.VMEM((128, MLP), F32)
    tables = [pltpu.VMEM((8, 256), F32), pltpu.VMEM((HEADS, 64, 128), F32)]
    par = dict(zip(PAR_NAMES, params))
    par_kinds = {n: BF16 if n in WEIGHTS else F32 for n in PAR_NAMES}
    par_vmem = {n: pltpu.VMEM(PAR_SHAPES[n], par_kinds[n]) for n in PAR_NAMES}
    res_vmem = [pltpu.VMEM(s, BF16) for s in RES_SHAPES]
    sems = pltpu.SemaphoreType.DMA((32,))
    one = call(
        first_forward,
        (),
        (imagery, cotangent, *params),
        [held] + strips,
        [shaped((C, TOK))] + [shaped(s) for s in RES_SHAPES],
        [grid, edge, vec] + tables + [sems] + list(par_vmem.values()) + res_vmem + [held, held, pltpu.VMEM((C, TOK), BF16)],
        5 * 10**9,
    )
    own, got, xt, res = one[0], exchange(one[1:4], -1), one[4], one[5:]
    channels = pltpu.VMEM((C, TOK), BF16)
    grad_vmem = [pltpu.VMEM(s, F32 if n == "rel" else BF16) for n, s in zip(GRAD_NAMES, GRAD_SHAPES)]
    small = pltpu.VMEM((48, 128), F32)
    two = call(
        second_block,
        (own, *got),
        (cotangent, *params),
        [held, held] + strips + grad_vmem + [res_vmem[4], res_vmem[2]],
        [],
        [grid, edge, vec] + tables + [sems] + list(par_vmem.values()) + [res_vmem[i] for i in (0, 1, 3, 5)] + [held],
        10**10,
    )
    got = exchange(two[2:5], 1)
    flat_two = call(second_grads, two[5:], (), [packed_grads], [], [small], 10**9)[0]
    dx, kept, sent = call(
        first_backward,
        (two[1], *got, flat_two),
        (*[par[n] for n in BACK_NAMES], xt, *res),
        [channels, packed_grads, packed_grads],
        [],
        [grid, edge, vec, sems]
        + [par_vmem[n] for n in BACK_NAMES]
        + grad_vmem
        + res_vmem
        + [channels, packed_grads, small],
        5 * 10**9,
    )
    sent = swap(sent)
    tiles = [shaped(tile), shaped(tile)]
    output, grad = call(make_tiles, (two[0], *got, dx), (), [], [], [grid, edge], 10**9, plain=tiles)
    parts = send_parts(call(add_pair, (kept, sent), (), [packed_grads], [], [], 10**6)[0])
    share = 2 * FLAT // (lax.axis_size("rows") * lax.axis_size("cols"))
    spread_sum = functools.partial(sum_spread, share)
    mine = send_parts(call(spread_sum, (parts,), (), [packed_grads], [], [], 10**6)[0])
    weights = [pltpu.VMEM(PAR_SHAPES[n], F32) for n in WEIGHTS]
    weights_far = [pltpu.HBM((2,) + PAR_SHAPES[n], F32) for n in WEIGHTS]
    few_sems = pltpu.SemaphoreType.DMA((4,))
    half = call(unpack_mine, (mine,), (), [], weights_far, weights + [few_sems], 10**9)
    grads = pl.pallas_call(
        unpack_rest,
        in_specs=[VMEM, VMEM] + [FAR] * 4,
        out_specs=[FAR if n in WEIGHTS else VMEM for n in PAR_NAMES],
        out_shape=[pltpu.HBM(p.shape, F32) if n in WEIGHTS else shaped(p.shape, F32) for n, p in zip(PAR_NAMES, params)],
        scratch_shapes=weights + [few_sems],
        input_output_aliases={2: 2, 3: 5, 4: 9, 5: 11},
        name="unpack_rest",
        compiler_params=pltpu.CompilerParams(vmem_limit_bytes=30 * 2**20),
    )(near(mine), near(swap(mine)), *[pltpu.with_memory_space_constraint(h, pltpu.HBM) for h in half])
    grads = list(grads)
    grads[4] = grads[4].transpose(1, 0, 2)
    grads[11] = grads[11].swapaxes(1, 2)
    return (output, grad, *grads)


def solution(mesh):
    tile = P("rows", "cols", None)
    return jax.shard_map(
        both_blocks,
        mesh=mesh,
        in_specs=(tile, tile) + (P(),) * 13,
        out_specs=(tile, tile) + (P(),) * 13,
        check_vma=False,
    )
```

```python
import functools

import jax
import jax.numpy as jnp
from jax import lax
from jax.experimental import pallas as pl
from jax.experimental.pallas import tpu as pltpu
from jax.sharding import PartitionSpec as P


F32 = jnp.float32
BF16 = jnp.bfloat16
C = 192
HEADS = 6
DIM = 32
MLP = 768
TILE = 16
TOK = TILE * TILE
SPAN = 15
SCALE = DIM**-0.5
EPSILON = 1e-05
FLAT = 3584
SMALL = 3456
MASKED = -1e30


def dot_tn(a, b):
    return lax.dot_general(a, b, (((0,), (0,)), ((), ())), preferred_element_type=F32)


def dot_nn(a, b):
    return lax.dot_general(a, b, (((1,), (0,)), ((), ())), preferred_element_type=F32)


def dot_nt(a, b):
    return lax.dot_general(a, b, (((1,), (1,)), ((), ())), preferred_element_type=F32)


def iota(shape, dim):
    return lax.broadcasted_iota(jnp.int32, shape, dim)


def split3(value):
    high = value.astype(BF16)
    rest = value - high.astype(F32)
    mid = rest.astype(BF16)
    return high, mid, (rest - mid.astype(F32)).astype(BF16)


def window_row(r, wc):
    return ((r // 8) * 2 + wc) * 64 + (r % 8) * 8


def halves():
    return iota((64, 128), 1) < 64


def stack_windows(value, left):
    zero = jnp.zeros_like(value)
    return jnp.concatenate([jnp.where(left, value, zero), jnp.where(left, zero, value)], axis=0).astype(BF16)


def own_window(full, left):
    return jnp.where(left, full[:64], full[64:])


def norm_fwd(x):
    center = x - jnp.mean(x, axis=0, keepdims=True)
    rstd = lax.rsqrt(jnp.mean(center * center, axis=0, keepdims=True) + EPSILON)
    return center * rstd, rstd


def norm_bwd(dn, xhat, rstd, gain):
    dxh = dn * gain
    along = jnp.mean(dxh * xhat, axis=0, keepdims=True)
    return rstd * (dxh - jnp.mean(dxh, axis=0, keepdims=True) - xhat * along)


def spread(lane_q):
    q = lane_q % 64
    return (q // 8) * SPAN + q % 8


VEC_NAMES = ("ng", "nb", "pb", "mg", "mb", "db", "qb", "ub")


def load_columns(vec, par, b):
    for i, name in enumerate(VEC_NAMES):
        n = par[name].shape[-1]
        vec[i : i + 1, 0:n] = par[name][b : b + 1, :]
    return vec[...].T


def position_bias(par, b, table, bias):
    table[...] = jnp.zeros((8, 256), F32)
    for h in range(HEADS):
        table[h : h + 1, 0 : SPAN * SPAN] = par["rel"][h, b : b + 1, :]
    select = (iota((128, 128), 0) == spread(iota((128, 128), 1))).astype(BF16)
    for h in range(HEADS):
        row = jnp.broadcast_to(table[h : h + 1, :], (8, 256))
        rows = []
        for ky in range(8):
            shift = (249 - SPAN * (7 - ky)) % 256
            rows.append(pltpu.roll(row, shift, 1, stride=1, stride_axis=0)[:, 0:128])
        high, mid, low = split3(jnp.concatenate(rows, axis=0))
        bias[h] = dot_nn(high, select) + (dot_nn(mid, select) + dot_nn(low, select))


def same_zone(p, last_row, last_col):
    k = iota((64, 128), 0)
    lane = iota((64, 128), 1)
    q = lane % 64
    rows = ((q // 8) < 4) == ((k // 8) < 4)
    cols = ((q % 8) < 4) == ((k % 8) < 4)
    keep = jnp.logical_or(cols, jnp.logical_or(lane < 64, jnp.logical_not(last_col)))
    if p == 1:
        keep = jnp.logical_and(keep, jnp.logical_or(rows, jnp.logical_not(last_row)))
    return keep


def forward(x, par, need, cols, bias, res, zones, keep):
    left = halves()
    xhat, _ = norm_fwd(x)
    normed = (xhat * cols[0:C, 0:1] + cols[0:C, 1:2]).astype(BF16)
    need("qw")
    res["packed"][...] = (dot_tn(par["qw"][...], normed) + cols[0:576, 6:7]).astype(BF16)
    for p in range(2):
        lanes = slice(128 * p, 128 * p + 128)
        for h in range(HEADS):
            q = res["packed"][DIM * h : DIM * h + DIM, lanes]
            k = res["packed"][C + DIM * h : C + DIM * h + DIM, lanes]
            v = res["packed"][2 * C + DIM * h : 2 * C + DIM * h + DIM, lanes]
            s = own_window(dot_tn(k, q), left) * SCALE + bias[h]
            if zones is not None:
                s = jnp.where(zones[p], s, MASKED)
            e = jnp.exp(s - jnp.max(s, axis=0, keepdims=True))
            a = e * (1.0 / jnp.sum(e, axis=0, keepdims=True))
            res["attn"][p * HEADS + h] = a.astype(BF16)
            res["mixed"][DIM * h : DIM * h + DIM, lanes] = dot_nn(v, stack_windows(a, left)).astype(BF16)
    keep("packed")
    need("pw")
    middle = x + dot_tn(par["pw"][...], res["mixed"][...]) + cols[0:C, 2:3]
    res["middle"][...] = middle.astype(BF16)
    middle = res["middle"][...].astype(F32)
    xhat, _ = norm_fwd(middle)
    normed = (xhat * cols[0:C, 3:4] + cols[0:C, 4:5]).astype(BF16)
    keep("attn", "mixed")
    need("uw")
    for i in range(0, MLP, 128):
        u = dot_tn(par["uw"][:, i : i + 128], normed) + cols[i : i + 128, 7:8]
        half = 0.5 + 0.5 * lax.erf(u * (0.5**0.5))
        res["hidden"][i : i + 128, :] = (u * half).astype(BF16)
        res["slope"][i : i + 128, :] = (half + u * (jnp.exp(-0.5 * u * u) * 0.3989422804014327)).astype(BF16)
    keep("middle")
    need("dw")
    out = (middle + dot_nn(par["dw"][...], res["hidden"][...]) + cols[0:C, 5:6]).astype(BF16)
    keep("hidden", "slope")
    return out


def put_row(small, at, row):
    n = row.shape[-1]
    for i in range(0, n, 128):
        w = min(128, n - i)
        small[at + i // 128 : at + i // 128 + 1, 0:w] = row[0:1, i : i + w]


def put_pairs(flat, at, lhs, rhs, n):
    for i in range(0, n, 256):
        wide = dot_nt(lhs, rhs[i : i + 256, :]).astype(BF16)
        for j in range(0, 256, 128):
            first = at + C * ((i + j) // 128)
            flat[first : first + C, :] = wide[:, j : j + 128]


def mlp_grads(g, flat, small):
    ones = jnp.ones((8, TOK), BF16)
    small[...] = jnp.zeros(small.shape, F32)
    put_row(small, 21, dot_nt(ones, g["dout"][...]))
    put_row(small, 15, dot_nt(ones, g["du"][...]))
    put_row(small, 13, dot_nt(ones, g["dn2"][...]))
    put_row(small, 11, dot_nt(ones, g["dg2"][...]))
    put_pairs(flat, 1152, g["n2"][...], g["du"], MLP)
    put_pairs(flat, 2304, g["dout"][...], g["hidden"], MLP)


def attention_grads(g, flat, small):
    ones = jnp.ones((8, TOK), BF16)
    none = jnp.zeros((64, TOK), BF16)
    put_row(small, 9, dot_nt(ones, g["dmid"][...]))
    flat[960:1152, :] = dot_nt(g["mixed"][...], g["dmid"][0:128, :]).astype(BF16)
    mirror = ((127 - iota((128, 128), 0)) == spread(iota((128, 128), 1))).astype(BF16)
    for h in range(HEADS):
        high, mid, _ = split3(g["rel"][h])
        back = dot_nt(high, mirror) + dot_nt(mid, mirror)
        total = jnp.zeros((8, 256), F32)
        for ky in range(8):
            wide = jnp.concatenate([back[8 * ky : 8 * ky + 8], jnp.zeros((8, 128), F32)], axis=1)
            total = total + pltpu.roll(wide, 121 - SPAN * (7 - ky), 1, stride=1, stride_axis=0)
        total = jnp.sum(total, axis=0, keepdims=True)
        small[24 + h : 25 + h, :] = total[:, 0:128]
        small[32 + h : 33 + h, :] = total[:, 128:256]
    put_pairs(flat, 0, g["n1"][...], g["dpacked"], 512)
    tail = dot_nt(g["n1"][...], jnp.concatenate([g["dpacked"][512:576, :], none], axis=0))
    tail = tail + dot_nt(g["mixed"][...], jnp.concatenate([none, g["dmid"][128:192, :]], axis=0))
    flat[768:960, :] = tail.astype(BF16)
    put_row(small, 4, dot_nt(ones, g["dpacked"][...]))
    put_row(small, 2, dot_nt(ones, g["dn1"][...]))
    put_row(small, 0, dot_nt(ones, g["dg1"][...]))
    flat[SMALL : SMALL + 48, :] = small[...].astype(BF16)
    flat[SMALL + 48 : FLAT, :] = jnp.zeros((FLAT - SMALL - 48, 128), BF16)


def backward(x, par, need, cols, res, g, after_mlp):
    left = halves()
    dout = g["dout"][...]
    need("dw", "slope")
    for i in range(0, MLP, 128):
        dh = dot_tn(par["dw"][:, i : i + 128], dout).astype(BF16).astype(F32)
        g["du"][i : i + 128, :] = (dh * res["slope"][i : i + 128, :].astype(F32)).astype(BF16)
    need("middle", "uw")
    xhat, rstd = norm_fwd(res["middle"][...].astype(F32))
    g["n2"][...] = (xhat * cols[0:C, 3:4] + cols[0:C, 4:5]).astype(BF16)
    dn = dot_nn(par["uw"][...], g["du"][...]).astype(BF16)
    g["dn2"][...] = dn
    dn = dn.astype(F32)
    g["dg2"][...] = (dn * xhat).astype(BF16)
    dmid = (dout.astype(F32) + norm_bwd(dn, xhat, rstd, cols[0:C, 3:4])).astype(BF16)
    g["dmid"][...] = dmid
    after_mlp()
    need("pw", "mixed")
    dmixed = dot_nn(par["pw"][...], dmid).astype(BF16)
    need("packed", "attn")
    for h in range(HEADS):
        drel = None
        for p in range(2):
            lanes = slice(128 * p, 128 * p + 128)
            q = res["packed"][DIM * h : DIM * h + DIM, lanes]
            k = res["packed"][C + DIM * h : C + DIM * h + DIM, lanes]
            v = res["packed"][2 * C + DIM * h : 2 * C + DIM * h + DIM, lanes]
            a = res["attn"][p * HEADS + h].astype(F32)
            dm = dmixed[DIM * h : DIM * h + DIM, lanes]
            da = own_window(dot_tn(v, dm), left).astype(BF16).astype(F32)
            ds = a * (da - jnp.sum(da * a, axis=0, keepdims=True))
            drel = ds if drel is None else drel + ds
            wide = stack_windows(ds * SCALE, left)
            g["dpacked"][DIM * h : DIM * h + DIM, lanes] = dot_nn(k, wide).astype(BF16)
            g["dpacked"][C + DIM * h : C + DIM * h + DIM, lanes] = dot_nt(q, wide).astype(BF16)
            dv = dot_nt(dm, stack_windows(a, left)).astype(BF16)
            g["dpacked"][2 * C + DIM * h : 2 * C + DIM * h + DIM, lanes] = dv
        g["rel"][h] = drel
    need("xt")
    xhat, rstd = norm_fwd(x[...].astype(F32))
    g["n1"][...] = (xhat * cols[0:C, 0:1] + cols[0:C, 1:2]).astype(BF16)
    need("qw")
    dn = dot_nn(par["qw"][...], g["dpacked"][...]).astype(BF16)
    g["dn1"][...] = dn
    dn = dn.astype(F32)
    g["dg1"][...] = (dn * xhat).astype(BF16)
    return dmid.astype(F32) + norm_bwd(dn, xhat, rstd, cols[0:C, 0:1])


def to_channels(pieces):
    return jnp.concatenate(pieces, axis=0).T[0:C]


def to_tokens(value):
    return jnp.concatenate([value, jnp.zeros((64, TOK), F32)], axis=0).T


def grid_put(grid, tokens):
    for r in range(TILE):
        for wc in range(2):
            at = window_row(r, wc)
            grid[r, 8 * wc : 8 * wc + 8, :] = tokens[at : at + 8]


def grid_get(grid, row_at, col_at):
    pieces = []
    for wr in range(2):
        for wc in range(2):
            for ir in range(8):
                at = col_at + 8 * wc
                pieces.append(grid[row_at + 8 * wr + ir, at : at + 8, :])
    return pieces


def emit_strips(grid, edge, strips, which, row_at, col_at):
    col_out, row_out, corner_out = strips
    for r in range(TILE):
        edge[4 * r : 4 * r + 4, :] = grid[r, col_at : col_at + 4, :]
    col_out[64 * which : 64 * which + 64, :] = edge[:, 0:C].astype(BF16)
    for r in range(4):
        row_out[64 * which + 16 * r : 64 * which + 16 * r + 16, :] = grid[row_at + r, 0:TILE, 0:C].astype(BF16)
    for r in range(4):
        edge[4 * r : 4 * r + 4, :] = grid[row_at + r, col_at : col_at + 4, :]
    corner_out[16 * which : 16 * which + 16, :] = edge[0:16, 0:C].astype(BF16)


def fill_grid(grid, edge, own, strips, which, own_row, own_col, strip_row, strip_col):
    col_in, row_in, corner_in = strips
    for r in range(TILE):
        grid[own_row + r, own_col : own_col + TILE, 0:C] = own[r].astype(F32)
    edge[:, 0:C] = col_in[64 * which : 64 * which + 64, :].astype(F32)
    for r in range(TILE):
        grid[own_row + r, strip_col : strip_col + 4, :] = edge[4 * r : 4 * r + 4, :]
    for r in range(4):
        at = 64 * which + 16 * r
        grid[strip_row + r, own_col : own_col + TILE, 0:C] = row_in[at : at + 16, :].astype(F32)
    edge[0:16, 0:C] = corner_in[16 * which : 16 * which + 16, :].astype(F32)
    for r in range(4):
        grid[strip_row + r, strip_col : strip_col + 4, :] = edge[4 * r : 4 * r + 4, :]


PAR_NAMES = ("ng", "nb", "qw", "qb", "rel", "pw", "pb", "mg", "mb", "uw", "ub", "dw", "db")
RES_NAMES = ("packed", "attn", "mixed", "middle", "hidden", "slope")
GRAD_NAMES = ("dout", "n1", "n2", "dmid", "dn1", "dn2", "dg1", "dg2", "du", "dpacked", "rel")
GRAD_SHAPES = ((C, TOK),) * 8 + ((MLP, TOK), (576, TOK), (HEADS, 64, 128))
RES_SHAPES = ((576, TOK), (12, 64, 128), (C, TOK), (C, TOK), (MLP, TOK), (MLP, TOK))


class Copies:
    def __init__(self, sems):
        self.sems = sems
        self.used = 0
        self.open = {}

    def start(self, name, source, target):
        self.open[name] = pltpu.make_async_copy(source, target, self.sems.at[self.used])
        self.open[name].start()
        self.used += 1

    def __call__(self, *names):
        for name in names:
            if name in self.open:
                self.open.pop(name).wait()

    def rest(self):
        self(*list(self.open))


def start_params(copies, names, far, par, b):
    for name in names:
        source = far[name].at[b] if name in WEIGHTS else far[name]
        copies.start(name, source, par[name])


WEIGHTS = ("qw", "pw", "uw", "dw")
PAR_SHAPES = dict(
    ng=(2, C), nb=(2, C), qw=(C, 3 * C), qb=(2, 3 * C), rel=(HEADS, 2, SPAN * SPAN), pw=(C, C), pb=(2, C),
    mg=(2, C), mb=(2, C), uw=(C, MLP), ub=(2, MLP), dw=(C, MLP), db=(2, C),
)


def nothing(*_):
    pass


def first_forward(*refs):
    imagery_far, cotangent_far = refs[0:2]
    far = dict(zip(PAR_NAMES, refs[2:15]))
    own = refs[15]
    strips = refs[16:19]
    xt_far = refs[19]
    res_far = dict(zip(RES_NAMES, refs[20:26]))
    grid, edge, vec, table, bias, sems = refs[26:32]
    par = dict(zip(PAR_NAMES, refs[32:45]))
    res = dict(zip(RES_NAMES, refs[45:51]))
    imagery, cotangent, xt = refs[51:]
    need = Copies(sems)
    need.start("imagery", imagery_far, imagery)
    start_params(need, VEC_NAMES, far, par, 0)
    start_params(need, ("qw", "rel", "pw"), far, par, 0)
    need.start("cotangent", cotangent_far, cotangent)
    start_params(need, ("uw", "dw"), far, par, 0)

    def keep(*names):
        for name in names:
            need.start("out " + name, res[name], res_far[name])

    need("imagery")
    for r in range(TILE):
        grid[r, 0:TILE, 0:C] = imagery[r].astype(F32)
    x = to_channels(grid_get(grid, 0, 0))
    xt[...] = x.astype(BF16)
    need(*VEC_NAMES, "rel", "qw", "pw", "cotangent")
    cols = load_columns(vec, par, 0)
    position_bias(par, 0, table, bias)
    for r in range(TILE):
        grid[r, 0:TILE, 0:C] = cotangent[r].astype(F32)
    emit_strips(grid, edge, strips, 1, 0, 0)
    need.start("out xt", xt, xt_far)
    out = forward(x, par, need, cols, bias, res, None, keep)
    grid_put(grid, to_tokens(out.astype(F32)))
    for r in range(TILE):
        own[r] = grid[r, 0:TILE, 0:C].astype(BF16)
    emit_strips(grid, edge, strips, 0, 0, 0)
    need.rest()


def second_block(*refs):
    own_in = refs[0]
    strips_in = refs[1:4]
    cotangent_far = refs[4]
    far = dict(zip(PAR_NAMES, refs[5:18]))
    out_own, back_own = refs[18:20]
    strips = refs[20:23]
    g = dict(zip(GRAD_NAMES + ("hidden", "mixed"), refs[23:36]))
    grid, edge, vec, table, bias, sems = refs[36:42]
    par = dict(zip(PAR_NAMES, refs[42:55]))
    res = dict(zip(("packed", "attn", "middle", "slope"), refs[55:59]), hidden=g["hidden"], mixed=g["mixed"])
    cotangent, xt = refs[59:]
    need = Copies(sems)
    start_params(need, VEC_NAMES + ("rel",), far, par, 1)
    need.start("cotangent", cotangent_far, cotangent)
    start_params(need, ("qw", "pw", "uw", "dw"), far, par, 1)
    last_row = lax.axis_index("rows") == lax.axis_size("rows") - 1
    last_col = lax.axis_index("cols") == lax.axis_size("cols") - 1
    zones = [same_zone(p, last_row, last_col) for p in range(2)]
    fill_grid(grid, edge, own_in, strips_in, 0, 0, 0, 16, 16)
    x = to_channels(grid_get(grid, 4, 4))
    xt[...] = x.astype(BF16)
    need(*VEC_NAMES, "rel", "cotangent")
    cols = load_columns(vec, par, 1)
    position_bias(par, 1, table, bias)
    fill_grid(grid, edge, cotangent, strips_in, 1, 0, 0, 16, 16)
    g["dout"][...] = to_channels(grid_get(grid, 4, 4)).astype(BF16)
    out = forward(x, par, need, cols, bias, res, zones, nothing)
    grid_put(grid, to_tokens(out.astype(F32)))
    for r in range(TILE):
        out_own[r] = grid[r, 0:TILE, 0:C].astype(BF16)
    emit_strips(grid, edge, strips, 0, 12, 12)
    dx = backward(xt, par, need, cols, res, g, nothing)
    grid_put(grid, to_tokens(dx))
    for r in range(TILE):
        back_own[r] = grid[r, 0:TILE, 0:C].astype(BF16)
    emit_strips(grid, edge, strips, 1, 12, 12)
    need.rest()


def second_grads(*refs):
    g = dict(zip(GRAD_NAMES + ("hidden", "mixed"), refs[0:13]))
    flat, small = refs[13:]
    mlp_grads(g, flat, small)
    attention_grads(g, flat, small)


BACK_NAMES = VEC_NAMES + WEIGHTS


def first_backward(*refs):
    back_in = refs[0]
    strips_in = refs[1:4]
    flat_two = refs[4]
    far = dict(zip(BACK_NAMES, refs[5:17]))
    xt_far = refs[17]
    res_far = dict(zip(RES_NAMES, refs[18:24]))
    dx_channels, kept, sent = refs[24:27]
    grid, edge, vec, sems = refs[27:31]
    par = dict(zip(BACK_NAMES, refs[31:43]))
    g = dict(zip(GRAD_NAMES, refs[43:54]))
    res = dict(zip(RES_NAMES, refs[54:60]))
    xt, flat, small = refs[60:]
    g["hidden"] = res["hidden"]
    g["mixed"] = res["mixed"]
    need = Copies(sems)
    start_params(need, ("dw",), far, par, 0)
    need.start("slope", res_far["slope"], res["slope"])
    start_params(need, VEC_NAMES, far, par, 0)
    need.start("middle", res_far["middle"], res["middle"])
    start_params(need, ("uw",), far, par, 0)
    need.start("hidden", res_far["hidden"], res["hidden"])
    need.start("mixed", res_far["mixed"], res["mixed"])
    start_params(need, ("pw",), far, par, 0)
    need.start("packed", res_far["packed"], res["packed"])
    need.start("attn", res_far["attn"], res["attn"])
    need.start("xt", xt_far, xt)
    start_params(need, ("qw",), far, par, 0)
    fill_grid(grid, edge, back_in, strips_in, 1, 4, 8, 0, 4)
    g["dout"][...] = to_channels(grid_get(grid, 0, 4)).astype(BF16)
    need(*VEC_NAMES)
    cols = load_columns(vec, par, 0)

    def after_mlp():
        need("hidden")
        mlp_grads(g, flat, small)

    dx_channels[...] = backward(xt, par, need, cols, res, g, after_mlp).astype(BF16)
    attention_grads(g, flat, small)
    even = lax.axis_index("cols") % 2 == 0
    for at in range(0, FLAT, 256):
        rows = slice(at, at + 256)
        kept[rows, :] = jnp.where(even, flat[rows, :], flat_two[rows, :])
        sent[rows, :] = jnp.where(even, flat_two[rows, :], flat[rows, :])
    need.rest()


def make_tiles(out_own, col_in, row_in, corner_in, dx_channels, output, grad, grid, edge):
    fill_grid(grid, edge, out_own, (col_in, row_in, corner_in), 0, 4, 8, 0, 4)
    for r in range(TILE):
        output[r] = grid[r, 4:20, 0:C].astype(BF16)
    grid_put(grid, to_tokens(dx_channels[...].astype(F32)))
    for r in range(TILE):
        grad[r] = grid[r, 0:TILE, 0:C].astype(BF16)


def add_pair(kept, got, out):
    for at in range(0, FLAT, 256):
        rows = slice(at, at + 256)
        out[rows, :] = (kept[rows, :].astype(F32) + got[rows, :].astype(F32)).astype(BF16)


def sum_spread(share, parts, out):
    total = jnp.zeros((share, 128), F32)
    for at in range(0, FLAT, share):
        total = total + parts[at : at + share, :].astype(F32)
    total = total.astype(BF16)
    for at in range(0, FLAT, share):
        out[at : at + share, :] = total


def unpack_weights(rows, b, near_refs, far_refs, copies):
    qw, pw, uw, dw = near_refs
    for j in range(4):
        qw[:, 128 * j : 128 * j + 128] = rows(C * j, C)
    tail = rows(768, C)
    qw[:, 512:576] = tail[:, 0:64]
    copies.start("qw", qw, far_refs[0].at[b])
    pw[:, 128:192] = pltpu.roll(tail, 64, 1)[:, 0:64]
    pw[:, 0:128] = rows(960, C)
    copies.start("pw", pw, far_refs[1].at[b])
    for j in range(6):
        uw[:, 128 * j : 128 * j + 128] = rows(1152 + C * j, C)
    copies.start("uw", uw, far_refs[2].at[b])
    for j in range(6):
        dw[:, 128 * j : 128 * j + 128] = rows(2304 + C * j, C)
    copies.start("dw", dw, far_refs[3].at[b])


def unpack_mine(mine, *refs):
    copies = Copies(refs[8])
    parity = lax.axis_index("cols") % 2
    unpack_weights(lambda at, n: mine[at : at + n, :].astype(F32) * outs_factor, parity, refs[4:8], refs[0:4], copies)
    copies.rest()


def unpack_rest(mine, other, *refs):
    far = dict(zip(PAR_NAMES, refs[4:17]))
    near_refs = dict(zip(PAR_NAMES, refs[17:30]))
    copies = Copies(refs[30])
    factor = outs_factor
    parity = lax.axis_index("cols") % 2
    unpack_weights(lambda at, n: other[at : at + n, :].astype(F32) * factor, 1 - parity, [near_refs[n] for n in WEIGHTS], [far[n] for n in WEIGHTS], copies)
    flip = (iota((256, 256), 0) + iota((256, 256), 1) == 255).astype(BF16)
    for b in range(2):

        def raw(at, n):
            return jnp.where(parity == b, mine[at : at + n, :], other[at : at + n, :])

        small = raw(SMALL, 48).astype(F32) * factor
        for at, name in ((0, "ng"), (2, "nb"), (4, "qb"), (9, "pb"), (11, "mg"), (13, "mb"), (15, "ub"), (21, "db")):
            ref = near_refs[name]
            n = ref.shape[-1]
            for i in range(0, n, 128):
                w = min(128, n - i)
                ref[b : b + 1, i : i + w] = small[at + i // 128 : at + i // 128 + 1, 0:w]
        table = jnp.concatenate([raw(SMALL + 24, 8), raw(SMALL + 32, 8)], axis=1)
        table = dot_nn(table, flip) * factor
        for h in range(HEADS):
            near_refs["rel"][h, b : b + 1, :] = table[h : h + 1, 0 : SPAN * SPAN]
    for name in VEC_NAMES + ("rel",):
        copies.start(name, near_refs[name], far[name])
    copies.rest()


outs_factor = float(128 * 256) ** (-0.5)


VMEM = pl.BlockSpec(memory_space=pltpu.VMEM)


def near(value):
    return pltpu.with_memory_space_constraint(value, pltpu.VMEM)


FAR = pl.BlockSpec(memory_space=pltpu.HBM)


def call(kernel, args, far_args, outs, far_outs, scratch, flops, plain=()):
    return pl.pallas_call(
        kernel,
        in_specs=[VMEM] * len(args) + [FAR] * len(far_args),
        out_specs=[VMEM] * (len(outs) + len(plain)) + [FAR] * len(far_outs),
        out_shape=list(outs) + list(plain) + [pltpu.HBM(o.shape, o.dtype) for o in far_outs],
        scratch_shapes=scratch,
        compiler_params=pltpu.CompilerParams(vmem_limit_bytes=30 * 2**20),
        cost_estimate=pl.CostEstimate(flops=flops, transcendentals=0, bytes_accessed=4000000),
    )(*[near(a) for a in args], *[pltpu.with_memory_space_constraint(a, pltpu.HBM) for a in far_args])


def shaped(shape, dtype=BF16):
    return jax.ShapeDtypeStruct(shape, dtype)


def exchange(strips, step):
    n_rows = lax.axis_size("rows")
    n_cols = lax.axis_size("cols")
    col_strip, row_strip, corner = strips
    along = [(c, (c + step) % n_cols) for c in range(n_cols)]
    down = [(r, (r + step) % n_rows) for r in range(n_rows)]
    both = [
        (r * n_cols + c, ((r + step) % n_rows) * n_cols + (c + step) % n_cols)
        for r in range(n_rows)
        for c in range(n_cols)
    ]
    return [
        lax.ppermute(col_strip, "cols", along),
        lax.ppermute(row_strip, "rows", down),
        lax.ppermute(corner, ("rows", "cols"), both),
    ]


def swap(value):
    return lax.ppermute(value, "cols", [(c, c ^ 1) for c in range(lax.axis_size("cols"))])


def send_parts(value):
    n_cols = lax.axis_size("cols")
    n = lax.axis_size("rows") * n_cols
    groups = [[d for d in range(n) if d % n_cols % 2 == p] for p in range(2)]
    parts = value.reshape(n // 2, 2 * FLAT // n, 128)
    got = lax.all_to_all(parts, ("rows", "cols"), 0, 0, axis_index_groups=groups, tiled=True)
    return got.reshape(value.shape)


def both_blocks(imagery, cotangent, *params):
    params = list(params)
    params[4] = params[4].transpose(1, 0, 2)
    params[11] = params[11].swapaxes(1, 2)
    tile = (TILE, TILE, C)
    strips = [pltpu.VMEM(s, BF16) for s in ((128, C), (128, C), (32, C))]
    packed_grads = pltpu.VMEM((FLAT, 128), BF16)
    held = pltpu.VMEM(tile, BF16)
    grid = pltpu.VMEM((24, 24, 256), F32)
    edge = pltpu.VMEM((64, 256), F32)
    vec = pltpu.VMEM((128, MLP), F32)
    tables = [pltpu.VMEM((8, 256), F32), pltpu.VMEM((HEADS, 64, 128), F32)]
    par = dict(zip(PAR_NAMES, params))
    par_kinds = {n: BF16 if n in WEIGHTS else F32 for n in PAR_NAMES}
    par_vmem = {n: pltpu.VMEM(PAR_SHAPES[n], par_kinds[n]) for n in PAR_NAMES}
    res_vmem = [pltpu.VMEM(s, BF16) for s in RES_SHAPES]
    sems = pltpu.SemaphoreType.DMA((32,))
    one = call(
        first_forward,
        (),
        (imagery, cotangent, *params),
        [held] + strips,
        [shaped((C, TOK))] + [shaped(s) for s in RES_SHAPES],
        [grid, edge, vec] + tables + [sems] + list(par_vmem.values()) + res_vmem + [held, held, pltpu.VMEM((C, TOK), BF16)],
        5 * 10**9,
    )
    own, xt, res = one[0], one[4], one[5:]
    got = exchange(one[1:4], -1)
    channels = pltpu.VMEM((C, TOK), BF16)
    grad_vmem = [pltpu.VMEM(s, F32 if n == "rel" else BF16) for n, s in zip(GRAD_NAMES, GRAD_SHAPES)]
    small = pltpu.VMEM((48, 128), F32)
    two = call(
        second_block,
        (own, *got),
        (cotangent, *params),
        [held, held] + strips + grad_vmem + [res_vmem[4], res_vmem[2]],
        [],
        [grid, edge, vec]
        + tables
        + [sems]
        + list(par_vmem.values())
        + [res_vmem[i] for i in (0, 1, 3, 5)]
        + [held, pltpu.VMEM((C, TOK), BF16)],
        10**10,
    )
    got = exchange(two[2:5], 1)
    flat_two = call(second_grads, two[5:], (), [packed_grads], [], [small], 10**9)[0]
    dx, kept, sent = call(
        first_backward,
        (two[1], *got, flat_two),
        (*[par[n] for n in BACK_NAMES], xt, *res),
        [channels, packed_grads, packed_grads],
        [],
        [grid, edge, vec, sems]
        + [par_vmem[n] for n in BACK_NAMES]
        + grad_vmem
        + res_vmem
        + [channels, packed_grads, small],
        5 * 10**9,
    )
    sent = swap(sent)
    tiles = [shaped(tile), shaped(tile)]
    output, grad = call(make_tiles, (two[0], *got, dx), (), [], [], [grid, edge], 10**9, plain=tiles)
    parts = send_parts(call(add_pair, (kept, sent), (), [packed_grads], [], [], 10**6)[0])
    share = 2 * FLAT // (lax.axis_size("rows") * lax.axis_size("cols"))
    spread_sum = functools.partial(sum_spread, share)
    mine = send_parts(call(spread_sum, (parts,), (), [packed_grads], [], [], 10**6)[0])
    weights = [pltpu.VMEM(PAR_SHAPES[n], F32) for n in WEIGHTS]
    weights_far = [pltpu.HBM((2,) + PAR_SHAPES[n], F32) for n in WEIGHTS]
    few_sems = pltpu.SemaphoreType.DMA((4,))
    half = call(unpack_mine, (mine,), (), [], weights_far, weights + [few_sems], 10**9)
    grads = pl.pallas_call(
        unpack_rest,
        in_specs=[VMEM, VMEM] + [FAR] * 4,
        out_specs=[FAR] * len(PAR_NAMES),
        out_shape=[pltpu.HBM(p.shape, F32) for p in params],
        scratch_shapes=[pltpu.VMEM(PAR_SHAPES[n], F32) for n in PAR_NAMES] + [pltpu.SemaphoreType.DMA((16,))],
        input_output_aliases={2: 2, 3: 5, 4: 9, 5: 11},
        name="unpack_rest",
        compiler_params=pltpu.CompilerParams(vmem_limit_bytes=30 * 2**20),
    )(near(mine), near(swap(mine)), *[pltpu.with_memory_space_constraint(h, pltpu.HBM) for h in half])
    grads = list(grads)
    grads[4] = grads[4].transpose(1, 0, 2)
    grads[11] = grads[11].swapaxes(1, 2)
    return (output, grad, *grads)


def solution(mesh):
    tile = P("rows", "cols", None)
    return jax.shard_map(
        both_blocks,
        mesh=mesh,
        in_specs=(tile, tile) + (P(),) * 13,
        out_specs=(tile, tile) + (P(),) * 13,
        check_vma=False,
    )
```

```python
import functools

import jax
import jax.numpy as jnp
from jax import lax
from jax.experimental import pallas as pl
from jax.experimental.pallas import tpu as pltpu
from jax.sharding import PartitionSpec as P


F32 = jnp.float32
BF16 = jnp.bfloat16
C = 192
HEADS = 6
DIM = 32
MLP = 768
TILE = 16
TOK = TILE * TILE
SPAN = 15
SCALE = DIM**-0.5
EPSILON = 1e-05
FLAT = 3584
SMALL = 3456
MASKED = -1e30


def dot_tn(a, b):
    return lax.dot_general(a, b, (((0,), (0,)), ((), ())), preferred_element_type=F32)


def dot_nn(a, b):
    return lax.dot_general(a, b, (((1,), (0,)), ((), ())), preferred_element_type=F32)


def dot_nt(a, b):
    return lax.dot_general(a, b, (((1,), (1,)), ((), ())), preferred_element_type=F32)


def iota(shape, dim):
    return lax.broadcasted_iota(jnp.int32, shape, dim)


def split3(value):
    high = value.astype(BF16)
    rest = value - high.astype(F32)
    mid = rest.astype(BF16)
    return high, mid, (rest - mid.astype(F32)).astype(BF16)


def window_row(r, wc):
    return ((r // 8) * 2 + wc) * 64 + (r % 8) * 8


def halves():
    return iota((64, 128), 1) < 64


def stack_windows(value, left):
    zero = jnp.zeros_like(value)
    return jnp.concatenate([jnp.where(left, value, zero), jnp.where(left, zero, value)], axis=0).astype(BF16)


def own_window(full, left):
    return jnp.where(left, full[:64], full[64:])


def norm_fwd(x):
    center = x - jnp.mean(x, axis=0, keepdims=True)
    rstd = lax.rsqrt(jnp.mean(center * center, axis=0, keepdims=True) + EPSILON)
    return center * rstd, rstd


def norm_bwd(dn, xhat, rstd, gain):
    dxh = dn * gain
    along = jnp.mean(dxh * xhat, axis=0, keepdims=True)
    return rstd * (dxh - jnp.mean(dxh, axis=0, keepdims=True) - xhat * along)


def spread(lane_q):
    q = lane_q % 64
    return (q // 8) * SPAN + q % 8


VEC_NAMES = ("ng", "nb", "pb", "mg", "mb", "db", "qb", "ub")


def load_columns(vec, par, b):
    for i, name in enumerate(VEC_NAMES):
        n = par[name].shape[-1]
        vec[i : i + 1, 0:n] = par[name][b : b + 1, :]
    return vec[...].T


def position_bias(par, b, table, bias):
    table[...] = jnp.zeros((8, 256), F32)
    for h in range(HEADS):
        table[h : h + 1, 0 : SPAN * SPAN] = par["rel"][h, b : b + 1, :]
    select = (iota((128, 128), 0) == spread(iota((128, 128), 1))).astype(BF16)
    for h in range(HEADS):
        row = jnp.broadcast_to(table[h : h + 1, :], (8, 256))
        rows = []
        for ky in range(8):
            shift = (249 - SPAN * (7 - ky)) % 256
            rows.append(pltpu.roll(row, shift, 1, stride=1, stride_axis=0)[:, 0:128])
        high, mid, low = split3(jnp.concatenate(rows, axis=0))
        bias[h] = dot_nn(high, select) + (dot_nn(mid, select) + dot_nn(low, select))


def same_zone(p, last_row, last_col):
    k = iota((64, 128), 0)
    lane = iota((64, 128), 1)
    q = lane % 64
    rows = ((q // 8) < 4) == ((k // 8) < 4)
    cols = ((q % 8) < 4) == ((k % 8) < 4)
    keep = jnp.logical_or(cols, jnp.logical_or(lane < 64, jnp.logical_not(last_col)))
    if p == 1:
        keep = jnp.logical_and(keep, jnp.logical_or(rows, jnp.logical_not(last_row)))
    return keep


UNITS = [(p, h, slice(128 * p, 128 * p + 128)) for p in range(2) for h in range(HEADS)]


def forward(x, par, need, cols, bias, res, stage, zones, keep):
    left = halves()
    xhat, _ = norm_fwd(x)
    normed = (xhat * cols[0:C, 0:1] + cols[0:C, 1:2]).astype(BF16)
    need("qw")
    res["packed"][...] = (dot_tn(par["qw"][...], normed) + cols[0:576, 6:7]).astype(BF16)
    for p, h, lanes in UNITS:
        q = res["packed"][DIM * h : DIM * h + DIM, lanes]
        k = res["packed"][C + DIM * h : C + DIM * h + DIM, lanes]
        s = own_window(dot_tn(k, q), left) * SCALE + bias[h]
        if zones is not None:
            s = jnp.where(zones[p], s, MASKED)
        stage[p * HEADS + h] = s
    for p, h, _ in UNITS:
        s = stage[p * HEADS + h]
        e = jnp.exp(s - jnp.max(s, axis=0, keepdims=True))
        a = e * (1.0 / jnp.sum(e, axis=0, keepdims=True))
        res["attn"][p * HEADS + h] = a.astype(BF16)
    for p, h, lanes in UNITS:
        v = res["packed"][2 * C + DIM * h : 2 * C + DIM * h + DIM, lanes]
        wide = stack_windows(res["attn"][p * HEADS + h].astype(F32), left)
        res["mixed"][DIM * h : DIM * h + DIM, lanes] = dot_nn(v, wide).astype(BF16)
    keep("packed")
    need("pw")
    middle = x + dot_tn(par["pw"][...], res["mixed"][...]) + cols[0:C, 2:3]
    res["middle"][...] = middle.astype(BF16)
    middle = res["middle"][...].astype(F32)
    xhat, _ = norm_fwd(middle)
    normed = (xhat * cols[0:C, 3:4] + cols[0:C, 4:5]).astype(BF16)
    keep("attn", "mixed")
    need("uw")
    for i in range(0, MLP, 128):
        u = dot_tn(par["uw"][:, i : i + 128], normed) + cols[i : i + 128, 7:8]
        half = 0.5 + 0.5 * lax.erf(u * (0.5**0.5))
        res["hidden"][i : i + 128, :] = (u * half).astype(BF16)
        res["slope"][i : i + 128, :] = (half + u * (jnp.exp(-0.5 * u * u) * 0.3989422804014327)).astype(BF16)
    keep("middle")
    need("dw")
    out = (middle + dot_nn(par["dw"][...], res["hidden"][...]) + cols[0:C, 5:6]).astype(BF16)
    keep("hidden", "slope")
    return out


def put_row(small, at, row):
    n = row.shape[-1]
    for i in range(0, n, 128):
        w = min(128, n - i)
        small[at + i // 128 : at + i // 128 + 1, 0:w] = row[0:1, i : i + w]


def put_pairs(flat, at, lhs, rhs, n):
    for i in range(0, n, 256):
        wide = dot_nt(lhs, rhs[i : i + 256, :]).astype(BF16)
        for j in range(0, 256, 128):
            first = at + C * ((i + j) // 128)
            flat[first : first + C, :] = wide[:, j : j + 128]


def mlp_grads(g, flat, small):
    ones = jnp.ones((8, TOK), BF16)
    small[...] = jnp.zeros(small.shape, F32)
    put_row(small, 21, dot_nt(ones, g["dout"][...]))
    put_row(small, 15, dot_nt(ones, g["du"][...]))
    put_row(small, 13, dot_nt(ones, g["dn2"][...]))
    put_row(small, 11, dot_nt(ones, g["dg2"][...]))
    put_pairs(flat, 1152, g["n2"][...], g["du"], MLP)
    put_pairs(flat, 2304, g["dout"][...], g["hidden"], MLP)


def attention_grads(g, flat, small):
    ones = jnp.ones((8, TOK), BF16)
    none = jnp.zeros((64, TOK), BF16)
    put_row(small, 9, dot_nt(ones, g["dmid"][...]))
    flat[960:1152, :] = dot_nt(g["mixed"][...], g["dmid"][0:128, :]).astype(BF16)
    mirror = ((127 - iota((128, 128), 0)) == spread(iota((128, 128), 1))).astype(BF16)
    for h in range(HEADS):
        high, mid, _ = split3(g["rel"][h])
        back = dot_nt(high, mirror) + dot_nt(mid, mirror)
        total = jnp.zeros((8, 256), F32)
        for ky in range(8):
            wide = jnp.concatenate([back[8 * ky : 8 * ky + 8], jnp.zeros((8, 128), F32)], axis=1)
            total = total + pltpu.roll(wide, 121 - SPAN * (7 - ky), 1, stride=1, stride_axis=0)
        total = jnp.sum(total, axis=0, keepdims=True)
        small[24 + h : 25 + h, :] = total[:, 0:128]
        small[32 + h : 33 + h, :] = total[:, 128:256]
    put_pairs(flat, 0, g["n1"][...], g["dpacked"], 512)
    tail = dot_nt(g["n1"][...], jnp.concatenate([g["dpacked"][512:576, :], none], axis=0))
    tail = tail + dot_nt(g["mixed"][...], jnp.concatenate([none, g["dmid"][128:192, :]], axis=0))
    flat[768:960, :] = tail.astype(BF16)
    put_row(small, 4, dot_nt(ones, g["dpacked"][...]))
    put_row(small, 2, dot_nt(ones, g["dn1"][...]))
    put_row(small, 0, dot_nt(ones, g["dg1"][...]))
    flat[SMALL : SMALL + 48, :] = small[...].astype(BF16)
    flat[SMALL + 48 : FLAT, :] = jnp.zeros((FLAT - SMALL - 48, 128), BF16)


def backward(x, par, need, cols, res, stage, g, after_mlp):
    left = halves()
    dout = g["dout"][...]
    need("dw", "slope")
    for i in range(0, MLP, 128):
        dh = dot_tn(par["dw"][:, i : i + 128], dout).astype(BF16).astype(F32)
        g["du"][i : i + 128, :] = (dh * res["slope"][i : i + 128, :].astype(F32)).astype(BF16)
    need("middle", "uw")
    xhat, rstd = norm_fwd(res["middle"][...].astype(F32))
    g["n2"][...] = (xhat * cols[0:C, 3:4] + cols[0:C, 4:5]).astype(BF16)
    dn = dot_nn(par["uw"][...], g["du"][...]).astype(BF16)
    g["dn2"][...] = dn
    dn = dn.astype(F32)
    g["dg2"][...] = (dn * xhat).astype(BF16)
    dmid = (dout.astype(F32) + norm_bwd(dn, xhat, rstd, cols[0:C, 3:4])).astype(BF16)
    g["dmid"][...] = dmid
    after_mlp()
    need("pw", "mixed")
    dmixed = dot_nn(par["pw"][...], dmid).astype(BF16)
    need("packed", "attn")
    for p, h, lanes in UNITS:
        v = res["packed"][2 * C + DIM * h : 2 * C + DIM * h + DIM, lanes]
        dm = dmixed[DIM * h : DIM * h + DIM, lanes]
        stage[p * HEADS + h] = own_window(dot_tn(v, dm), left).astype(BF16).astype(F32)
        dv = dot_nt(dm, stack_windows(res["attn"][p * HEADS + h].astype(F32), left)).astype(BF16)
        g["dpacked"][2 * C + DIM * h : 2 * C + DIM * h + DIM, lanes] = dv
    for h in range(HEADS):
        drel = None
        for p in range(2):
            a = res["attn"][p * HEADS + h].astype(F32)
            da = stage[p * HEADS + h]
            ds = a * (da - jnp.sum(da * a, axis=0, keepdims=True))
            drel = ds if drel is None else drel + ds
            stage[p * HEADS + h] = ds * SCALE
        g["rel"][h] = drel
    for p, h, lanes in UNITS:
        q = res["packed"][DIM * h : DIM * h + DIM, lanes]
        k = res["packed"][C + DIM * h : C + DIM * h + DIM, lanes]
        wide = stack_windows(stage[p * HEADS + h], left)
        g["dpacked"][DIM * h : DIM * h + DIM, lanes] = dot_nn(k, wide).astype(BF16)
        g["dpacked"][C + DIM * h : C + DIM * h + DIM, lanes] = dot_nt(q, wide).astype(BF16)
    need("xt")
    xhat, rstd = norm_fwd(x[...].astype(F32))
    g["n1"][...] = (xhat * cols[0:C, 0:1] + cols[0:C, 1:2]).astype(BF16)
    need("qw")
    dn = dot_nn(par["qw"][...], g["dpacked"][...]).astype(BF16)
    g["dn1"][...] = dn
    dn = dn.astype(F32)
    g["dg1"][...] = (dn * xhat).astype(BF16)
    return dmid.astype(F32) + norm_bwd(dn, xhat, rstd, cols[0:C, 0:1])


def to_channels(pieces):
    return jnp.concatenate(pieces, axis=0).T[0:C]


def to_tokens(value):
    return jnp.concatenate([value, jnp.zeros((64, TOK), F32)], axis=0).T


def grid_put(grid, tokens):
    for r in range(TILE):
        for wc in range(2):
            at = window_row(r, wc)
            grid[r, 8 * wc : 8 * wc + 8, :] = tokens[at : at + 8]


def grid_get(grid, row_at, col_at):
    pieces = []
    for wr in range(2):
        for wc in range(2):
            for ir in range(8):
                at = col_at + 8 * wc
                pieces.append(grid[row_at + 8 * wr + ir, at : at + 8, :])
    return pieces


def emit_strips(grid, edge, strips, which, row_at, col_at):
    col_out, row_out, corner_out = strips
    for r in range(TILE):
        edge[4 * r : 4 * r + 4, :] = grid[r, col_at : col_at + 4, :]
    col_out[64 * which : 64 * which + 64, :] = edge[:, 0:C].astype(BF16)
    for r in range(4):
        row_out[64 * which + 16 * r : 64 * which + 16 * r + 16, :] = grid[row_at + r, 0:TILE, 0:C].astype(BF16)
    for r in range(4):
        edge[4 * r : 4 * r + 4, :] = grid[row_at + r, col_at : col_at + 4, :]
    corner_out[16 * which : 16 * which + 16, :] = edge[0:16, 0:C].astype(BF16)


def fill_grid(grid, edge, own, strips, which, own_row, own_col, strip_row, strip_col):
    col_in, row_in, corner_in = strips
    for r in range(TILE):
        grid[own_row + r, own_col : own_col + TILE, 0:C] = own[r].astype(F32)
    edge[:, 0:C] = col_in[64 * which : 64 * which + 64, :].astype(F32)
    for r in range(TILE):
        grid[own_row + r, strip_col : strip_col + 4, :] = edge[4 * r : 4 * r + 4, :]
    for r in range(4):
        at = 64 * which + 16 * r
        grid[strip_row + r, own_col : own_col + TILE, 0:C] = row_in[at : at + 16, :].astype(F32)
    edge[0:16, 0:C] = corner_in[16 * which : 16 * which + 16, :].astype(F32)
    for r in range(4):
        grid[strip_row + r, strip_col : strip_col + 4, :] = edge[4 * r : 4 * r + 4, :]


PAR_NAMES = ("ng", "nb", "qw", "qb", "rel", "pw", "pb", "mg", "mb", "uw", "ub", "dw", "db")
RES_NAMES = ("packed", "attn", "mixed", "middle", "hidden", "slope")
GRAD_NAMES = ("dout", "n1", "n2", "dmid", "dn1", "dn2", "dg1", "dg2", "du", "dpacked", "rel")
GRAD_SHAPES = ((C, TOK),) * 8 + ((MLP, TOK), (576, TOK), (HEADS, 64, 128))
RES_SHAPES = ((576, TOK), (12, 64, 128), (C, TOK), (C, TOK), (MLP, TOK), (MLP, TOK))


class Copies:
    def __init__(self, sems):
        self.sems = sems
        self.used = 0
        self.open = {}

    def start(self, name, source, target):
        self.open[name] = pltpu.make_async_copy(source, target, self.sems.at[self.used])
        self.open[name].start()
        self.used += 1

    def __call__(self, *names):
        for name in names:
            if name in self.open:
                self.open.pop(name).wait()

    def rest(self):
        self(*list(self.open))


def start_params(copies, names, far, par, b):
    for name in names:
        source = far[name].at[b] if name in WEIGHTS else far[name]
        copies.start(name, source, par[name])


WEIGHTS = ("qw", "pw", "uw", "dw")
PAR_SHAPES = dict(
    ng=(2, C), nb=(2, C), qw=(C, 3 * C), qb=(2, 3 * C), rel=(HEADS, 2, SPAN * SPAN), pw=(C, C), pb=(2, C),
    mg=(2, C), mb=(2, C), uw=(C, MLP), ub=(2, MLP), dw=(C, MLP), db=(2, C),
)


def nothing(*_):
    pass


def first_forward(*refs):
    imagery_far, cotangent_far = refs[0:2]
    far = dict(zip(PAR_NAMES, refs[2:15]))
    own = refs[15]
    strips = refs[16:19]
    xt_far = refs[19]
    res_far = dict(zip(RES_NAMES, refs[20:26]))
    grid, edge, vec, table, bias, sems = refs[26:32]
    par = dict(zip(PAR_NAMES, refs[32:45]))
    res = dict(zip(RES_NAMES, refs[45:51]))
    imagery, cotangent, xt, stage = refs[51:]
    need = Copies(sems)
    need.start("imagery", imagery_far, imagery)
    start_params(need, VEC_NAMES, far, par, 0)
    start_params(need, ("qw", "rel", "pw"), far, par, 0)
    need.start("cotangent", cotangent_far, cotangent)
    start_params(need, ("uw", "dw"), far, par, 0)

    def keep(*names):
        for name in names:
            need.start("out " + name, res[name], res_far[name])

    need("imagery")
    for r in range(TILE):
        grid[r, 0:TILE, 0:C] = imagery[r].astype(F32)
    x = to_channels(grid_get(grid, 0, 0))
    xt[...] = x.astype(BF16)
    need(*VEC_NAMES, "rel", "qw", "pw", "cotangent")
    cols = load_columns(vec, par, 0)
    position_bias(par, 0, table, bias)
    for r in range(TILE):
        grid[r, 0:TILE, 0:C] = cotangent[r].astype(F32)
    emit_strips(grid, edge, strips, 1, 0, 0)
    need.start("out xt", xt, xt_far)
    out = forward(x, par, need, cols, bias, res, stage, None, keep)
    grid_put(grid, to_tokens(out.astype(F32)))
    for r in range(TILE):
        own[r] = grid[r, 0:TILE, 0:C].astype(BF16)
    emit_strips(grid, edge, strips, 0, 0, 0)
    need.rest()


def second_block(*refs):
    own_in = refs[0]
    strips_in = refs[1:4]
    cotangent_far = refs[4]
    far = dict(zip(PAR_NAMES, refs[5:18]))
    out_own, back_own = refs[18:20]
    strips = refs[20:23]
    g = dict(zip(GRAD_NAMES + ("hidden", "mixed"), refs[23:36]))
    grid, edge, vec, table, bias, sems = refs[36:42]
    par = dict(zip(PAR_NAMES, refs[42:55]))
    res = dict(zip(("packed", "attn", "middle", "slope"), refs[55:59]), hidden=g["hidden"], mixed=g["mixed"])
    cotangent, xt, stage = refs[59:]
    need = Copies(sems)
    start_params(need, VEC_NAMES + ("rel",), far, par, 1)
    need.start("cotangent", cotangent_far, cotangent)
    start_params(need, ("qw", "pw", "uw", "dw"), far, par, 1)
    last_row = lax.axis_index("rows") == lax.axis_size("rows") - 1
    last_col = lax.axis_index("cols") == lax.axis_size("cols") - 1
    zones = [same_zone(p, last_row, last_col) for p in range(2)]
    fill_grid(grid, edge, own_in, strips_in, 0, 0, 0, 16, 16)
    x = to_channels(grid_get(grid, 4, 4))
    xt[...] = x.astype(BF16)
    need(*VEC_NAMES, "rel", "cotangent")
    cols = load_columns(vec, par, 1)
    position_bias(par, 1, table, bias)
    fill_grid(grid, edge, cotangent, strips_in, 1, 0, 0, 16, 16)
    g["dout"][...] = to_channels(grid_get(grid, 4, 4)).astype(BF16)
    out = forward(x, par, need, cols, bias, res, stage, zones, nothing)
    grid_put(grid, to_tokens(out.astype(F32)))
    for r in range(TILE):
        out_own[r] = grid[r, 0:TILE, 0:C].astype(BF16)
    emit_strips(grid, edge, strips, 0, 12, 12)
    dx = backward(xt, par, need, cols, res, stage, g, nothing)
    grid_put(grid, to_tokens(dx))
    for r in range(TILE):
        back_own[r] = grid[r, 0:TILE, 0:C].astype(BF16)
    emit_strips(grid, edge, strips, 1, 12, 12)
    need.rest()


def second_grads(*refs):
    g = dict(zip(GRAD_NAMES + ("hidden", "mixed"), refs[0:13]))
    flat, small = refs[13:]
    mlp_grads(g, flat, small)
    attention_grads(g, flat, small)


BACK_NAMES = VEC_NAMES + WEIGHTS


def first_backward(*refs):
    back_in = refs[0]
    strips_in = refs[1:4]
    flat_two = refs[4]
    far = dict(zip(BACK_NAMES, refs[5:17]))
    xt_far = refs[17]
    res_far = dict(zip(RES_NAMES, refs[18:24]))
    dx_channels, kept, sent = refs[24:27]
    grid, edge, vec, sems = refs[27:31]
    par = dict(zip(BACK_NAMES, refs[31:43]))
    g = dict(zip(GRAD_NAMES, refs[43:54]))
    res = dict(zip(RES_NAMES, refs[54:60]))
    xt, flat, small, stage = refs[60:]
    g["hidden"] = res["hidden"]
    g["mixed"] = res["mixed"]
    need = Copies(sems)
    start_params(need, ("dw",), far, par, 0)
    need.start("slope", res_far["slope"], res["slope"])
    start_params(need, VEC_NAMES, far, par, 0)
    need.start("middle", res_far["middle"], res["middle"])
    start_params(need, ("uw",), far, par, 0)
    need.start("hidden", res_far["hidden"], res["hidden"])
    need.start("mixed", res_far["mixed"], res["mixed"])
    start_params(need, ("pw",), far, par, 0)
    need.start("packed", res_far["packed"], res["packed"])
    need.start("attn", res_far["attn"], res["attn"])
    need.start("xt", xt_far, xt)
    start_params(need, ("qw",), far, par, 0)
    fill_grid(grid, edge, back_in, strips_in, 1, 4, 8, 0, 4)
    g["dout"][...] = to_channels(grid_get(grid, 0, 4)).astype(BF16)
    need(*VEC_NAMES)
    cols = load_columns(vec, par, 0)

    def after_mlp():
        need("hidden")
        mlp_grads(g, flat, small)

    dx_channels[...] = backward(xt, par, need, cols, res, stage, g, after_mlp).astype(BF16)
    attention_grads(g, flat, small)
    even = lax.axis_index("cols") % 2 == 0
    for at in range(0, FLAT, 256):
        rows = slice(at, at + 256)
        kept[rows, :] = jnp.where(even, flat[rows, :], flat_two[rows, :])
        sent[rows, :] = jnp.where(even, flat_two[rows, :], flat[rows, :])
    need.rest()


def make_tiles(out_own, col_in, row_in, corner_in, dx_channels, output, grad, grid, edge):
    fill_grid(grid, edge, out_own, (col_in, row_in, corner_in), 0, 4, 8, 0, 4)
    for r in range(TILE):
        output[r] = grid[r, 4:20, 0:C].astype(BF16)
    grid_put(grid, to_tokens(dx_channels[...].astype(F32)))
    for r in range(TILE):
        grad[r] = grid[r, 0:TILE, 0:C].astype(BF16)


def add_pair(kept, got, out):
    for at in range(0, FLAT, 256):
        rows = slice(at, at + 256)
        out[rows, :] = (kept[rows, :].astype(F32) + got[rows, :].astype(F32)).astype(BF16)


def sum_spread(share, parts, out):
    total = jnp.zeros((share, 128), F32)
    for at in range(0, FLAT, share):
        total = total + parts[at : at + share, :].astype(F32)
    total = total.astype(BF16)
    for at in range(0, FLAT, share):
        out[at : at + share, :] = total


def unpack_weights(rows, b, near_refs, far_refs, copies):
    qw, pw, uw, dw = near_refs
    for j in range(4):
        qw[:, 128 * j : 128 * j + 128] = rows(C * j, C)
    tail = rows(768, C)
    qw[:, 512:576] = tail[:, 0:64]
    copies.start("qw", qw, far_refs[0].at[b])
    pw[:, 128:192] = pltpu.roll(tail, 64, 1)[:, 0:64]
    pw[:, 0:128] = rows(960, C)
    copies.start("pw", pw, far_refs[1].at[b])
    for j in range(6):
        uw[:, 128 * j : 128 * j + 128] = rows(1152 + C * j, C)
    copies.start("uw", uw, far_refs[2].at[b])
    for j in range(6):
        dw[:, 128 * j : 128 * j + 128] = rows(2304 + C * j, C)
    copies.start("dw", dw, far_refs[3].at[b])


def unpack_mine(mine, *refs):
    copies = Copies(refs[8])
    parity = lax.axis_index("cols") % 2
    unpack_weights(lambda at, n: mine[at : at + n, :].astype(F32) * outs_factor, parity, refs[4:8], refs[0:4], copies)
    copies.rest()


def unpack_rest(mine, other, *refs):
    far = dict(zip(PAR_NAMES, refs[4:17]))
    near_refs = dict(zip(PAR_NAMES, refs[17:30]))
    copies = Copies(refs[30])
    factor = outs_factor
    parity = lax.axis_index("cols") % 2
    unpack_weights(lambda at, n: other[at : at + n, :].astype(F32) * factor, 1 - parity, [near_refs[n] for n in WEIGHTS], [far[n] for n in WEIGHTS], copies)
    flip = (iota((256, 256), 0) + iota((256, 256), 1) == 255).astype(BF16)
    for b in range(2):

        def raw(at, n):
            return jnp.where(parity == b, mine[at : at + n, :], other[at : at + n, :])

        small = raw(SMALL, 48).astype(F32) * factor
        for at, name in ((0, "ng"), (2, "nb"), (4, "qb"), (9, "pb"), (11, "mg"), (13, "mb"), (15, "ub"), (21, "db")):
            ref = near_refs[name]
            n = ref.shape[-1]
            for i in range(0, n, 128):
                w = min(128, n - i)
                ref[b : b + 1, i : i + w] = small[at + i // 128 : at + i // 128 + 1, 0:w]
        table = jnp.concatenate([raw(SMALL + 24, 8), raw(SMALL + 32, 8)], axis=1)
        table = dot_nn(table, flip) * factor
        for h in range(HEADS):
            near_refs["rel"][h, b : b + 1, :] = table[h : h + 1, 0 : SPAN * SPAN]
    for name in VEC_NAMES + ("rel",):
        copies.start(name, near_refs[name], far[name])
    copies.rest()


outs_factor = float(128 * 256) ** (-0.5)


VMEM = pl.BlockSpec(memory_space=pltpu.VMEM)


def near(value):
    return pltpu.with_memory_space_constraint(value, pltpu.VMEM)


FAR = pl.BlockSpec(memory_space=pltpu.HBM)


def call(kernel, args, far_args, outs, far_outs, scratch, flops, plain=()):
    return pl.pallas_call(
        kernel,
        in_specs=[VMEM] * len(args) + [FAR] * len(far_args),
        out_specs=[VMEM] * (len(outs) + len(plain)) + [FAR] * len(far_outs),
        out_shape=list(outs) + list(plain) + [pltpu.HBM(o.shape, o.dtype) for o in far_outs],
        scratch_shapes=scratch,
        compiler_params=pltpu.CompilerParams(vmem_limit_bytes=30 * 2**20),
        cost_estimate=pl.CostEstimate(flops=flops, transcendentals=0, bytes_accessed=4000000),
    )(*[near(a) for a in args], *[pltpu.with_memory_space_constraint(a, pltpu.HBM) for a in far_args])


def shaped(shape, dtype=BF16):
    return jax.ShapeDtypeStruct(shape, dtype)


def exchange(strips, step):
    n_rows = lax.axis_size("rows")
    n_cols = lax.axis_size("cols")
    col_strip, row_strip, corner = strips
    along = [(c, (c + step) % n_cols) for c in range(n_cols)]
    down = [(r, (r + step) % n_rows) for r in range(n_rows)]
    both = [
        (r * n_cols + c, ((r + step) % n_rows) * n_cols + (c + step) % n_cols)
        for r in range(n_rows)
        for c in range(n_cols)
    ]
    return [
        lax.ppermute(col_strip, "cols", along),
        lax.ppermute(row_strip, "rows", down),
        lax.ppermute(corner, ("rows", "cols"), both),
    ]


def swap(value):
    return lax.ppermute(value, "cols", [(c, c ^ 1) for c in range(lax.axis_size("cols"))])


def send_parts(value):
    n_cols = lax.axis_size("cols")
    n = lax.axis_size("rows") * n_cols
    groups = [[d for d in range(n) if d % n_cols % 2 == p] for p in range(2)]
    parts = value.reshape(n // 2, 2 * FLAT // n, 128)
    got = lax.all_to_all(parts, ("rows", "cols"), 0, 0, axis_index_groups=groups, tiled=True)
    return got.reshape(value.shape)


def both_blocks(imagery, cotangent, *params):
    params = list(params)
    params[4] = params[4].transpose(1, 0, 2)
    params[11] = params[11].swapaxes(1, 2)
    tile = (TILE, TILE, C)
    strips = [pltpu.VMEM(s, BF16) for s in ((128, C), (128, C), (32, C))]
    packed_grads = pltpu.VMEM((FLAT, 128), BF16)
    held = pltpu.VMEM(tile, BF16)
    grid = pltpu.VMEM((24, 24, 256), F32)
    edge = pltpu.VMEM((64, 256), F32)
    vec = pltpu.VMEM((128, MLP), F32)
    tables = [pltpu.VMEM((8, 256), F32), pltpu.VMEM((HEADS, 64, 128), F32)]
    par = dict(zip(PAR_NAMES, params))
    par_kinds = {n: BF16 if n in WEIGHTS else F32 for n in PAR_NAMES}
    par_vmem = {n: pltpu.VMEM(PAR_SHAPES[n], par_kinds[n]) for n in PAR_NAMES}
    res_vmem = [pltpu.VMEM(s, BF16) for s in RES_SHAPES]
    sems = pltpu.SemaphoreType.DMA((32,))
    stage = pltpu.VMEM((2 * HEADS, 64, 128), F32)
    one = call(
        first_forward,
        (),
        (imagery, cotangent, *params),
        [held] + strips,
        [shaped((C, TOK))] + [shaped(s) for s in RES_SHAPES],
        [grid, edge, vec] + tables + [sems] + list(par_vmem.values()) + res_vmem + [held, held, pltpu.VMEM((C, TOK), BF16), stage],
        5 * 10**9,
    )
    own, xt, res = one[0], one[4], one[5:]
    got = exchange(one[1:4], -1)
    channels = pltpu.VMEM((C, TOK), BF16)
    grad_vmem = [pltpu.VMEM(s, F32 if n == "rel" else BF16) for n, s in zip(GRAD_NAMES, GRAD_SHAPES)]
    small = pltpu.VMEM((48, 128), F32)
    two = call(
        second_block,
        (own, *got),
        (cotangent, *params),
        [held, held] + strips + grad_vmem + [res_vmem[4], res_vmem[2]],
        [],
        [grid, edge, vec]
        + tables
        + [sems]
        + list(par_vmem.values())
        + [res_vmem[i] for i in (0, 1, 3, 5)]
        + [held, pltpu.VMEM((C, TOK), BF16), stage],
        10**10,
    )
    got = exchange(two[2:5], 1)
    flat_two = call(second_grads, two[5:], (), [packed_grads], [], [small], 10**9)[0]
    dx, kept, sent = call(
        first_backward,
        (two[1], *got, flat_two),
        (*[par[n] for n in BACK_NAMES], xt, *res),
        [channels, packed_grads, packed_grads],
        [],
        [grid, edge, vec, sems]
        + [par_vmem[n] for n in BACK_NAMES]
        + grad_vmem
        + res_vmem
        + [channels, packed_grads, small, stage],
        5 * 10**9,
    )
    sent = swap(sent)
    tiles = [shaped(tile), shaped(tile)]
    output, grad = call(make_tiles, (two[0], *got, dx), (), [], [], [grid, edge], 10**9, plain=tiles)
    parts = send_parts(call(add_pair, (kept, sent), (), [packed_grads], [], [], 10**6)[0])
    share = 2 * FLAT // (lax.axis_size("rows") * lax.axis_size("cols"))
    spread_sum = functools.partial(sum_spread, share)
    mine = send_parts(call(spread_sum, (parts,), (), [packed_grads], [], [], 10**6)[0])
    weights = [pltpu.VMEM(PAR_SHAPES[n], F32) for n in WEIGHTS]
    weights_far = [pltpu.HBM((2,) + PAR_SHAPES[n], F32) for n in WEIGHTS]
    few_sems = pltpu.SemaphoreType.DMA((4,))
    half = call(unpack_mine, (mine,), (), [], weights_far, weights + [few_sems], 10**9)
    grads = pl.pallas_call(
        unpack_rest,
        in_specs=[VMEM, VMEM] + [FAR] * 4,
        out_specs=[FAR] * len(PAR_NAMES),
        out_shape=[pltpu.HBM(p.shape, F32) for p in params],
        scratch_shapes=[pltpu.VMEM(PAR_SHAPES[n], F32) for n in PAR_NAMES] + [pltpu.SemaphoreType.DMA((16,))],
        input_output_aliases={2: 2, 3: 5, 4: 9, 5: 11},
        name="unpack_rest",
        compiler_params=pltpu.CompilerParams(vmem_limit_bytes=30 * 2**20),
    )(near(mine), near(swap(mine)), *[pltpu.with_memory_space_constraint(h, pltpu.HBM) for h in half])
    grads = list(grads)
    grads[4] = grads[4].transpose(1, 0, 2)
    grads[11] = grads[11].swapaxes(1, 2)
    return (output, grad, *grads)


def solution(mesh):
    tile = P("rows", "cols", None)
    return jax.shard_map(
        both_blocks,
        mesh=mesh,
        in_specs=(tile, tile) + (P(),) * 13,
        out_specs=(tile, tile) + (P(),) * 13,
        check_vma=False,
    )
```

```python
import functools

import jax
import jax.numpy as jnp
from jax import lax
from jax.experimental import pallas as pl
from jax.experimental.pallas import tpu as pltpu
from jax.sharding import PartitionSpec as P


F32 = jnp.float32
BF16 = jnp.bfloat16
C = 192
HEADS = 6
DIM = 32
MLP = 768
TILE = 16
TOK = TILE * TILE
SPAN = 15
SCALE = DIM**-0.5
EPSILON = 1e-05
FLAT = 3584
SMALL = 3456
MASKED = -1e30


class Box(dict):
    __getattr__ = dict.__getitem__


def dot_tn(a, b):
    return lax.dot_general(a, b, (((0,), (0,)), ((), ())), preferred_element_type=F32)


def dot_nn(a, b):
    return lax.dot_general(a, b, (((1,), (0,)), ((), ())), preferred_element_type=F32)


def dot_nt(a, b):
    return lax.dot_general(a, b, (((1,), (1,)), ((), ())), preferred_element_type=F32)


def iota(shape, dim):
    return lax.broadcasted_iota(jnp.int32, shape, dim)


def split3(value):
    high = value.astype(BF16)
    rest = value - high.astype(F32)
    mid = rest.astype(BF16)
    return high, mid, (rest - mid.astype(F32)).astype(BF16)


def window_row(r, wc):
    return ((r // 8) * 2 + wc) * 64 + (r % 8) * 8


def halves():
    return iota((64, 128), 1) < 64


def stack_windows(value, left):
    zero = jnp.zeros_like(value)
    return jnp.concatenate([jnp.where(left, value, zero), jnp.where(left, zero, value)], axis=0).astype(BF16)


def own_window(full, left):
    return jnp.where(left, full[:64], full[64:])


def norm_fwd(x):
    center = x - jnp.mean(x, axis=0, keepdims=True)
    rstd = lax.rsqrt(jnp.mean(center * center, axis=0, keepdims=True) + EPSILON)
    return center * rstd, rstd


def norm_bwd(dn, xhat, rstd, gain):
    dxh = dn * gain
    along = jnp.mean(dxh * xhat, axis=0, keepdims=True)
    return rstd * (dxh - jnp.mean(dxh, axis=0, keepdims=True) - xhat * along)


def spread(lane_q):
    q = lane_q % 64
    return (q // 8) * SPAN + q % 8


VEC_NAMES = ("ng", "nb", "pb", "mg", "mb", "db", "qb", "ub")


def load_columns(vec, par, b):
    for i, name in enumerate(VEC_NAMES):
        n = par[name].shape[-1]
        vec[i : i + 1, 0:n] = par[name][b : b + 1, :]
    return vec[...].T


def position_bias(par, b, table, bias):
    table[...] = jnp.zeros((8, 256), F32)
    for h in range(HEADS):
        table[h : h + 1, 0 : SPAN * SPAN] = par.rel[h, b : b + 1, :]
    select = (iota((128, 128), 0) == spread(iota((128, 128), 1))).astype(BF16)
    for h in range(HEADS):
        row = jnp.broadcast_to(table[h : h + 1, :], (8, 256))
        rows = []
        for ky in range(8):
            shift = (249 - SPAN * (7 - ky)) % 256
            rows.append(pltpu.roll(row, shift, 1, stride=1, stride_axis=0)[:, 0:128])
        high, mid, low = split3(jnp.concatenate(rows, axis=0))
        bias[h] = dot_nn(high, select) + (dot_nn(mid, select) + dot_nn(low, select))


def same_zone(p, last_row, last_col):
    k = iota((64, 128), 0)
    lane = iota((64, 128), 1)
    q = lane % 64
    rows = ((q // 8) < 4) == ((k // 8) < 4)
    cols = ((q % 8) < 4) == ((k % 8) < 4)
    keep = jnp.logical_or(cols, jnp.logical_or(lane < 64, jnp.logical_not(last_col)))
    if p == 1:
        keep = jnp.logical_and(keep, jnp.logical_or(rows, jnp.logical_not(last_row)))
    return keep


UNITS = [(p, h, slice(128 * p, 128 * p + 128)) for p in range(2) for h in range(HEADS)]


def forward(x, par, need, cols, bias, res, stage, zones, keep):
    left = halves()
    xhat, _ = norm_fwd(x)
    normed = (xhat * cols[0:C, 0:1] + cols[0:C, 1:2]).astype(BF16)
    need("qw")
    res.packed[...] = (dot_tn(par.qw[...], normed) + cols[0:576, 6:7]).astype(BF16)
    for p, h, lanes in UNITS:
        q = res.packed[DIM * h : DIM * h + DIM, lanes]
        k = res.packed[C + DIM * h : C + DIM * h + DIM, lanes]
        s = own_window(dot_tn(k, q), left) * SCALE + bias[h]
        if zones is not None:
            s = jnp.where(zones[p], s, MASKED)
        stage[p * HEADS + h] = s
    for p, h, _ in UNITS:
        s = stage[p * HEADS + h]
        e = jnp.exp(s - jnp.max(s, axis=0, keepdims=True))
        a = e * (1.0 / jnp.sum(e, axis=0, keepdims=True))
        res.attn[p * HEADS + h] = a.astype(BF16)
    for p, h, lanes in UNITS:
        v = res.packed[2 * C + DIM * h : 2 * C + DIM * h + DIM, lanes]
        wide = stack_windows(res.attn[p * HEADS + h].astype(F32), left)
        res.mixed[DIM * h : DIM * h + DIM, lanes] = dot_nn(v, wide).astype(BF16)
    keep("packed")
    need("pw")
    middle = x + dot_tn(par.pw[...], res.mixed[...]) + cols[0:C, 2:3]
    res.middle[...] = middle.astype(BF16)
    middle = res.middle[...].astype(F32)
    xhat, _ = norm_fwd(middle)
    normed = (xhat * cols[0:C, 3:4] + cols[0:C, 4:5]).astype(BF16)
    keep("attn", "mixed")
    need("uw")
    for i in range(0, MLP, 128):
        u = dot_tn(par.uw[:, i : i + 128], normed) + cols[i : i + 128, 7:8]
        half = 0.5 + 0.5 * lax.erf(u * (0.5**0.5))
        res.hidden[i : i + 128, :] = (u * half).astype(BF16)
        res.slope[i : i + 128, :] = (half + u * (jnp.exp(-0.5 * u * u) * 0.3989422804014327)).astype(BF16)
    keep("middle")
    need("dw")
    out = (middle + dot_nn(par.dw[...], res.hidden[...]) + cols[0:C, 5:6]).astype(BF16)
    keep("hidden", "slope")
    return out


def put_row(small, at, row):
    n = row.shape[-1]
    for i in range(0, n, 128):
        w = min(128, n - i)
        small[at + i // 128 : at + i // 128 + 1, 0:w] = row[0:1, i : i + w]


def put_pairs(flat, at, lhs, rhs, n):
    for i in range(0, n, 256):
        wide = dot_nt(lhs, rhs[i : i + 256, :]).astype(BF16)
        for j in range(0, 256, 128):
            first = at + C * ((i + j) // 128)
            flat[first : first + C, :] = wide[:, j : j + 128]


def mlp_grads(g, flat, small):
    ones = jnp.ones((8, TOK), BF16)
    small[...] = jnp.zeros(small.shape, F32)
    put_row(small, 21, dot_nt(ones, g.dout[...]))
    put_row(small, 15, dot_nt(ones, g.du[...]))
    put_row(small, 13, dot_nt(ones, g.dn2[...]))
    put_row(small, 11, dot_nt(ones, g.dg2[...]))
    put_pairs(flat, 1152, g.n2[...], g.du, MLP)
    put_pairs(flat, 2304, g.dout[...], g.hidden, MLP)


def attention_grads(g, flat, small):
    ones = jnp.ones((8, TOK), BF16)
    none = jnp.zeros((64, TOK), BF16)
    put_row(small, 9, dot_nt(ones, g.dmid[...]))
    flat[960:1152, :] = dot_nt(g.mixed[...], g.dmid[0:128, :]).astype(BF16)
    mirror = ((127 - iota((128, 128), 0)) == spread(iota((128, 128), 1))).astype(BF16)
    for h in range(HEADS):
        high, mid, _ = split3(g.rel[h])
        back = dot_nt(high, mirror) + dot_nt(mid, mirror)
        total = jnp.zeros((8, 256), F32)
        for ky in range(8):
            wide = jnp.concatenate([back[8 * ky : 8 * ky + 8], jnp.zeros((8, 128), F32)], axis=1)
            total = total + pltpu.roll(wide, 121 - SPAN * (7 - ky), 1, stride=1, stride_axis=0)
        total = jnp.sum(total, axis=0, keepdims=True)
        small[24 + h : 25 + h, :] = total[:, 0:128]
        small[32 + h : 33 + h, :] = total[:, 128:256]
    put_pairs(flat, 0, g.n1[...], g.dpacked, 512)
    tail = dot_nt(g.n1[...], jnp.concatenate([g.dpacked[512:576, :], none], axis=0))
    tail = tail + dot_nt(g.mixed[...], jnp.concatenate([none, g.dmid[128:192, :]], axis=0))
    flat[768:960, :] = tail.astype(BF16)
    put_row(small, 4, dot_nt(ones, g.dpacked[...]))
    put_row(small, 2, dot_nt(ones, g.dn1[...]))
    put_row(small, 0, dot_nt(ones, g.dg1[...]))
    flat[SMALL : SMALL + 48, :] = small[...].astype(BF16)
    flat[SMALL + 48 : FLAT, :] = jnp.zeros((FLAT - SMALL - 48, 128), BF16)


def backward(x, par, need, cols, res, stage, g, after_mlp):
    left = halves()
    dout = g.dout[...]
    need("dw", "slope")
    for i in range(0, MLP, 128):
        dh = dot_tn(par.dw[:, i : i + 128], dout).astype(BF16).astype(F32)
        g.du[i : i + 128, :] = (dh * res.slope[i : i + 128, :].astype(F32)).astype(BF16)
    need("middle", "uw")
    xhat, rstd = norm_fwd(res.middle[...].astype(F32))
    g.n2[...] = (xhat * cols[0:C, 3:4] + cols[0:C, 4:5]).astype(BF16)
    dn = dot_nn(par.uw[...], g.du[...]).astype(BF16)
    g.dn2[...] = dn
    dn = dn.astype(F32)
    g.dg2[...] = (dn * xhat).astype(BF16)
    dmid = (dout.astype(F32) + norm_bwd(dn, xhat, rstd, cols[0:C, 3:4])).astype(BF16)
    g.dmid[...] = dmid
    after_mlp()
    need("pw", "mixed")
    dmixed = dot_nn(par.pw[...], dmid).astype(BF16)
    need("packed", "attn")
    for p, h, lanes in UNITS:
        v = res.packed[2 * C + DIM * h : 2 * C + DIM * h + DIM, lanes]
        dm = dmixed[DIM * h : DIM * h + DIM, lanes]
        stage[p * HEADS + h] = own_window(dot_tn(v, dm), left).astype(BF16).astype(F32)
        dv = dot_nt(dm, stack_windows(res.attn[p * HEADS + h].astype(F32), left)).astype(BF16)
        g.dpacked[2 * C + DIM * h : 2 * C + DIM * h + DIM, lanes] = dv
    for h in range(HEADS):
        drel = None
        for p in range(2):
            a = res.attn[p * HEADS + h].astype(F32)
            da = stage[p * HEADS + h]
            ds = a * (da - jnp.sum(da * a, axis=0, keepdims=True))
            drel = ds if drel is None else drel + ds
            stage[p * HEADS + h] = ds * SCALE
        g.rel[h] = drel
    for p, h, lanes in UNITS:
        q = res.packed[DIM * h : DIM * h + DIM, lanes]
        k = res.packed[C + DIM * h : C + DIM * h + DIM, lanes]
        wide = stack_windows(stage[p * HEADS + h], left)
        g.dpacked[DIM * h : DIM * h + DIM, lanes] = dot_nn(k, wide).astype(BF16)
        g.dpacked[C + DIM * h : C + DIM * h + DIM, lanes] = dot_nt(q, wide).astype(BF16)
    need("xt")
    xhat, rstd = norm_fwd(x[...].astype(F32))
    g.n1[...] = (xhat * cols[0:C, 0:1] + cols[0:C, 1:2]).astype(BF16)
    need("qw")
    dn = dot_nn(par.qw[...], g.dpacked[...]).astype(BF16)
    g.dn1[...] = dn
    dn = dn.astype(F32)
    g.dg1[...] = (dn * xhat).astype(BF16)
    return dmid.astype(F32) + norm_bwd(dn, xhat, rstd, cols[0:C, 0:1])


def to_channels(pieces):
    return jnp.concatenate(pieces, axis=0).T[0:C]


def to_tokens(value):
    return jnp.concatenate([value, jnp.zeros((64, TOK), F32)], axis=0).T


def grid_put(grid, tokens):
    for r in range(TILE):
        for wc in range(2):
            at = window_row(r, wc)
            grid[r, 8 * wc : 8 * wc + 8, :] = tokens[at : at + 8]


def grid_get(grid, row_at, col_at):
    pieces = []
    for wr in range(2):
        for wc in range(2):
            for ir in range(8):
                at = col_at + 8 * wc
                pieces.append(grid[row_at + 8 * wr + ir, at : at + 8, :])
    return pieces


def emit_strips(grid, edge, strips, which, row_at, col_at):
    col_out, row_out, corner_out = strips
    for r in range(TILE):
        edge[4 * r : 4 * r + 4, :] = grid[r, col_at : col_at + 4, :]
    col_out[64 * which : 64 * which + 64, :] = edge[:, 0:C].astype(BF16)
    for r in range(4):
        row_out[64 * which + 16 * r : 64 * which + 16 * r + 16, :] = grid[row_at + r, 0:TILE, 0:C].astype(BF16)
    for r in range(4):
        edge[4 * r : 4 * r + 4, :] = grid[row_at + r, col_at : col_at + 4, :]
    corner_out[16 * which : 16 * which + 16, :] = edge[0:16, 0:C].astype(BF16)


def fill_grid(grid, edge, own, strips, which, own_row, own_col, strip_row, strip_col):
    col_in, row_in, corner_in = strips
    for r in range(TILE):
        grid[own_row + r, own_col : own_col + TILE, 0:C] = own[r].astype(F32)
    edge[:, 0:C] = col_in[64 * which : 64 * which + 64, :].astype(F32)
    for r in range(TILE):
        grid[own_row + r, strip_col : strip_col + 4, :] = edge[4 * r : 4 * r + 4, :]
    for r in range(4):
        at = 64 * which + 16 * r
        grid[strip_row + r, own_col : own_col + TILE, 0:C] = row_in[at : at + 16, :].astype(F32)
    edge[0:16, 0:C] = corner_in[16 * which : 16 * which + 16, :].astype(F32)
    for r in range(4):
        grid[strip_row + r, strip_col : strip_col + 4, :] = edge[4 * r : 4 * r + 4, :]


PAR_NAMES = ("ng", "nb", "qw", "qb", "rel", "pw", "pb", "mg", "mb", "uw", "ub", "dw", "db")
RES_NAMES = ("packed", "attn", "mixed", "middle", "hidden", "slope")
GRAD_NAMES = ("dout", "n1", "n2", "dmid", "dn1", "dn2", "dg1", "dg2", "du", "dpacked", "rel")
GRAD_SHAPES = ((C, TOK),) * 8 + ((MLP, TOK), (576, TOK), (HEADS, 64, 128))
RES_SHAPES = ((576, TOK), (12, 64, 128), (C, TOK), (C, TOK), (MLP, TOK), (MLP, TOK))


class Copies:
    def __init__(self, sems):
        self.sems = sems
        self.used = 0
        self.open = {}

    def start(self, name, source, target):
        self.open[name] = pltpu.make_async_copy(source, target, self.sems.at[self.used])
        self.open[name].start()
        self.used += 1

    def __call__(self, *names):
        for name in names:
            if name in self.open:
                self.open.pop(name).wait()

    def rest(self):
        self(*list(self.open))


def start_params(copies, names, far, par, b):
    for name in names:
        source = far[name].at[b] if name in WEIGHTS else far[name]
        copies.start(name, source, par[name])


WEIGHTS = ("qw", "pw", "uw", "dw")
PAR_SHAPES = dict(
    ng=(2, C), nb=(2, C), qw=(C, 3 * C), qb=(2, 3 * C), rel=(HEADS, 2, SPAN * SPAN), pw=(C, C), pb=(2, C),
    mg=(2, C), mb=(2, C), uw=(C, MLP), ub=(2, MLP), dw=(C, MLP), db=(2, C),
)


def nothing(*_):
    pass


def first_forward(*refs):
    imagery_far, cotangent_far = refs[0:2]
    far = Box(zip(PAR_NAMES, refs[2:15]))
    own = refs[15]
    strips = refs[16:19]
    xt_far = refs[19]
    res_far = Box(zip(RES_NAMES, refs[20:26]))
    grid, edge, vec, table, bias, sems = refs[26:32]
    par = Box(zip(PAR_NAMES, refs[32:45]))
    res = Box(zip(RES_NAMES, refs[45:51]))
    imagery, cotangent, xt, stage = refs[51:]
    need = Copies(sems)
    need.start("imagery", imagery_far, imagery)
    start_params(need, VEC_NAMES, far, par, 0)
    start_params(need, ("qw", "rel", "pw"), far, par, 0)
    need.start("cotangent", cotangent_far, cotangent)
    start_params(need, ("uw", "dw"), far, par, 0)

    def keep(*names):
        for name in names:
            need.start("out " + name, res[name], res_far[name])

    need("imagery")
    for r in range(TILE):
        grid[r, 0:TILE, 0:C] = imagery[r].astype(F32)
    x = to_channels(grid_get(grid, 0, 0))
    xt[...] = x.astype(BF16)
    need(*VEC_NAMES, "rel", "qw", "pw", "cotangent")
    cols = load_columns(vec, par, 0)
    position_bias(par, 0, table, bias)
    for r in range(TILE):
        grid[r, 0:TILE, 0:C] = cotangent[r].astype(F32)
    emit_strips(grid, edge, strips, 1, 0, 0)
    need.start("out xt", xt, xt_far)
    out = forward(x, par, need, cols, bias, res, stage, None, keep)
    grid_put(grid, to_tokens(out.astype(F32)))
    for r in range(TILE):
        own[r] = grid[r, 0:TILE, 0:C].astype(BF16)
    emit_strips(grid, edge, strips, 0, 0, 0)
    need.rest()


def second_block(*refs):
    own_in = refs[0]
    strips_in = refs[1:4]
    cotangent_far = refs[4]
    far = Box(zip(PAR_NAMES, refs[5:18]))
    out_own, back_own = refs[18:20]
    strips = refs[20:23]
    g = Box(zip(GRAD_NAMES + ("hidden", "mixed"), refs[23:36]))
    grid, edge, vec, table, bias, sems = refs[36:42]
    par = Box(zip(PAR_NAMES, refs[42:55]))
    res = Box(zip(("packed", "attn", "middle", "slope"), refs[55:59]), hidden=g.hidden, mixed=g.mixed)
    cotangent, xt, stage = refs[59:]
    need = Copies(sems)
    start_params(need, VEC_NAMES + ("rel",), far, par, 1)
    need.start("cotangent", cotangent_far, cotangent)
    start_params(need, ("qw", "pw", "uw", "dw"), far, par, 1)
    last_row = lax.axis_index("rows") == lax.axis_size("rows") - 1
    last_col = lax.axis_index("cols") == lax.axis_size("cols") - 1
    zones = [same_zone(p, last_row, last_col) for p in range(2)]
    fill_grid(grid, edge, own_in, strips_in, 0, 0, 0, 16, 16)
    x = to_channels(grid_get(grid, 4, 4))
    xt[...] = x.astype(BF16)
    need(*VEC_NAMES, "rel", "cotangent")
    cols = load_columns(vec, par, 1)
    position_bias(par, 1, table, bias)
    fill_grid(grid, edge, cotangent, strips_in, 1, 0, 0, 16, 16)
    g.dout[...] = to_channels(grid_get(grid, 4, 4)).astype(BF16)
    out = forward(x, par, need, cols, bias, res, stage, zones, nothing)
    grid_put(grid, to_tokens(out.astype(F32)))
    for r in range(TILE):
        out_own[r] = grid[r, 0:TILE, 0:C].astype(BF16)
    emit_strips(grid, edge, strips, 0, 12, 12)
    dx = backward(xt, par, need, cols, res, stage, g, nothing)
    grid_put(grid, to_tokens(dx))
    for r in range(TILE):
        back_own[r] = grid[r, 0:TILE, 0:C].astype(BF16)
    emit_strips(grid, edge, strips, 1, 12, 12)
    need.rest()


def second_grads(*refs):
    g = Box(zip(GRAD_NAMES + ("hidden", "mixed"), refs[0:13]))
    flat, small = refs[13:]
    mlp_grads(g, flat, small)
    attention_grads(g, flat, small)


BACK_NAMES = VEC_NAMES + WEIGHTS


def first_backward(*refs):
    back_in = refs[0]
    strips_in = refs[1:4]
    flat_two = refs[4]
    far = Box(zip(BACK_NAMES, refs[5:17]))
    xt_far = refs[17]
    res_far = Box(zip(RES_NAMES, refs[18:24]))
    dx_channels, kept, sent = refs[24:27]
    grid, edge, vec, sems = refs[27:31]
    par = Box(zip(BACK_NAMES, refs[31:43]))
    g = Box(zip(GRAD_NAMES, refs[43:54]))
    res = Box(zip(RES_NAMES, refs[54:60]))
    xt, flat, small, stage = refs[60:]
    g = Box(g, hidden=res.hidden, mixed=res.mixed)
    need = Copies(sems)
    start_params(need, ("dw",), far, par, 0)
    need.start("slope", res_far.slope, res.slope)
    start_params(need, VEC_NAMES, far, par, 0)
    need.start("middle", res_far.middle, res.middle)
    start_params(need, ("uw",), far, par, 0)
    need.start("hidden", res_far.hidden, res.hidden)
    need.start("mixed", res_far.mixed, res.mixed)
    start_params(need, ("pw",), far, par, 0)
    need.start("packed", res_far.packed, res.packed)
    need.start("attn", res_far.attn, res.attn)
    need.start("xt", xt_far, xt)
    start_params(need, ("qw",), far, par, 0)
    fill_grid(grid, edge, back_in, strips_in, 1, 4, 8, 0, 4)
    g.dout[...] = to_channels(grid_get(grid, 0, 4)).astype(BF16)
    need(*VEC_NAMES)
    cols = load_columns(vec, par, 0)

    def after_mlp():
        need("hidden")
        mlp_grads(g, flat, small)

    dx_channels[...] = backward(xt, par, need, cols, res, stage, g, after_mlp).astype(BF16)
    attention_grads(g, flat, small)
    even = lax.axis_index("cols") % 2 == 0
    for at in range(0, FLAT, 256):
        rows = slice(at, at + 256)
        kept[rows, :] = jnp.where(even, flat[rows, :], flat_two[rows, :])
        sent[rows, :] = jnp.where(even, flat_two[rows, :], flat[rows, :])
    need.rest()


def make_tiles(out_own, col_in, row_in, corner_in, dx_channels, output, grad, grid, edge):
    fill_grid(grid, edge, out_own, (col_in, row_in, corner_in), 0, 4, 8, 0, 4)
    for r in range(TILE):
        output[r] = grid[r, 4:20, 0:C].astype(BF16)
    grid_put(grid, to_tokens(dx_channels[...].astype(F32)))
    for r in range(TILE):
        grad[r] = grid[r, 0:TILE, 0:C].astype(BF16)


def add_pair(kept, got, out):
    for at in range(0, FLAT, 256):
        rows = slice(at, at + 256)
        out[rows, :] = (kept[rows, :].astype(F32) + got[rows, :].astype(F32)).astype(BF16)


def sum_spread(share, parts, out):
    total = jnp.zeros((share, 128), F32)
    for at in range(0, FLAT, share):
        total = total + parts[at : at + share, :].astype(F32)
    total = total.astype(BF16)
    for at in range(0, FLAT, share):
        out[at : at + share, :] = total


def unpack_weights(rows, b, near_refs, far_refs, copies):
    qw, pw, uw, dw = near_refs
    for j in range(4):
        qw[:, 128 * j : 128 * j + 128] = rows(C * j, C)
    tail = rows(768, C)
    qw[:, 512:576] = tail[:, 0:64]
    copies.start("qw", qw, far_refs[0].at[b])
    pw[:, 128:192] = pltpu.roll(tail, 64, 1)[:, 0:64]
    pw[:, 0:128] = rows(960, C)
    copies.start("pw", pw, far_refs[1].at[b])
    for j in range(6):
        uw[:, 128 * j : 128 * j + 128] = rows(1152 + C * j, C)
    copies.start("uw", uw, far_refs[2].at[b])
    for j in range(6):
        dw[:, 128 * j : 128 * j + 128] = rows(2304 + C * j, C)
    copies.start("dw", dw, far_refs[3].at[b])


def unpack_mine(mine, *refs):
    copies = Copies(refs[8])
    parity = lax.axis_index("cols") % 2
    unpack_weights(lambda at, n: mine[at : at + n, :].astype(F32) * outs_factor, parity, refs[4:8], refs[0:4], copies)
    copies.rest()


def unpack_rest(mine, other, *refs):
    far = Box(zip(PAR_NAMES, refs[4:17]))
    near_refs = Box(zip(PAR_NAMES, refs[17:30]))
    copies = Copies(refs[30])
    factor = outs_factor
    parity = lax.axis_index("cols") % 2
    unpack_weights(lambda at, n: other[at : at + n, :].astype(F32) * factor, 1 - parity, [near_refs[n] for n in WEIGHTS], [far[n] for n in WEIGHTS], copies)
    flip = (iota((256, 256), 0) + iota((256, 256), 1) == 255).astype(BF16)
    for b in range(2):

        def raw(at, n):
            return jnp.where(parity == b, mine[at : at + n, :], other[at : at + n, :])

        small = raw(SMALL, 48).astype(F32) * factor
        for at, name in ((0, "ng"), (2, "nb"), (4, "qb"), (9, "pb"), (11, "mg"), (13, "mb"), (15, "ub"), (21, "db")):
            ref = near_refs[name]
            n = ref.shape[-1]
            for i in range(0, n, 128):
                w = min(128, n - i)
                ref[b : b + 1, i : i + w] = small[at + i // 128 : at + i // 128 + 1, 0:w]
        table = jnp.concatenate([raw(SMALL + 24, 8), raw(SMALL + 32, 8)], axis=1)
        table = dot_nn(table, flip) * factor
        for h in range(HEADS):
            near_refs.rel[h, b : b + 1, :] = table[h : h + 1, 0 : SPAN * SPAN]
    for name in VEC_NAMES + ("rel",):
        copies.start(name, near_refs[name], far[name])
    copies.rest()


outs_factor = float(128 * 256) ** (-0.5)


VMEM = pl.BlockSpec(memory_space=pltpu.VMEM)


def near(value):
    return pltpu.with_memory_space_constraint(value, pltpu.VMEM)


FAR = pl.BlockSpec(memory_space=pltpu.HBM)


def call(kernel, args, far_args, outs, far_outs, scratch, flops, plain=()):
    return pl.pallas_call(
        kernel,
        in_specs=[VMEM] * len(args) + [FAR] * len(far_args),
        out_specs=[VMEM] * (len(outs) + len(plain)) + [FAR] * len(far_outs),
        out_shape=list(outs) + list(plain) + [pltpu.HBM(o.shape, o.dtype) for o in far_outs],
        scratch_shapes=scratch,
        compiler_params=pltpu.CompilerParams(vmem_limit_bytes=30 * 2**20),
        cost_estimate=pl.CostEstimate(flops=flops, transcendentals=0, bytes_accessed=4000000),
    )(*[near(a) for a in args], *[pltpu.with_memory_space_constraint(a, pltpu.HBM) for a in far_args])


def shaped(shape, dtype=BF16):
    return jax.ShapeDtypeStruct(shape, dtype)


def exchange(strips, step):
    n_rows = lax.axis_size("rows")
    n_cols = lax.axis_size("cols")
    col_strip, row_strip, corner = strips
    along = [(c, (c + step) % n_cols) for c in range(n_cols)]
    down = [(r, (r + step) % n_rows) for r in range(n_rows)]
    both = [
        (r * n_cols + c, ((r + step) % n_rows) * n_cols + (c + step) % n_cols)
        for r in range(n_rows)
        for c in range(n_cols)
    ]
    return [
        lax.ppermute(col_strip, "cols", along),
        lax.ppermute(row_strip, "rows", down),
        lax.ppermute(corner, ("rows", "cols"), both),
    ]


def swap(value):
    return lax.ppermute(value, "cols", [(c, c ^ 1) for c in range(lax.axis_size("cols"))])


def send_parts(value):
    n_cols = lax.axis_size("cols")
    n = lax.axis_size("rows") * n_cols
    groups = [[d for d in range(n) if d % n_cols % 2 == p] for p in range(2)]
    parts = value.reshape(n // 2, 2 * FLAT // n, 128)
    got = lax.all_to_all(parts, ("rows", "cols"), 0, 0, axis_index_groups=groups, tiled=True)
    return got.reshape(value.shape)


def both_blocks(imagery, cotangent, *params):
    params = list(params)
    params[4] = params[4].transpose(1, 0, 2)
    params[11] = params[11].swapaxes(1, 2)
    tile = (TILE, TILE, C)
    strips = [pltpu.VMEM(s, BF16) for s in ((128, C), (128, C), (32, C))]
    packed_grads = pltpu.VMEM((FLAT, 128), BF16)
    held = pltpu.VMEM(tile, BF16)
    grid = pltpu.VMEM((24, 24, 256), F32)
    edge = pltpu.VMEM((64, 256), F32)
    vec = pltpu.VMEM((128, MLP), F32)
    tables = [pltpu.VMEM((8, 256), F32), pltpu.VMEM((HEADS, 64, 128), F32)]
    par = Box(zip(PAR_NAMES, params))
    par_kinds = {n: BF16 if n in WEIGHTS else F32 for n in PAR_NAMES}
    par_vmem = {n: pltpu.VMEM(PAR_SHAPES[n], par_kinds[n]) for n in PAR_NAMES}
    res_vmem = [pltpu.VMEM(s, BF16) for s in RES_SHAPES]
    sems = pltpu.SemaphoreType.DMA((32,))
    stage = pltpu.VMEM((2 * HEADS, 64, 128), F32)
    one = call(
        first_forward,
        (),
        (imagery, cotangent, *params),
        [held] + strips,
        [shaped((C, TOK))] + [shaped(s) for s in RES_SHAPES],
        [grid, edge, vec] + tables + [sems] + list(par_vmem.values()) + res_vmem + [held, held, pltpu.VMEM((C, TOK), BF16), stage],
        5 * 10**9,
    )
    own, xt, res = one[0], one[4], one[5:]
    got = exchange(one[1:4], -1)
    channels = pltpu.VMEM((C, TOK), BF16)
    grad_vmem = [pltpu.VMEM(s, F32 if n == "rel" else BF16) for n, s in zip(GRAD_NAMES, GRAD_SHAPES)]
    small = pltpu.VMEM((48, 128), F32)
    two = call(
        second_block,
        (own, *got),
        (cotangent, *params),
        [held, held] + strips + grad_vmem + [res_vmem[4], res_vmem[2]],
        [],
        [grid, edge, vec]
        + tables
        + [sems]
        + list(par_vmem.values())
        + [res_vmem[i] for i in (0, 1, 3, 5)]
        + [held, pltpu.VMEM((C, TOK), BF16), stage],
        10**10,
    )
    got = exchange(two[2:5], 1)
    flat_two = call(second_grads, two[5:], (), [packed_grads], [], [small], 10**9)[0]
    dx, kept, sent = call(
        first_backward,
        (two[1], *got, flat_two),
        (*[par[n] for n in BACK_NAMES], xt, *res),
        [channels, packed_grads, packed_grads],
        [],
        [grid, edge, vec, sems]
        + [par_vmem[n] for n in BACK_NAMES]
        + grad_vmem
        + res_vmem
        + [channels, packed_grads, small, stage],
        5 * 10**9,
    )
    sent = swap(sent)
    tiles = [shaped(tile), shaped(tile)]
    output, grad = call(make_tiles, (two[0], *got, dx), (), [], [], [grid, edge], 10**9, plain=tiles)
    parts = send_parts(call(add_pair, (kept, sent), (), [packed_grads], [], [], 10**6)[0])
    share = 2 * FLAT // (lax.axis_size("rows") * lax.axis_size("cols"))
    spread_sum = functools.partial(sum_spread, share)
    mine = send_parts(call(spread_sum, (parts,), (), [packed_grads], [], [], 10**6)[0])
    weights = [pltpu.VMEM(PAR_SHAPES[n], F32) for n in WEIGHTS]
    weights_far = [pltpu.HBM((2,) + PAR_SHAPES[n], F32) for n in WEIGHTS]
    few_sems = pltpu.SemaphoreType.DMA((4,))
    half = call(unpack_mine, (mine,), (), [], weights_far, weights + [few_sems], 10**9)
    grads = pl.pallas_call(
        unpack_rest,
        in_specs=[VMEM, VMEM] + [FAR] * 4,
        out_specs=[FAR] * len(PAR_NAMES),
        out_shape=[pltpu.HBM(p.shape, F32) for p in params],
        scratch_shapes=[pltpu.VMEM(PAR_SHAPES[n], F32) for n in PAR_NAMES] + [pltpu.SemaphoreType.DMA((16,))],
        input_output_aliases={2: 2, 3: 5, 4: 9, 5: 11},
        compiler_params=pltpu.CompilerParams(vmem_limit_bytes=30 * 2**20),
    )(near(mine), near(swap(mine)), *[pltpu.with_memory_space_constraint(h, pltpu.HBM) for h in half])
    grads = list(grads)
    grads[4] = grads[4].transpose(1, 0, 2)
    grads[11] = grads[11].swapaxes(1, 2)
    return (output, grad, *grads)


def solution(mesh):
    tile = P("rows", "cols", None)
    return jax.shard_map(
        both_blocks,
        mesh=mesh,
        in_specs=(tile, tile) + (P(),) * 13,
        out_specs=(tile, tile) + (P(),) * 13,
        check_vma=False,
    )
```
